32 devices in a mesh: data: 1 (over z), dap: 32 (over y, x, core).
Axes of the slice: x: 4, y: 4, z: 1, core: 2. Of those that a mesh axis runs over, the one named last changes fastest.
The devices are a block of a 4x4x8 slice.
Arguments:
- msa_act: bfloat16 [256, 128, 384], P(('data', 'dap'))
- pair_act: bfloat16 [128, 128, 288], P(('data', 'dap'))
- msa_mask: int32 [256, 128], P('data')
- res_mask: int32 [128], P('data')
- w_row_bias: bfloat16 [2, 288, 12], replicated
- w_row_in: bfloat16 [2, 384, 4, 12, 32], replicated
- w_row_out: bfloat16 [2, 12, 32, 384], replicated
- w_col_in: bfloat16 [2, 384, 4, 12, 32], replicated
- w_col_out: bfloat16 [2, 12, 32, 384], replicated
- w_opm_in: bfloat16 [2, 384, 2, 32], replicated
- w_opm_out: bfloat16 [2, 32, 32, 288], replicated
- w_ts_bias: bfloat16 [2, 288, 8], replicated
- w_ts_in: bfloat16 [2, 288, 4, 8, 36], replicated
- w_ts_out: bfloat16 [2, 8, 36, 288], replicated
- w_te_bias: bfloat16 [2, 288, 8], replicated
- w_te_in: bfloat16 [2, 288, 4, 8, 36], replicated
- w_te_out: bfloat16 [2, 8, 36, 288], replicated
Outputs:
- output 1: bfloat16 [256, 128, 384], P(('data', 'dap'))
- output 2: bfloat16 [128, 128, 288], P(('data', 'dap'))
All inputs are finite; a program needn't handle non-finite values.
Results may differ from the reference program's by a relative error of at most 0.0173621.
Values are sent between devices in bfloat16 or wider.
A program may use at most 768 MiB of HBM per device.

```python
import jax
import jax.numpy as jnp
from jax import lax

NR = 128
NS = 256
C_M = 384
C_Z = 288
HEADS_MSA = 12
HEAD_MSA = 32
HEADS_TRI = 8
HEAD_TRI = 36
OPM_DIM = 32


def draw_normal(key, shape, scale):
    return (jax.random.normal(key, shape, jnp.float32) * scale).astype(jnp.bfloat16)


def setup_inputs(seed: int = 0, part: int = 0) -> dict:
    base_key = jax.random.key(seed)
    part_keys = jax.random.split(jax.random.fold_in(base_key, part), 4)
    w_keys = jax.random.split(jax.random.fold_in(base_key, 1000), 13)
    width_msa = HEADS_MSA * HEAD_MSA
    width_tri = HEADS_TRI * HEAD_TRI
    return {
        'msa_act': draw_normal(part_keys[0], (NS, NR, C_M), 1.0),
        'pair_act': draw_normal(part_keys[1], (NR, NR, C_Z), 1.0),
        'msa_mask': (jax.random.randint(part_keys[2], (NS, NR), 0, 4) > 0).astype(jnp.int32),
        'res_mask': (jax.random.randint(part_keys[3], (NR,), 0, 4) > 0).astype(jnp.int32),
        'w_row_bias': draw_normal(w_keys[0], (2, C_Z, HEADS_MSA), 1.5 * C_Z ** -0.5),
        'w_row_in': draw_normal(w_keys[1], (2, C_M, 4, HEADS_MSA, HEAD_MSA), 1.25 * C_M ** -0.5),
        'w_row_out': draw_normal(w_keys[2], (2, HEADS_MSA, HEAD_MSA, C_M), 0.5 * width_msa ** -0.5),
        'w_col_in': draw_normal(w_keys[3], (2, C_M, 4, HEADS_MSA, HEAD_MSA), 1.25 * C_M ** -0.5),
        'w_col_out': draw_normal(w_keys[4], (2, HEADS_MSA, HEAD_MSA, C_M), 0.5 * width_msa ** -0.5),
        'w_opm_in': draw_normal(w_keys[5], (2, C_M, 2, OPM_DIM), C_M ** -0.5),
        'w_opm_out': draw_normal(w_keys[6], (2, OPM_DIM, OPM_DIM, C_Z), 0.25 * NS ** 0.5 / OPM_DIM),
        'w_ts_bias': draw_normal(w_keys[7], (2, C_Z, HEADS_TRI), 1.5 * C_Z ** -0.5),
        'w_ts_in': draw_normal(w_keys[8], (2, C_Z, 4, HEADS_TRI, HEAD_TRI), 1.25 * C_Z ** -0.5),
        'w_ts_out': draw_normal(w_keys[9], (2, HEADS_TRI, HEAD_TRI, C_Z), 0.5 * width_tri ** -0.5),
        'w_te_bias': draw_normal(w_keys[10], (2, C_Z, HEADS_TRI), 1.5 * C_Z ** -0.5),
        'w_te_in': draw_normal(w_keys[11], (2, C_Z, 4, HEADS_TRI, HEAD_TRI), 1.25 * C_Z ** -0.5),
        'w_te_out': draw_normal(w_keys[12], (2, HEADS_TRI, HEAD_TRI, C_Z), 0.5 * width_tri ** -0.5),
    }


def layer_norm(values):
    flat = values.astype(jnp.float32)
    row_mean = jnp.mean(flat, axis=-1, keepdims=True)
    centered = flat - row_mean
    row_var = jnp.mean(centered * centered, axis=-1, keepdims=True)
    return (centered * lax.rsqrt(row_var + 1e-5)).astype(jnp.bfloat16)


def add_residual(current, update):
    return (current.astype(jnp.float32) + update).astype(jnp.bfloat16)


def pair_bias(pair_ln, w_bias):
    num_res = pair_ln.shape[0]
    flat = jnp.dot(pair_ln.reshape(num_res * num_res, -1), w_bias, preferred_element_type=jnp.float32)
    return jnp.transpose(flat.astype(jnp.bfloat16).reshape(num_res, num_res, -1), (2, 0, 1))


def attend_one(x_ln, w_in, w_out, bias_hqk, key_mask):
    length = x_ln.shape[0]
    heads = w_in.shape[2]
    head_dim = w_in.shape[3]
    projected = jnp.dot(x_ln, w_in.reshape(w_in.shape[0], -1), preferred_element_type=jnp.float32)
    projected = projected.astype(jnp.bfloat16).astype(jnp.float32).reshape(length, 4, heads, head_dim)
    logits = jnp.einsum('qhd,khd->hqk', projected[:, 0], projected[:, 1]) * head_dim ** -0.5
    if bias_hqk is not None:
        logits = logits + bias_hqk.astype(jnp.float32)
    logits = jnp.where(key_mask[None, None, :] > 0, logits, -1e9)
    attn_probs = jax.nn.softmax(logits, axis=-1).astype(jnp.bfloat16).astype(jnp.float32)
    attended = jnp.einsum('hqk,khd->qhd', attn_probs, projected[:, 2])
    gated = (attended * jax.nn.sigmoid(projected[:, 3])).astype(jnp.bfloat16)
    return jnp.dot(gated.reshape(length, heads * head_dim), w_out.reshape(heads * head_dim, -1), preferred_element_type=jnp.float32)


def row_attention(msa_act, bias_hqk, msa_mask, w_in, w_out):
    def one_seq(inputs):
        seq_act, seq_mask = inputs
        return add_residual(seq_act, attend_one(layer_norm(seq_act), w_in, w_out, bias_hqk, seq_mask))
    return lax.map(one_seq, (msa_act, msa_mask))


def column_attention(msa_act, msa_mask, w_in, w_out):
    def one_col(inputs):
        col_act, col_mask = inputs
        return add_residual(col_act, attend_one(layer_norm(col_act), w_in, w_out, None, col_mask))
    result = lax.map(one_col, (jnp.swapaxes(msa_act, 0, 1), msa_mask.T))
    return jnp.swapaxes(result, 0, 1)


def outer_mean(msa_act, pair_act, msa_mask, w_in, w_out):
    num_seq, num_res, width = msa_act.shape
    mask_f32 = msa_mask.astype(jnp.float32)
    projected = jnp.dot(layer_norm(msa_act).reshape(num_seq * num_res, width), w_in.reshape(width, -1), preferred_element_type=jnp.float32)
    projected = projected.reshape(num_seq, num_res, 2, -1) * mask_f32[:, :, None, None]
    projected = projected.astype(jnp.bfloat16).astype(jnp.float32)
    left = jnp.swapaxes(projected[:, :, 0], 0, 1)
    right = projected[:, :, 1]
    pair_norm = jnp.dot(mask_f32.T, mask_f32)
    w_flat = w_out.reshape(-1, w_out.shape[-1])
    def one_row(inputs):
        left_row, norm_row = inputs
        outer = jnp.einsum('sp,sjq->jpq', left_row, right).astype(jnp.bfloat16)
        update = jnp.dot(outer.reshape(num_res, -1), w_flat, preferred_element_type=jnp.float32)
        return update / (1e-3 + norm_row[:, None])
    return add_residual(pair_act, lax.map(one_row, (left, pair_norm)))


def triangle_start(pair_act, res_mask, w_bias, w_in, w_out):
    pair_ln = layer_norm(pair_act)
    bias_hqk = pair_bias(pair_ln, w_bias)
    def one_row(row_ln):
        return attend_one(row_ln, w_in, w_out, bias_hqk, res_mask)
    return add_residual(pair_act, lax.map(one_row, pair_ln))


def triangle_end(pair_act, res_mask, w_bias, w_in, w_out):
    flipped = triangle_start(jnp.swapaxes(pair_act, 0, 1), res_mask, w_bias, w_in, w_out)
    return jnp.swapaxes(flipped, 0, 1)


def reference(msa_act, pair_act, msa_mask, res_mask, w_row_bias, w_row_in, w_row_out, w_col_in, w_col_out, w_opm_in, w_opm_out, w_ts_bias, w_ts_in, w_ts_out, w_te_bias, w_te_in, w_te_out):
    bias_first = pair_bias(layer_norm(pair_act), w_row_bias[0])
    msa_act = row_attention(msa_act, bias_first, msa_mask, w_row_in[0], w_row_out[0])
    msa_act = column_attention(msa_act, msa_mask, w_col_in[0], w_col_out[0])
    pair_act = outer_mean(msa_act, pair_act, msa_mask, w_opm_in[0], w_opm_out[0])
    pair_act = triangle_start(pair_act, res_mask, w_ts_bias[0], w_ts_in[0], w_ts_out[0])
    pair_act = triangle_end(pair_act, res_mask, w_te_bias[0], w_te_in[0], w_te_out[0])
    bias_second = pair_bias(layer_norm(pair_act), w_row_bias[1])
    msa_act = column_attention(msa_act, msa_mask, w_col_in[1], w_col_out[1])
    pair_act = outer_mean(msa_act, pair_act, msa_mask, w_opm_in[1], w_opm_out[1])
    msa_act = row_attention(msa_act, bias_second, msa_mask, w_row_in[1], w_row_out[1])
    pair_act = triangle_end(pair_act, res_mask, w_te_bias[1], w_te_in[1], w_te_out[1])
    pair_act = triangle_start(pair_act, res_mask, w_ts_bias[1], w_ts_in[1], w_ts_out[1])
    return msa_act, pair_act
```

```python
import functools

import jax
import jax.numpy as jnp
from jax import lax
from jax.experimental import pallas as pl
from jax.experimental.pallas import tpu as pltpu
from jax.sharding import PartitionSpec as P


def layer_norm(values):
    flat = values.astype(jnp.float32)
    row_mean = jnp.mean(flat, axis=-1, keepdims=True)
    centered = flat - row_mean
    row_var = jnp.mean(centered * centered, axis=-1, keepdims=True)
    return (centered * lax.rsqrt(row_var + 1e-5)).astype(jnp.bfloat16)


def add_residual(current, update):
    return (current.astype(jnp.float32) + update).astype(jnp.bfloat16)


def pair_bias(pair_ln, w_bias, form):
    return jnp.einsum(form, pair_ln, w_bias, preferred_element_type=jnp.float32).astype(jnp.bfloat16)


def gather_kernel(n, x_ref, o_ref, send_sem, recv_sem):
    me = lax.axis_index('dap')
    barrier = pltpu.get_barrier_semaphore()

    @pl.loop(1, n)
    def _(k):
        pl.semaphore_signal(barrier, inc=1, device_id={'dap': lax.rem(me + k, n)}, device_id_type=pl.DeviceIdType.MESH)
    o_ref[me] = x_ref[...]
    pl.semaphore_wait(barrier, n - 1)

    def copy(k):
        return pltpu.make_async_remote_copy(src_ref=x_ref, dst_ref=o_ref.at[me], send_sem=send_sem, recv_sem=recv_sem, device_id={'dap': lax.rem(me + k, n)}, device_id_type=pl.DeviceIdType.MESH)

    @pl.loop(1, n)
    def _(k):
        copy(k).start()

    bulk = o_ref.at[pl.ds(0, n - 1)]
    pltpu.make_async_copy(bulk, bulk, send_sem).wait()
    pltpu.make_async_copy(bulk, bulk, recv_sem).wait()


def gather_all(x, n, cid):
    return pl.pallas_call(
        functools.partial(gather_kernel, n),
        out_shape=jax.ShapeDtypeStruct((n,) + x.shape, x.dtype),
        in_specs=[pl.BlockSpec(memory_space=pltpu.VMEM)],
        out_specs=pl.BlockSpec(memory_space=pltpu.VMEM),
        scratch_shapes=[pltpu.SemaphoreType.DMA, pltpu.SemaphoreType.DMA],
        compiler_params=pltpu.CompilerParams(collective_id=cid, has_side_effects=True),
    )(x)


def gather_rows(x, n, cid, axis):
    if axis == 1:
        h, r, c = x.shape
        got = gather_all(x.transpose(1, 0, 2).reshape(r * h, c), n, cid).reshape(n, r, h, c)
        return got.transpose(2, 0, 1, 3).reshape(h, n * r, c)
    h, c, r = x.shape
    got = gather_all(x.transpose(2, 0, 1).reshape(r * h, c), n, cid).reshape(n, r, h, c)
    return got.transpose(2, 3, 0, 1).reshape(h, c, n * r)


def gated_attention(x_ln, w_in, w_out, bias_hqk, key_mask, batch_first):
    head_dim = w_in.shape[3]
    projected = jnp.einsum('abc,cfhd->abfhd', x_ln, w_in, preferred_element_type=jnp.float32).astype(jnp.bfloat16)
    query = projected[:, :, 0]
    keys = projected[:, :, 1]
    values = projected[:, :, 2]
    gate_raw = projected[:, :, 3]
    if batch_first:
        logits = jnp.einsum('bqhd,bkhd->bhqk', query, keys, preferred_element_type=jnp.float32)
    else:
        logits = jnp.einsum('qbhd,kbhd->bhqk', query, keys, preferred_element_type=jnp.float32)
    logits = logits * head_dim ** -0.5
    if bias_hqk is not None:
        logits = logits + bias_hqk.astype(jnp.float32)
    logits = jnp.where(key_mask > 0, logits, -1e9)
    attn_probs = jax.nn.softmax(logits, axis=-1).astype(jnp.bfloat16)
    if batch_first:
        attended = jnp.einsum('bhqk,bkhd->bqhd', attn_probs, values, preferred_element_type=jnp.float32)
    else:
        attended = jnp.einsum('bhqk,kbhd->qbhd', attn_probs, values, preferred_element_type=jnp.float32)
    gated = (attended * jax.nn.sigmoid(gate_raw.astype(jnp.float32))).astype(jnp.bfloat16)
    return jnp.einsum('abhd,hdc->abc', gated, w_out, preferred_element_type=jnp.float32)


def opm_halves(value_a8, mask_cols, w_in):
    projected = jnp.einsum('sic,cfp->sifp', layer_norm(value_a8), w_in, preferred_element_type=jnp.float32)
    projected = (projected * mask_cols.astype(jnp.float32)[:, :, None, None]).astype(jnp.bfloat16)
    return projected[:, :, 0], projected[:, :, 1]


def opm_update(pair_act, left, right, left_mask, right_mask, w_out):
    outer = jnp.einsum('sip,sjq->ijpq', left, right, preferred_element_type=jnp.float32).astype(jnp.bfloat16)
    update = jnp.einsum('ijpq,pqc->ijc', outer, w_out, preferred_element_type=jnp.float32)
    pair_norm = jnp.einsum('si,sj->ij', left_mask.astype(jnp.bfloat16), right_mask.astype(jnp.bfloat16), preferred_element_type=jnp.float32)
    return add_residual(pair_act, update / (1e-3 + pair_norm)[:, :, None])


def solution(mesh):
    n = mesh.shape['dap']

    def local_step(value_a7, pair_blk, array_b8, res_mask, w_row_bias, w_row_in, w_row_out, w_col_in, w_col_out, w_opm_in, w_opm_out, w_ts_bias, w_ts_in, w_ts_out, w_te_bias, w_te_in, w_te_out):
        dev_index = lax.axis_index('dap')
        seq_loc = value_a7.shape[0]
        res_loc = pair_blk.shape[0]
        mask_seq = lax.dynamic_slice_in_dim(array_b8, dev_index * seq_loc, seq_loc, 0)
        mask_cols = lax.dynamic_slice_in_dim(array_b8, dev_index * res_loc, res_loc, 1)
        row_keys = mask_seq[:, None, None, :]
        col_keys = mask_cols.T[:, None, None, :]
        tri_keys = res_mask[None, None, None, :]

        row_bias = gather_rows(pair_bias(layer_norm(pair_blk), w_row_bias[0], 'ijc,ch->hij'), n, 0, 1)
        value_a7 = add_residual(value_a7, gated_attention(layer_norm(value_a7), w_row_in[0], w_row_out[0], row_bias, row_keys, True))
        value_a7 = lax.all_to_all(value_a7, 'dap', 1, 0, tiled=True)
        value_a7 = add_residual(value_a7, gated_attention(layer_norm(value_a7), w_col_in[0], w_col_out[0], None, col_keys, False))
        left, right = opm_halves(value_a7, mask_cols, w_opm_in[0])
        right_full = lax.all_gather(right, 'dap', axis=1, tiled=True)
        pair_blk = opm_update(pair_blk, left, right_full, mask_cols, array_b8, w_opm_out[0])
        pair_ln = layer_norm(pair_blk)
        tri_bias = gather_rows(pair_bias(pair_ln, w_ts_bias[0], 'ijc,ch->hij'), n, 1, 1)
        pair_blk = add_residual(pair_blk, gated_attention(pair_ln, w_ts_in[0], w_ts_out[0], tri_bias, tri_keys, True))
        pair_blk = lax.all_to_all(pair_blk, 'dap', 1, 0, tiled=True)
        pair_ln = layer_norm(pair_blk)
        tri_bias = gather_rows(pair_bias(pair_ln, w_te_bias[0], 'kic,ch->hik'), n, 2, 1)
        pair_blk = add_residual(pair_blk, gated_attention(pair_ln, w_te_in[0], w_te_out[0], tri_bias, tri_keys, False))

        row_bias = gather_rows(pair_bias(layer_norm(pair_blk), w_row_bias[1], 'ijc,ch->hij'), n, 3, 2)
        value_a7 = add_residual(value_a7, gated_attention(layer_norm(value_a7), w_col_in[1], w_col_out[1], None, col_keys, False))
        left, right = opm_halves(value_a7, mask_cols, w_opm_in[1])
        left_full = lax.all_gather(left, 'dap', axis=1, tiled=True)
        pair_blk = opm_update(pair_blk, left_full, right, array_b8, mask_cols, w_opm_out[1])
        value_a7 = lax.all_to_all(value_a7, 'dap', 0, 1, tiled=True)
        value_a7 = add_residual(value_a7, gated_attention(layer_norm(value_a7), w_row_in[1], w_row_out[1], row_bias, row_keys, True))
        pair_ln = layer_norm(pair_blk)
        tri_bias = gather_rows(pair_bias(pair_ln, w_te_bias[1], 'kic,ch->hik'), n, 4, 1)
        pair_blk = add_residual(pair_blk, gated_attention(pair_ln, w_te_in[1], w_te_out[1], tri_bias, tri_keys, False))
        pair_blk = lax.all_to_all(pair_blk, 'dap', 0, 1, tiled=True)
        pair_ln = layer_norm(pair_blk)
        tri_bias = gather_rows(pair_bias(pair_ln, w_ts_bias[1], 'ijc,ch->hij'), n, 5, 1)
        pair_blk = add_residual(pair_blk, gated_attention(pair_ln, w_ts_in[1], w_ts_out[1], tri_bias, tri_keys, True))
        return value_a7, pair_blk

    in_specs = (P(('data', 'dap')), P(('data', 'dap')), P('data'), P('data')) + (P(),) * 13
    out_specs = (P(('data', 'dap')), P(('data', 'dap')))
    return jax.shard_map(local_step, mesh=mesh, in_specs=in_specs, out_specs=out_specs, check_vma=False)
```

```python
import functools

import jax
import jax.numpy as jnp
from jax import lax
from jax.experimental import pallas as pl
from jax.experimental.pallas import tpu as pltpu
from jax.sharding import PartitionSpec as P

F32 = jnp.float32
BF16 = jnp.bfloat16
EPS = 1e-5
NEG = -1e9
NN = (((1,), (0,)), ((), ()))
NT = (((1,), (1,)), ((), ()))
TN = (((0,), (0,)), ((), ()))
MESH = pl.DeviceIdType.MESH


def mm(a, b, dims=NN):
    return lax.dot_general(a, b, dims, preferred_element_type=F32)


def norm_axis(x, axis):
    mean = jnp.mean(x, axis=axis, keepdims=True)
    centered = x - mean
    var = jnp.mean(centered * centered, axis=axis, keepdims=True)
    return (centered * lax.rsqrt(var + EPS)).astype(BF16)


def one_hot(rows, cols, source):
    r = lax.broadcasted_iota(jnp.int32, (rows, cols), 0)
    c = lax.broadcasted_iota(jnp.int32, (rows, cols), 1)
    return jnp.where(c == source(r), 1.0, 0.0).astype(BF16)


def swap_matrix(a, b):
    return one_hot(a * b, a * b, lambda r: (r % a) * b + r // a)


def softmax_cols(t):
    e = jnp.exp(t - jnp.max(t, axis=0, keepdims=True))
    return (e * (1.0 / jnp.sum(e, axis=0, keepdims=True))).astype(BF16)


EXCHANGES = ('b1', 'm1', 'c', 's1', 'z1', 'e1', 'b2', 'a', 'm2', 'e2', 'z2', 's2')


def step_kernel(cfg, *refs):
    n, sl, rl, S, R, CM, CZ, H, D, HT, DT, OP, HP = cfg
    WM = H * D
    WT = HT * DT
    it = iter(refs)
    (m_ref, z_ref, mask_ref, rmask_ref, wb_hbm, wr_hbm, wro_hbm, wc_hbm, wco_hbm, wpi_hbm, wpo_hbm,
     wsb_hbm, ws_hbm, wso_hbm, web_hbm, we_hbm, weo_hbm) = [next(it) for _ in range(17)]
    m_out, z_out = next(it), next(it)
    wb, wr, wro, wc, wco, wpi, wpo, wsb, ws, wso, web, we, weo = weights = [next(it) for _ in range(13)]
    bias_f, biast_f = next(it), next(it)
    xz, qkvg, pbuf, vbuf = [next(it) for _ in range(4)]
    qvg, kbuf, gbuf = [next(it) for _ in range(3)]
    mrow, mcol, zb, znb = [next(it) for _ in range(4)]
    abuf, cbuf, abuf2, cbuf2, perm, obuf = [next(it) for _ in range(6)]
    mcolmask, seqmask, rmaskt, colmask, norm_ref = [next(it) for _ in range(5)]
    send = {}
    recv = {}
    for name in EXCHANGES:
        send[name] = next(it)
        recv[name] = next(it)
    send_sem, recv_sem, w_sem = next(it), next(it), next(it)
    hbm = [wb_hbm, wr_hbm, wro_hbm, wc_hbm, wco_hbm, wpi_hbm, wpo_hbm, wsb_hbm, ws_hbm, wso_hbm, web_hbm, we_hbm, weo_hbm]
    loads = [pltpu.make_async_copy(src, dst, w_sem.at[i]) for i, (src, dst) in enumerate(zip(hbm, weights))]
    for load in loads:
        load.start()
    (ld_wb, ld_wr, ld_wro, ld_wc, ld_wco, ld_wpi, ld_wpo, ld_wsb, ld_ws, ld_wso, ld_web, ld_we, ld_weo) = loads

    me = lax.axis_index('dap')
    barrier = pltpu.get_barrier_semaphore()

    @pl.loop(1, n)
    def _(k):
        pl.semaphore_signal(barrier, inc=1, device_id={'dap': lax.rem(me + k, n)}, device_id_type=MESH)

    def push(name, scatter):
        x = EXCHANGES.index(name)
        src, dst = send[name], recv[name]

        @pl.loop(1, n)
        def _(k):
            peer = lax.rem(me + k, n)
            pltpu.make_async_remote_copy(
                src_ref=src.at[peer] if scatter else src, dst_ref=dst.at[me], send_sem=send_sem.at[x],
                recv_sem=recv_sem.at[x], device_id={'dap': peer}, device_id_type=MESH).start()
        dst[me] = src[me] if scatter else src[...]

    def bulk_wait(name, sems):
        x = EXCHANGES.index(name)
        bulk = recv[name].at[pl.ds(0, n - 1)]
        pltpu.make_async_copy(bulk, bulk, sems.at[x]).wait()

    def arrived(name):
        bulk_wait(name, recv_sem)

    eye = one_hot(R, R, lambda r: r)

    def pair_norm(zref):
        for i in range(rl):
            xz[:, i * R:(i + 1) * R] = norm_axis(zref[i].astype(F32), 0)

    def bias_block(name, w, heads):
        got = mm(w, xz[...]).astype(BF16).astype(F32)
        send[name][...] = jnp.concatenate([got[:, i * R:(i + 1) * R] for i in range(rl)], axis=0).astype(BF16)
        push(name, False)

    def bias_build(name, heads, padded, dst, transpose):
        group = R // (rl * padded)
        swap = swap_matrix(group * rl, padded)
        rows = group * rl

        @pl.loop(0, n // group)
        def _(g):
            got = mm(swap, recv[name][pl.ds(g * group, group)].reshape(R, R))
            at = pl.ds(pl.multiple_of(g * rows, rows), rows)
            for h in range(heads):
                dst[h, at, :] = got[h * rows:(h + 1) * rows]
        if transpose:
            @pl.loop(0, heads)
            def _(h):
                dst[h] = dst[h].T

    def pair_project(w):
        got = mm(w, xz[...])
        for i in range(rl):
            qkvg[i] = got[:, i * R:(i + 1) * R].astype(BF16)

    def pair_attend(zref, wo, dst):
        scale = DT ** -0.5
        lane_head = lax.broadcasted_iota(jnp.int32, (R, WT), 1) % HT
        sub_head = lax.broadcasted_iota(jnp.int32, (WT, R), 0) % HT

        @pl.loop(0, rl)
        def _(i):
            qt = qkvg[i, 0:WT]
            k = qkvg[i, WT:2 * WT].astype(F32).T
            vt = qkvg[i, 2 * WT:3 * WT].astype(F32)
            for h in range(HT):
                kh = jnp.where(lane_head == h, k, 0.0).astype(BF16)
                t = mm(kh, qt) * scale + biast_f[h]
                t = jnp.where(rmaskt[...] > 0, t, NEG)
                pbuf[h * R:(h + 1) * R, :] = softmax_cols(t)
                vbuf[:, h * R:(h + 1) * R] = jnp.where(sub_head == h, vt, 0.0).astype(BF16)
            o = mm(vbuf[...], pbuf[...])
            gated = (o * jax.nn.sigmoid(qkvg[i, 3 * WT:4 * WT].astype(F32))).astype(BF16)
            dst[i] = (zref[i].astype(F32) + mm(wo, gated)).astype(BF16)

    def pair_send(name):
        for i in range(rl):
            znb[i] = zb[i].astype(F32).T.astype(BF16)
        swap = one_hot(4 * rl * rl, 4 * rl * rl, lambda r: (r % rl) * (4 * rl) + r // rl)
        width = 4 * rl

        @pl.loop(0, n // 4)
        def _(g):
            got = znb[:, pl.ds(pl.multiple_of(g * width, width), width), :].reshape(rl * width, CZ)
            send[name][pl.ds(g * 4, 4)] = mm(swap, got).astype(BF16).reshape(4, rl * rl, CZ)
        push(name, True)

    def pair_receive(name):
        rows = 8 * rl
        swap = one_hot(rows * rl, rows * rl, lambda r: ((r % rows) // rl) * (rl * rl) + (r // rows) * rl + r % rl)

        @pl.loop(0, n // 8)
        def _(g):
            got = mm(swap, recv[name][pl.ds(g * 8, 8)].reshape(rows * rl, CZ)).astype(BF16)
            at = pl.ds(pl.multiple_of(g * rows, rows), rows)
            for i in range(rl):
                znb[i, at, :] = got[i * rows:(i + 1) * rows]
        for i in range(rl):
            zb[i] = znb[i].astype(F32).T.astype(BF16)

    def outer_update(name, left, wo, zref, dst):
        swap = swap_matrix(4 * rl, 16)
        width = 4 * rl

        @pl.loop(0, n // 4)
        def _(g):
            for half in range(OP // 16):
                got = recv[name][pl.ds(g * 4, 4)].reshape(width, OP, S)[:, half * 16:(half + 1) * 16].reshape(width * 16, S)
                perm[half * 16:(half + 1) * 16, pl.ds(pl.multiple_of(g * width, width), width), :] = mm(swap, got).astype(BF16).reshape(16, width, S)

        @pl.loop(0, OP // 2)
        def _(t):
            o = mm(left[...], perm[pl.ds(t * 2, 2)].reshape(2 * R, S), NT).astype(BF16)
            for u in range(2):
                at = pl.ds(pl.multiple_of((t * 2 + u) * OP, OP), OP)
                for i in range(rl):
                    obuf[at, i * R:(i + 1) * R] = o[i * OP:(i + 1) * OP, u * R:(u + 1) * R]
        upd = mm(wo, obuf[...])
        for i in range(rl):
            dst[i] = (zref[i].astype(F32) + upd[:, i * R:(i + 1) * R] * (1.0 / (1e-3 + norm_ref[i:i + 1, :]))).astype(BF16)

    def project(x, w):
        qvg[0:WM] = mm(w[0:WM], x, NT).astype(BF16)
        kbuf[...] = mm(x, w[WM:2 * WM], NT).astype(BF16)
        qvg[WM:3 * WM] = mm(w[2 * WM:4 * WM], x, NT).astype(BF16)

    per_tile = 128 // D

    def attend(lo, size, mask, bias):
        scale = D ** -0.5
        lane_head = lax.broadcasted_iota(jnp.int32, (size, 128), 1) // D
        at = slice(lo, lo + size)
        for h in range(H):
            tile = (h // per_tile) * 128
            kh = jnp.where(lane_head == h % per_tile, kbuf[at, tile:tile + 128].astype(F32), 0.0).astype(BF16)
            t = mm(kh, qvg[tile:tile + 128, at]) * scale
            if bias is not None:
                t = t + bias[h]
            t = jnp.where(mask > 0, t, NEG)
            o = mm(qvg[WM + h * D:WM + (h + 1) * D, at], softmax_cols(t))
            g = qvg[2 * WM + h * D:2 * WM + (h + 1) * D, at].astype(F32)
            gbuf[h * D:(h + 1) * D, at] = (o * jax.nn.sigmoid(g)).astype(BF16)

    def row_attention(src, w, wo, bias, dst):
        @pl.loop(0, sl // 2)
        def _(t):
            xf = src[pl.ds(2 * t, 2)].astype(F32).reshape(2 * R, CM)
            project(norm_axis(xf, 1), w)
            for u in range(2):
                row = seqmask[pl.ds(2 * t + u, 1), :]
                mask = mm(eye, jnp.broadcast_to(row, (R, R)).astype(BF16), NT)
                attend(u * R, R, mask, bias)
            upd = mm(gbuf[...], wo[...], TN)
            dst[pl.ds(2 * t, 2)] = (xf + upd).astype(BF16).reshape(2, R, CM)

    def col_attention(load, w, wo, wp, a_dst, c_dst):
        @pl.loop(0, rl)
        def _(i):
            xf = load(i)
            project(norm_axis(xf, 1), w)
            pick = jnp.where(lax.broadcasted_iota(jnp.int32, (R, R), 0) == me * rl + i, 1.0, 0.0).astype(BF16)
            mask = mm(mcolmask[...], pick)
            attend(0, S, jnp.concatenate([mask, mask], axis=1), None)
            y = (xf + mm(gbuf[...], wo[...], TN)).astype(BF16)
            mcol[i] = y
            x = norm_axis(y.astype(F32), 1)
            half = (mm(wp, x, NT) * colmask[pl.ds(i, 1), :]).astype(BF16)
            at = pl.ds(pl.multiple_of(i * OP, OP), OP)
            a_dst[at, :] = half[0:OP]
            c_dst[at, :] = half[OP:2 * OP]

    maskf = mask_ref[...].astype(F32).astype(BF16)
    mcolmask[...] = maskf
    seqmask[...] = mask_ref[pl.ds(pl.multiple_of(me * sl, sl), sl), :].astype(F32)
    rmaskt[...] = mm(eye, jnp.broadcast_to(rmask_ref[...].astype(F32), (R, R)).astype(BF16), NT)
    pick = jnp.where(lax.broadcasted_iota(jnp.int32, (8, R), 1) == lax.broadcasted_iota(jnp.int32, (8, R), 0) + me * rl, 1.0, 0.0).astype(BF16)
    colmask[...] = mm(pick, maskf, NT)
    norm_ref[...] = mm(colmask[...].astype(BF16), maskf)

    pair_norm(z_ref)
    ld_wb.wait()
    pl.semaphore_wait(barrier, n - 1)
    bias_block('b1', wb[0], HP)
    ld_wr.wait()
    ld_wro.wait()
    arrived('b1')
    bias_build('b1', H, HP, bias_f, True)
    row_attention(m_ref, wr.at[0], wro.at[0], bias_f, mrow)

    swap = one_hot(16 * sl, 16 * sl, lambda r: (r % sl) * 16 + r // sl)

    @pl.loop(0, R // 16)
    def _(g):
        got = mrow[:, pl.ds(pl.multiple_of(g * 16, 16), 16), :].reshape(sl * 16, CM)
        send['m1'][pl.ds(g * (16 // rl), 16 // rl)] = mm(swap, got).astype(BF16).reshape(16 // rl, rl * sl, CM)
    push('m1', True)
    ld_wc.wait()
    ld_wco.wait()
    ld_wpi.wait()
    arrived('m1')

    def load_first(i):
        got = recv['m1'][:, pl.ds(pl.multiple_of((i // 2) * 16, 16), 16), :].astype(F32)
        return jnp.where(i % 2 == 0, got[:, 0:sl], got[:, sl:2 * sl]).reshape(S, CM)

    col_attention(load_first, wc.at[0], wco.at[0], wpi[0], abuf, send['c'])
    push('c', False)
    col_attention(lambda i: mcol[i].astype(F32), wc.at[1], wco.at[1], wpi[1], send['a'], cbuf2)
    push('a', False)

    for p in range(rl // 2):
        pair = [mcol[2 * p + u].astype(F32).reshape(n, sl, CM) for u in range(2)]
        send['m2'][:, p * 2 * sl:(p + 1) * 2 * sl, :] = jnp.concatenate(pair, axis=1).astype(BF16)
    push('m2', True)

    for load in (ld_wpo, ld_wsb, ld_ws, ld_wso, ld_web, ld_we, ld_weo):
        load.wait()
    arrived('c')
    outer_update('c', abuf, wpo[0], z_ref, zb)
    pair_norm(zb)
    bias_block('s1', wsb[0], HT)
    pair_project(ws[0])
    arrived('s1')
    bias_build('s1', HT, HT, biast_f, True)
    pair_attend(zb, wso[0], zb)
    pair_send('z1')
    pair_norm(zb)
    bias_block('e1', web[0], HT)
    arrived('z1')
    pair_receive('z1')
    pair_norm(zb)
    pair_project(we[0])
    arrived('e1')
    bias_build('e1', HT, HT, biast_f, False)
    pair_attend(zb, weo[0], zb)

    pair_norm(zb)
    bias_block('b2', wb[1], HP)
    arrived('a')
    outer_update('a', cbuf2, wpo[1], zb, zb)
    pair_norm(zb)
    bias_block('e2', web[1], HT)
    pair_project(we[1])

    arrived('m2')
    back = one_hot(16 * sl, 16 * sl, lambda r: (r % 16) * sl + r // 16)

    @pl.loop(0, R // 16)
    def _(g):
        got = recv['m2'][pl.ds(g * (16 // rl), 16 // rl)].reshape(16 * sl, CM)
        mrow[:, pl.ds(pl.multiple_of(g * 16, 16), 16), :] = mm(back, got).astype(BF16).reshape(sl, 16, CM)
    arrived('b2')
    bias_build('b2', H, HP, bias_f, False)
    row_attention(mrow, wr.at[1], wro.at[1], bias_f, m_out)

    arrived('e2')
    bias_build('e2', HT, HT, biast_f, True)
    pair_attend(zb, weo[1], zb)
    pair_send('z2')
    pair_norm(zb)
    bias_block('s2', wsb[1], HT)
    arrived('z2')
    pair_receive('z2')
    pair_norm(zb)
    pair_project(ws[1])
    arrived('s2')
    bias_build('s2', HT, HT, biast_f, False)
    pair_attend(zb, wso[1], z_out)
    for name in EXCHANGES:
        bulk_wait(name, send_sem)


def solution(mesh):
    n = mesh.shape['dap']

    def local_step(m, z, mask, rmask, w_row_bias, w_row_in, w_row_out, w_col_in, w_col_out, w_opm_in, w_opm_out, w_ts_bias, w_ts_in, w_ts_out, w_te_bias, w_te_in, w_te_out):
        sl, R, CM = m.shape
        rl, _, CZ = z.shape
        S = mask.shape[0]
        H, D = w_row_in.shape[3:]
        HT, DT = w_ts_in.shape[3:]
        OP = w_opm_in.shape[3]
        HP = -(-H // 8) * 8
        WM, WT = H * D, HT * DT
        zt = z.transpose(0, 2, 1)
        wb = jnp.pad(w_row_bias.transpose(0, 2, 1), ((0, 0), (0, HP - H), (0, 0)))
        wr = w_row_in.transpose(0, 2, 3, 4, 1).reshape(2, 4 * WM, CM)
        wc = w_col_in.transpose(0, 2, 3, 4, 1).reshape(2, 4 * WM, CM)
        wro = w_row_out.reshape(2, WM, CM)
        wco = w_col_out.reshape(2, WM, CM)
        wpi = w_opm_in.transpose(0, 2, 3, 1).reshape(2, 2 * OP, CM)
        wpo = jnp.stack([w_opm_out[0].transpose(2, 1, 0).reshape(CZ, OP * OP), w_opm_out[1].transpose(2, 0, 1).reshape(CZ, OP * OP)])
        wsb = w_ts_bias.transpose(0, 2, 1)
        web = w_te_bias.transpose(0, 2, 1)
        ws = w_ts_in.transpose(0, 2, 4, 3, 1).reshape(2, 4 * WT, CZ)
        we = w_te_in.transpose(0, 2, 4, 3, 1).reshape(2, 4 * WT, CZ)
        wso = w_ts_out.transpose(0, 3, 2, 1).reshape(2, CZ, WT)
        weo = w_te_out.transpose(0, 3, 2, 1).reshape(2, CZ, WT)
        weights = [wb, wr, wro, wc, wco, wpi, wpo, wsb, ws, wso, web, we, weo]

        def vm(shape, dtype=BF16):
            return pltpu.VMEM(shape, dtype)
        scratch = [vm(w.shape) for w in weights]
        scratch += [vm((H, R, R), F32), vm((HT, R, R), F32)]
        scratch += [vm((CZ, rl * R)), vm((rl, 4 * WT, R)), vm((HT * R, R)), vm((WT, HT * R))]
        scratch += [vm((3 * WM, S)), vm((S, WM)), vm((WM, S))]
        scratch += [vm((sl, R, CM)), vm((rl, S, CM)), vm((rl, CZ, R)), vm((rl, R, CZ))]
        scratch += [vm((rl * OP, S))] * 4 + [vm((OP, R, S)), vm((OP * OP, rl * R))]
        scratch += [vm((S, R)), vm((sl, R), F32), vm((R, R), F32), vm((8, S), F32), vm((8, R), F32)]
        bias_row, bias_tri = (rl * HP, R), (rl * HT, R)
        shapes = {'b1': bias_row, 'b2': bias_row, 's1': bias_tri, 'e1': bias_tri, 'e2': bias_tri, 's2': bias_tri,
                  'c': (rl * OP, S), 'a': (rl * OP, S), 'm1': (rl * sl, CM), 'm2': (rl * sl, CM), 'z1': (rl * rl, CZ), 'z2': (rl * rl, CZ)}
        for name in EXCHANGES:
            shape = shapes[name]
            scratch += [vm((n,) + shape if name[0] in 'mz' else shape), vm((n,) + shape)]
        scratch += [pltpu.SemaphoreType.DMA((len(EXCHANGES),)), pltpu.SemaphoreType.DMA((len(EXCHANGES),)), pltpu.SemaphoreType.DMA((len(weights),))]
        cfg = (n, sl, rl, S, R, CM, CZ, H, D, HT, DT, OP, HP)
        vmem = pl.BlockSpec(memory_space=pltpu.VMEM)
        hbm = pl.BlockSpec(memory_space=pl.ANY)
        m_new, z_new = pl.pallas_call(
            functools.partial(step_kernel, cfg),
            out_shape=[jax.ShapeDtypeStruct(m.shape, BF16), jax.ShapeDtypeStruct(zt.shape, BF16)],
            in_specs=[vmem] * 4 + [hbm] * len(weights),
            out_specs=[vmem, vmem],
            scratch_shapes=scratch,
            compiler_params=pltpu.CompilerParams(collective_id=0, has_side_effects=True, vmem_limit_bytes=60 * 2**20),
            name='evoformer',
        )(m, zt, mask, rmask.reshape(1, R), *weights)
        return m_new, z_new.transpose(0, 2, 1)

    in_specs = (P(('data', 'dap')), P(('data', 'dap')), P('data'), P('data')) + (P(),) * 13
    out_specs = (P(('data', 'dap')), P(('data', 'dap')))
    return jax.shard_map(local_step, mesh=mesh, in_specs=in_specs, out_specs=out_specs, check_vma=False)
```

```python
import functools
import math

import jax
import jax.numpy as jnp
from jax import lax
from jax.experimental import pallas as pl
from jax.experimental.pallas import tpu as pltpu
from jax.sharding import PartitionSpec as P

F32 = jnp.float32
BF16 = jnp.bfloat16
EPS = 1e-5
LOG2E = 1.4426950408889634
NEG = -1e9 * LOG2E
NN = (((1,), (0,)), ((), ()))
NT = (((1,), (1,)), ((), ()))
TN = (((0,), (0,)), ((), ()))
MESH = pl.DeviceIdType.MESH


def mm(a, b, dims=NN):
    return lax.dot_general(a, b, dims, preferred_element_type=F32)


def norm_axis(x, axis):
    mean = jnp.mean(x, axis=axis, keepdims=True)
    centered = x - mean
    var = jnp.mean(centered * centered, axis=axis, keepdims=True)
    return (centered * lax.rsqrt(var + EPS)).astype(BF16)


def one_hot(rows, cols, source):
    r = lax.broadcasted_iota(jnp.int32, (rows, cols), 0)
    c = lax.broadcasted_iota(jnp.int32, (rows, cols), 1)
    return jnp.where(c == source(r), 1.0, 0.0).astype(BF16)


def swap_matrix(a, b):
    return one_hot(a * b, a * b, lambda r: (r % a) * b + r // a)


def softmax_cols(t):
    e = jnp.exp2(t - jnp.max(t, axis=0, keepdims=True))
    return (e * (1.0 / jnp.sum(e, axis=0, keepdims=True))).astype(BF16)


EXCHANGES = ('b1', 'm1', 'c', 's1', 'z1', 'e1', 'b2', 'a', 'm2', 'e2', 'z2', 's2')
FLOWS = ('b1', 'm1_0', 'm1_1', 's1', 'z1', 'e1', 'b2', 'm2_0', 'm2_1', 'e2', 'z2', 's2',
         'c_a1', 'c_b1', 'c_a2', 'c_b2', 'c_t', 'a_a1', 'a_b1', 'a_a2', 'a_b2', 'a_t')
STRIDE = 13


def step_kernel(cfg, *refs):
    n, sl, rl, S, R, CM, CZ, H, D, HT, DT, OP, HP = cfg
    WM = H * D
    WT = HT * DT
    side = math.isqrt(n // 2)
    chunk = rl * OP // 2
    it = iter(refs)
    (m_ref, z_ref, mask_ref, rmask_ref, wb_hbm, wr_hbm, wro_hbm, wc_hbm, wco_hbm, wpi_hbm, wpo_hbm,
     wsb_hbm, ws_hbm, wso_hbm, web_hbm, we_hbm, weo_hbm) = [next(it) for _ in range(17)]
    m_out, z_out = next(it), next(it)
    wb, wr, wro, wc, wco, wpi, wpo, wsb, ws, wso, web, we, weo = weights = [next(it) for _ in range(13)]
    bias_f, biast_f = next(it), next(it)
    xz, qkvg, pbuf, vbuf = [next(it) for _ in range(4)]
    qvg, kbuf, gbuf, kmask, vmask = [next(it) for _ in range(5)]
    mrow, mcol, zb, znb = [next(it) for _ in range(4)]
    abuf, cbuf, abuf2, cbuf2, perm, obuf = [next(it) for _ in range(6)]
    mcolmask, seqmask, rmaskt, colmask, norm_ref = [next(it) for _ in range(5)]
    send = {}
    recv = {}
    for name in EXCHANGES:
        send[name] = next(it)
        recv[name] = next(it)
    send_sem, recv_sem, w_sem = next(it), next(it), next(it)
    hbm = [wb_hbm, wr_hbm, wro_hbm, wc_hbm, wco_hbm, wpi_hbm, wpo_hbm, wsb_hbm, ws_hbm, wso_hbm, web_hbm, we_hbm, weo_hbm]
    loads = [pltpu.make_async_copy(src, dst, w_sem.at[i]) for i, (src, dst) in enumerate(zip(hbm, weights))]
    for load in loads:
        load.start()
    (ld_wb, ld_wr, ld_wro, ld_wc, ld_wco, ld_wpi, ld_wpo, ld_wsb, ld_ws, ld_wso, ld_web, ld_we, ld_weo) = loads

    me = lax.axis_index('dap')
    barrier = pltpu.get_barrier_semaphore()

    @pl.loop(1, n)
    def _(k):
        pl.semaphore_signal(barrier, inc=1, device_id={'dap': lax.rem(me + k, n)}, device_id_type=MESH)

    core, px, py = me % 2, (me // 2) % side, me // (2 * side)

    def at(y, x, c):
        return {'dap': ((y % side) * side + x % side) * 2 + c % 2}

    def remote(flow, src, dst, device):
        f = FLOWS.index(flow)
        return pltpu.make_async_remote_copy(src_ref=src, dst_ref=dst, send_sem=send_sem.at[f], recv_sem=recv_sem.at[f], device_id=device, device_id_type=MESH)

    def wait_for(flow, sems, like):
        pltpu.make_async_copy(like, like, sems.at[FLOWS.index(flow)]).wait()

    def push(flow, src, dst, scatter):
        @pl.loop(1, n)
        def _(k):
            peer = lax.rem(me + k * STRIDE, n)
            remote(flow, src.at[peer] if scatter else src, dst.at[me], {'dap': peer}).start()
        dst[me] = src[me] if scatter else src[...]

    def target(flow):
        if flow[0] == 'm':
            return recv[flow[:2]].at[int(flow[3])]
        return recv[flow]

    def like(flow):
        if flow[1] != '_':
            return target(flow).at[pl.ds(0, n - 1)]
        dst, part = recv[flow[0]], flow[2:]
        rows = slice(0, chunk)
        if part == 't':
            return dst.at[:, :, 0]
        if part[1] == '1':
            return dst.at[0, pl.ds(0, side - 1), 0, rows]
        return dst.at[pl.ds(0, side - 1), :, 0, rows]

    def arrived(flow):
        wait_for(flow, recv_sem, like(flow))

    def spread(name, half):
        rows = slice(half * chunk, (half + 1) * chunk)
        dst = recv[name]
        dst[py, px, core, rows] = send[name][rows]
        for d in range(1, side):
            device = at(py, px + d, core) if half == 0 else at(py + d, px, core)
            remote(name + '_' + 'ab'[half] + '1', send[name].at[rows], dst.at[py, px, core, rows], device).start()

    def relay(name, half):
        arrived(name + '_' + 'ab'[half] + '1')
        rows = slice(half * chunk, (half + 1) * chunk)
        dst = recv[name]
        for d in range(1, side):
            if half == 0:
                part, device = dst.at[py, :, core, rows], at(py + d, px, core)
            else:
                part, device = dst.at[:, px, core, rows], at(py, px + d, core)
            remote(name + '_' + 'ab'[half] + '2', part, part, device).start()

    def share(name):
        arrived(name + '_a2')
        arrived(name + '_b2')
        part = recv[name].at[:, :, core]
        remote(name + '_t', part, part, at(py, px, core + 1)).start()

    eye = one_hot(R, R, lambda r: r)

    def pair_norm(zref):
        for i in range(rl):
            xz[:, i * R:(i + 1) * R] = norm_axis(zref[i].astype(F32), 0)

    def bias_block(name, w, heads):
        got = mm(w, xz[...]).astype(BF16).astype(F32)
        got = jnp.concatenate([got[:, i * R:(i + 1) * R] for i in range(rl)], axis=0).astype(BF16)
        padded = w.shape[0]
        if padded != heads:
            pack = one_hot(rl * heads, rl * padded, lambda r: (r // heads) * padded + r % heads)
            got = mm(pack, got).astype(BF16)
        send[name][...] = got
        push(name, send[name], recv[name], False)

    def bias_build(name, heads, group, dst, transpose):
        swap = swap_matrix(group * rl, heads)
        rows = group * rl

        @pl.loop(0, n // group)
        def _(g):
            got = mm(swap, recv[name][pl.ds(g * group, group)].reshape(rows * heads, R)) * LOG2E
            at = pl.ds(pl.multiple_of(g * rows, rows), rows)
            for h in range(heads):
                dst[h, at, :] = got[h * rows:(h + 1) * rows]
        if transpose:
            @pl.loop(0, heads)
            def _(h):
                dst[h] = dst[h].T

    def pair_project(w):
        got = mm(w, xz[...])
        for i in range(rl):
            qkvg[i] = got[:, i * R:(i + 1) * R].astype(BF16)

    def pair_attend(zref, wo, dst):
        scale = DT ** -0.5 * LOG2E

        @pl.loop(0, rl)
        def _(i):
            qt = qkvg[i, 0:WT]
            k = qkvg[i, WT:2 * WT].astype(F32).T.astype(BF16).reshape(R // 16, 16, WT)
            vt = qkvg[i, 2 * WT:3 * WT].reshape(WT // 16, 16, R)
            for h in range(HT):
                kh = (k * kmask[h][None]).reshape(R, WT)
                t = mm(kh, qt) * scale + biast_f[h]
                t = jnp.where(rmaskt[...] > 0, t, NEG)
                pbuf[h * R:(h + 1) * R, :] = softmax_cols(t)
                vbuf[:, h * R:(h + 1) * R] = (vt * vmask[h][None]).reshape(WT, R)
            o = mm(vbuf[...], pbuf[...])
            gated = (o * jax.nn.sigmoid(qkvg[i, 3 * WT:4 * WT].astype(F32))).astype(BF16)
            dst[i] = (zref[i].astype(F32) + mm(wo, gated)).astype(BF16)

    def pair_send(name):
        for i in range(rl):
            znb[i] = zb[i].astype(F32).T.astype(BF16)
        swap = one_hot(4 * rl * rl, 4 * rl * rl, lambda r: (r % rl) * (4 * rl) + r // rl)
        width = 4 * rl

        @pl.loop(0, n // 4)
        def _(g):
            got = znb[:, pl.ds(pl.multiple_of(g * width, width), width), :].reshape(rl * width, CZ)
            send[name][pl.ds(g * 4, 4)] = mm(swap, got).astype(BF16).reshape(4, rl * rl, CZ)
        push(name, send[name], recv[name], True)

    def pair_receive(name):
        rows = 8 * rl
        swap = one_hot(rows * rl, rows * rl, lambda r: ((r % rows) // rl) * (rl * rl) + (r // rows) * rl + r % rl)

        @pl.loop(0, n // 8)
        def _(g):
            got = mm(swap, recv[name][pl.ds(g * 8, 8)].reshape(rows * rl, CZ)).astype(BF16)
            at = pl.ds(pl.multiple_of(g * rows, rows), rows)
            for i in range(rl):
                znb[i, at, :] = got[i * rows:(i + 1) * rows]
        for i in range(rl):
            zb[i] = znb[i].astype(F32).T.astype(BF16)

    def outer_update(name, left, wo, zref, dst):
        swap = swap_matrix(4 * rl, 16)
        width = 4 * rl

        @pl.loop(0, n // 4)
        def _(g):
            for half in range(OP // 16):
                per = side // 2
                got = recv[name][g // per, pl.ds((g % per) * 2, 2)].reshape(width, OP, S)[:, half * 16:(half + 1) * 16].reshape(width * 16, S)
                perm[half * 16:(half + 1) * 16, pl.ds(pl.multiple_of(g * width, width), width), :] = mm(swap, got).astype(BF16).reshape(16, width, S)

        @pl.loop(0, OP // 2)
        def _(t):
            o = mm(left[...], perm[pl.ds(t * 2, 2)].reshape(2 * R, S), NT).astype(BF16)
            for u in range(2):
                at = pl.ds(pl.multiple_of((t * 2 + u) * OP, OP), OP)
                for i in range(rl):
                    obuf[at, i * R:(i + 1) * R] = o[i * OP:(i + 1) * OP, u * R:(u + 1) * R]
        upd = mm(wo, obuf[...])
        for i in range(rl):
            dst[i] = (zref[i].astype(F32) + upd[:, i * R:(i + 1) * R] * (1.0 / (1e-3 + norm_ref[i:i + 1, :]))).astype(BF16)

    def project(x, w, p):
        qvg[p, 0:WM] = mm(w[0:WM], x, NT).astype(BF16)
        kbuf[p] = mm(x, w[WM:2 * WM], NT).astype(BF16)
        qvg[p, WM:3 * WM] = mm(w[2 * WM:4 * WM], x, NT).astype(BF16)

    per_tile = 128 // D
    tile_lane = lax.broadcasted_iota(jnp.int32, (16, 128), 1) // D
    head_mask = [jnp.where(tile_lane == j, 1.0, 0.0).astype(BF16) for j in range(per_tile)]

    def attend(p, lo, size, mask, bias):
        scale = D ** -0.5 * LOG2E
        keys = slice(lo, lo + size)

        def logits(h, q):
            tile = (h // per_tile) * 128
            kt = kbuf[p, keys, tile:tile + 128].reshape(size // 16, 16, 128)
            kh = (kt * head_mask[h % per_tile][None]).reshape(size, 128)
            return mm(kh, qvg[p, tile:tile + 128, q:q + 128])
        blocks = [(h, q) for h in range(H) for q in range(lo, lo + size, 128)]
        ahead = logits(*blocks[0])
        for b, (h, q) in enumerate(blocks):
            t = ahead * scale
            if b + 1 < len(blocks):
                ahead = logits(*blocks[b + 1])
            if bias is not None:
                t = t + bias[h]
            t = jnp.where(mask > 0, t, NEG)
            o = mm(qvg[p, WM + h * D:WM + (h + 1) * D, keys], softmax_cols(t))
            g = qvg[p, 2 * WM + h * D:2 * WM + (h + 1) * D, q:q + 128].astype(F32)
            gbuf[h * D:(h + 1) * D, q:q + 128] = (o * jax.nn.sigmoid(g)).astype(BF16)

    def row_project(src, w):
        @pl.loop(0, sl // 2)
        def _(t):
            xf = src[pl.ds(2 * t, 2)].astype(F32).reshape(2 * R, CM)
            project(norm_axis(xf, 1), w, t)

    def row_attend(src, wo, bias, dst, lo, hi, after):
        @pl.loop(lo, hi)
        def _(t):
            for u in range(2):
                row = seqmask[pl.ds(2 * t + u, 1), :]
                mask = mm(eye, jnp.broadcast_to(row, (R, R)).astype(BF16), NT)
                attend(t, u * R, R, mask, bias)
            xf = src[pl.ds(2 * t, 2)].astype(F32).reshape(2 * R, CM)
            upd = mm(gbuf[...], wo[...], TN)
            dst[pl.ds(2 * t, 2)] = (xf + upd).astype(BF16).reshape(2, R, CM)
            after(t)

    def col_attention(w, wo, wp, a_dst, c_dst, after):
        @pl.loop(0, rl)
        def _(i):
            xf = mcol[i].astype(F32)
            project(norm_axis(xf, 1), w, 0)
            pick = jnp.where(lax.broadcasted_iota(jnp.int32, (R, R), 0) == me * rl + i, 1.0, 0.0).astype(BF16)
            attend(0, 0, S, mm(mcolmask[...], pick), None)
            y = (xf + mm(gbuf[...], wo[...], TN)).astype(BF16)
            mcol[i] = y
            x = norm_axis(y.astype(F32), 1)
            half = (mm(wp, x, NT) * colmask[pl.ds(i, 1), :]).astype(BF16)
            at = pl.ds(pl.multiple_of(i * OP, OP), OP)
            a_dst[at, :] = half[0:OP]
            c_dst[at, :] = half[OP:2 * OP]
            after(i)

    sh = sl // 2
    order = one_hot(S, S, lambda r: ((r % (n * sh)) // sh) * sl + (r // (n * sh)) * sh + r % sh)
    maskf = mm(order, mask_ref[...].astype(F32).astype(BF16)).astype(BF16)
    mcolmask[...] = maskf
    seqmask[...] = mask_ref[pl.ds(pl.multiple_of(me * sl, sl), sl), :].astype(F32)
    rmaskt[...] = mm(eye, jnp.broadcast_to(rmask_ref[...].astype(F32), (R, R)).astype(BF16), NT)
    pick = jnp.where(lax.broadcasted_iota(jnp.int32, (8, R), 1) == lax.broadcasted_iota(jnp.int32, (8, R), 0) + me * rl, 1.0, 0.0).astype(BF16)
    colmask[...] = mm(pick, maskf, NT)
    norm_ref[...] = mm(colmask[...].astype(BF16), maskf)
    for h in range(HT):
        kmask[h] = jnp.where(lax.broadcasted_iota(jnp.int32, (16, WT), 1) % HT == h, 1.0, 0.0).astype(BF16)
        vmask[h] = jnp.where(lax.broadcasted_iota(jnp.int32, (16, R), 0) % HT == h, 1.0, 0.0).astype(BF16)

    pair_norm(z_ref)
    ld_wb.wait()
    pl.semaphore_wait(barrier, n - 1)
    bias_block('b1', wb[0], H)
    ld_wr.wait()
    row_project(m_ref, wr.at[0])
    ld_wro.wait()
    arrived('b1')
    bias_build('b1', H, 8, bias_f, True)

    per = 16 // rl
    split = one_hot(16 * sh, 16 * sh, lambda r: (r % sh) * 16 + r // sh)

    def send_rows(half):
        @pl.loop(0, R // 16)
        def _(g):
            got = mrow[half * sh:(half + 1) * sh, pl.ds(pl.multiple_of(g * 16, 16), 16), :].reshape(sh * 16, CM)
            send['m1'][half, pl.ds(g * per, per)] = mm(split, got).astype(BF16).reshape(per, rl * sh, CM)
        push('m1_%d' % half, send['m1'].at[half], recv['m1'].at[half], True)

    def after_row(t):
        for half in range(2):
            pl.when(t == (half + 1) * (sl // 4) - 1)(functools.partial(send_rows, half))
    row_attend(m_ref, wro.at[0], bias_f, mrow, 0, sl // 2, after_row)

    ld_wc.wait()
    ld_wco.wait()
    ld_wpi.wait()
    join = one_hot(8 * rl * sh, 8 * rl * sh, lambda r: ((r % (8 * sh)) // sh) * (rl * sh) + (r // (8 * sh)) * sh + r % sh)
    for half in range(2):
        arrived('m1_%d' % half)

        @pl.loop(0, n // 8)
        def _(g):
            got = mm(join, recv['m1'][half, pl.ds(g * 8, 8)].reshape(8 * rl * sh, CM)).astype(BF16)
            at = pl.ds(pl.multiple_of(half * n * sh + g * 8 * sh, 8 * sh), 8 * sh)
            for i in range(rl):
                mcol[i, at, :] = got[i * 8 * sh:(i + 1) * 8 * sh]

    def after_first(i):
        pl.when(i == rl // 2 - 1)(lambda: spread('c', 0))
    col_attention(wc.at[0], wco.at[0], wpi[0], abuf, send['c'], after_first)
    spread('c', 1)
    relay('c', 0)

    back = one_hot(8 * rl * sh, 8 * rl * sh, lambda r: ((r % (4 * sh)) // sh) * (8 * sh) + (r // (4 * sh)) * sh + r % sh)

    def send_cols(pair):
        @pl.loop(0, n // 8)
        def _(g):
            got = jnp.concatenate([mcol[2 * pair + u, pl.ds(pl.multiple_of(half * n * sh + g * 8 * sh, 8 * sh), 8 * sh), :] for u in range(2) for half in range(2)], axis=0)
            send['m2'][pair, pl.ds(g * 8, 8)] = mm(back, got).astype(BF16).reshape(8, 4 * sh, CM)
        push('m2_%d' % pair, send['m2'].at[pair], recv['m2'].at[pair], True)

    def after_second(i):
        @pl.when(i == 0)
        def _():
            relay('c', 1)

        @pl.when(i == 1)
        def _():
            spread('a', 0)
            send_cols(0)

        @pl.when(i == 2)
        def _():
            share('c')
    col_attention(wc.at[1], wco.at[1], wpi[1], send['a'], cbuf2, after_second)
    spread('a', 1)
    relay('a', 0)

    for load in (ld_wpo, ld_wsb, ld_ws, ld_wso, ld_web, ld_we, ld_weo):
        load.wait()
    arrived('c_t')
    outer_update('c', abuf, wpo[0], z_ref, zb)
    pair_norm(zb)
    bias_block('s1', wsb[0], HT)
    relay('a', 1)
    send_cols(1)
    pair_project(ws[0])
    arrived('s1')
    bias_build('s1', HT, 4, biast_f, True)
    pair_attend(zb, wso[0], zb)
    pair_send('z1')
    pair_norm(zb)
    bias_block('e1', web[0], HT)
    share('a')
    arrived('m2_0')
    arrived('m2_1')
    unsplit = one_hot(16 * sl, 16 * sl, lambda r: ((r % 4) // 2) * (8 * sl) + ((r % 16) // 4) * (2 * sl) + (r % 2) * sl + r // 16)

    @pl.loop(0, R // 16)
    def _(g):
        got = jnp.concatenate([recv['m2'][pair, pl.ds(g * per, per)].reshape(8 * sl, CM) for pair in range(2)], axis=0)
        mrow[:, pl.ds(pl.multiple_of(g * 16, 16), 16), :] = mm(unsplit, got).astype(BF16).reshape(sl, 16, CM)
    row_project(mrow, wr.at[1])
    arrived('z1')
    pair_receive('z1')
    pair_norm(zb)
    pair_project(we[0])
    arrived('e1')
    bias_build('e1', HT, 4, biast_f, False)
    pair_attend(zb, weo[0], zb)

    pair_norm(zb)
    bias_block('b2', wb[1], H)
    arrived('a_t')
    outer_update('a', cbuf2, wpo[1], zb, zb)
    pair_norm(zb)
    bias_block('e2', web[1], HT)
    pair_project(we[1])
    arrived('b2')
    bias_build('b2', H, 8, bias_f, False)
    row_attend(mrow, wro.at[1], bias_f, m_out, 0, sl // 4, lambda t: None)
    arrived('e2')
    bias_build('e2', HT, 4, biast_f, True)
    pair_attend(zb, weo[1], zb)
    pair_send('z2')
    pair_norm(zb)
    bias_block('s2', wsb[1], HT)
    row_attend(mrow, wro.at[1], bias_f, m_out, sl // 4, sl // 2, lambda t: None)
    arrived('z2')
    pair_receive('z2')
    pair_norm(zb)
    pair_project(ws[1])
    arrived('s2')
    bias_build('s2', HT, 4, biast_f, False)
    pair_attend(zb, wso[1], z_out)
    for flow in FLOWS:
        wait_for(flow, send_sem, like(flow))


def solution(mesh):
    n = mesh.shape['dap']

    def local_step(m, z, mask, rmask, w_row_bias, w_row_in, w_row_out, w_col_in, w_col_out, w_opm_in, w_opm_out, w_ts_bias, w_ts_in, w_ts_out, w_te_bias, w_te_in, w_te_out):
        sl, R, CM = m.shape
        rl, _, CZ = z.shape
        S = mask.shape[0]
        H, D = w_row_in.shape[3:]
        HT, DT = w_ts_in.shape[3:]
        OP = w_opm_in.shape[3]
        HP = -(-H // 8) * 8
        WM, WT = H * D, HT * DT
        zt = z.transpose(0, 2, 1)
        wb = jnp.pad(w_row_bias.transpose(0, 2, 1), ((0, 0), (0, HP - H), (0, 0)))
        wr = w_row_in.transpose(0, 2, 3, 4, 1).reshape(2, 4 * WM, CM)
        wc = w_col_in.transpose(0, 2, 3, 4, 1).reshape(2, 4 * WM, CM)
        wro = w_row_out.reshape(2, WM, CM)
        wco = w_col_out.reshape(2, WM, CM)
        wpi = w_opm_in.transpose(0, 2, 3, 1).reshape(2, 2 * OP, CM)
        wpo = jnp.stack([w_opm_out[0].transpose(2, 1, 0).reshape(CZ, OP * OP), w_opm_out[1].transpose(2, 0, 1).reshape(CZ, OP * OP)])
        wsb = w_ts_bias.transpose(0, 2, 1)
        web = w_te_bias.transpose(0, 2, 1)
        ws = w_ts_in.transpose(0, 2, 4, 3, 1).reshape(2, 4 * WT, CZ)
        we = w_te_in.transpose(0, 2, 4, 3, 1).reshape(2, 4 * WT, CZ)
        wso = w_ts_out.transpose(0, 3, 2, 1).reshape(2, CZ, WT)
        weo = w_te_out.transpose(0, 3, 2, 1).reshape(2, CZ, WT)
        weights = [wb, wr, wro, wc, wco, wpi, wpo, wsb, ws, wso, web, we, weo]

        def vm(shape, dtype=BF16):
            return pltpu.VMEM(shape, dtype)
        scratch = [vm(w.shape) for w in weights]
        scratch += [vm((H, R, R), F32), vm((HT, R, R), F32)]
        scratch += [vm((CZ, rl * R)), vm((rl, 4 * WT, R)), vm((HT * R, R)), vm((WT, HT * R))]
        scratch += [vm((sl // 2, 3 * WM, S)), vm((sl // 2, S, WM)), vm((WM, S)), vm((HT, 16, WT)), vm((HT, 16, R))]
        scratch += [vm((sl, R, CM)), vm((rl, S, CM)), vm((rl, CZ, R)), vm((rl, R, CZ))]
        scratch += [vm((rl * OP, S))] * 4 + [vm((OP, R, S)), vm((OP * OP, rl * R))]
        scratch += [vm((S, R)), vm((sl, R), F32), vm((R, R), F32), vm((8, S), F32), vm((8, R), F32)]
        side = math.isqrt(n // 2)
        bias_row, bias_tri = (rl * H, R), (rl * HT, R)
        shapes = {'b1': bias_row, 'b2': bias_row, 's1': bias_tri, 'e1': bias_tri, 'e2': bias_tri, 's2': bias_tri,
                  'c': (rl * OP, S), 'a': (rl * OP, S), 'm1': (rl * sl // 2, CM), 'm2': (rl * sl // 2, CM), 'z1': (rl * rl, CZ), 'z2': (rl * rl, CZ)}
        for name in EXCHANGES:
            shape = shapes[name]
            if name in 'ac':
                scratch += [vm(shape), vm((side, side, 2) + shape)]
            elif name[0] == 'm':
                scratch += [vm((2, n) + shape), vm((2, n) + shape)]
            else:
                scratch += [vm((n,) + shape if name[0] == 'z' else shape), vm((n,) + shape)]
        scratch += [pltpu.SemaphoreType.DMA((len(FLOWS),)), pltpu.SemaphoreType.DMA((len(FLOWS),)), pltpu.SemaphoreType.DMA((len(weights),))]
        cfg = (n, sl, rl, S, R, CM, CZ, H, D, HT, DT, OP, HP)
        vmem = pl.BlockSpec(memory_space=pltpu.VMEM)
        hbm = pl.BlockSpec(memory_space=pl.ANY)
        m_new, z_new = pl.pallas_call(
            functools.partial(step_kernel, cfg),
            out_shape=[jax.ShapeDtypeStruct(m.shape, BF16), jax.ShapeDtypeStruct(zt.shape, BF16)],
            in_specs=[vmem] * 4 + [hbm] * len(weights),
            out_specs=[vmem, vmem],
            scratch_shapes=scratch,
            compiler_params=pltpu.CompilerParams(collective_id=0, has_side_effects=True, vmem_limit_bytes=60 * 2**20),
            name='evoformer',
        )(m, zt, mask, rmask.reshape(1, R), *weights)
        return m_new, z_new.transpose(0, 2, 1)

    in_specs = (P(('data', 'dap')), P(('data', 'dap')), P('data'), P('data')) + (P(),) * 13
    out_specs = (P(('data', 'dap')), P(('data', 'dap')))
    return jax.shard_map(local_step, mesh=mesh, in_specs=in_specs, out_specs=out_specs, check_vma=False)
```

```python
import functools
import math

import jax
import jax.numpy as jnp
from jax import lax
from jax.experimental import pallas as pl
from jax.experimental.pallas import tpu as pltpu
from jax.sharding import PartitionSpec as P

F32 = jnp.float32
BF16 = jnp.bfloat16
EPS = 1e-5
LOG2E = 1.4426950408889634
NEG = -1e9 * LOG2E
NN = (((1,), (0,)), ((), ()))
NT = (((1,), (1,)), ((), ()))
TN = (((0,), (0,)), ((), ()))
MESH = pl.DeviceIdType.MESH


def mm(a, b, dims=NN):
    return lax.dot_general(a, b, dims, preferred_element_type=F32)


def norm_axis(x, axis):
    mean = jnp.mean(x, axis=axis, keepdims=True)
    centered = x - mean
    var = jnp.mean(centered * centered, axis=axis, keepdims=True)
    return (centered * lax.rsqrt(var + EPS)).astype(BF16)


def one_hot(rows, cols, source):
    r = lax.broadcasted_iota(jnp.int32, (rows, cols), 0)
    c = lax.broadcasted_iota(jnp.int32, (rows, cols), 1)
    return jnp.where(c == source(r), 1.0, 0.0).astype(BF16)


def swap_matrix(a, b):
    return one_hot(a * b, a * b, lambda r: (r % a) * b + r // a)


def softmax_cols(t):
    e = jnp.exp2(t - jnp.max(t, axis=0, keepdims=True))
    return (e * (1.0 / jnp.sum(e, axis=0, keepdims=True))).astype(BF16)


EXCHANGES = ('b1', 'm1', 'c', 's1', 'z1', 'e1', 'b2', 'a', 'm2', 'e2', 'z2', 's2')
FLOWS = ('b1', 'm1_0', 'm1_1', 's1', 'z1', 'e1', 'b2', 'm2_0', 'm2_1', 'e2', 'z2', 's2',
         'c_a1', 'c_b1', 'c_a2', 'c_b2', 'c_t', 'a_a1', 'a_b1', 'a_a2', 'a_b2', 'a_t')
STRIDE = 13


def step_kernel(cfg, *refs):
    n, sl, rl, S, R, CM, CZ, H, D, HT, DT, OP, HP = cfg
    WM = H * D
    WT = HT * DT
    side = math.isqrt(n // 2)
    chunk = rl * OP // 2
    it = iter(refs)
    (m_ref, z_ref, mask_ref, rmask_ref, wb_hbm, wr_hbm, wro_hbm, wc_hbm, wco_hbm, wpi_hbm, wpo_hbm,
     wsb_hbm, ws_hbm, wso_hbm, web_hbm, we_hbm, weo_hbm) = [next(it) for _ in range(17)]
    m_out, z_out = next(it), next(it)
    wb, wr, wro, wc, wco, wpi, wpo, wsb, ws, wso, web, we, weo = weights = [next(it) for _ in range(13)]
    wtmp, wpot, wsot, weot = [next(it) for _ in range(4)]
    bias_f, biast_f = next(it), next(it)
    xz, qkvg, pbuf, vbuf = [next(it) for _ in range(4)]
    qvg, kbuf, gbuf, kmask, vmask = [next(it) for _ in range(5)]
    mrow, mcol, zb, znb = [next(it) for _ in range(4)]
    abuf, cbuf, abuf2, cbuf2, perm, obuf = [next(it) for _ in range(6)]
    mcolmask, seqmask, rmaskt, colmask, norm_ref = [next(it) for _ in range(5)]
    send = {}
    recv = {}
    for name in EXCHANGES:
        send[name] = next(it)
        recv[name] = next(it)
    send_sem, recv_sem, w_sem = next(it), next(it), next(it)
    hbm = [wb_hbm, wr_hbm, wro_hbm, wc_hbm, wco_hbm, wpi_hbm, wpo_hbm, wsb_hbm, ws_hbm, wso_hbm, web_hbm, we_hbm, weo_hbm]
    loads = [pltpu.make_async_copy(src, dst, w_sem.at[i]) for i, (src, dst) in enumerate(zip(hbm, weights))]
    for load in loads:
        load.start()
    (ld_wb, ld_wr, ld_wro, ld_wc, ld_wco, ld_wpi, ld_wpo, ld_wsb, ld_ws, ld_wso, ld_web, ld_we, ld_weo) = loads

    me = lax.axis_index('dap')
    barrier = pltpu.get_barrier_semaphore()

    @pl.loop(1, n)
    def _(k):
        pl.semaphore_signal(barrier, inc=1, device_id={'dap': lax.rem(me + k, n)}, device_id_type=MESH)

    core, px, py = me % 2, (me // 2) % side, me // (2 * side)

    def at(y, x, c):
        return {'dap': ((y % side) * side + x % side) * 2 + c % 2}

    def remote(flow, src, dst, device):
        f = FLOWS.index(flow)
        return pltpu.make_async_remote_copy(src_ref=src, dst_ref=dst, send_sem=send_sem.at[f], recv_sem=recv_sem.at[f], device_id=device, device_id_type=MESH)

    def wait_for(flow, sems, like):
        pltpu.make_async_copy(like, like, sems.at[FLOWS.index(flow)]).wait()

    def push(flow, src, dst, scatter):
        @pl.loop(1, n)
        def _(k):
            peer = lax.rem(me + k * STRIDE, n)
            remote(flow, src.at[peer] if scatter else src, dst.at[me], {'dap': peer}).start()
        dst[me] = src[me] if scatter else src[...]

    def target(flow):
        if flow[0] == 'm':
            return recv[flow[:2]].at[int(flow[3])]
        return recv[flow]

    def like(flow):
        if flow[1] != '_':
            return target(flow).at[pl.ds(0, n - 1)]
        dst, part = recv[flow[0]], flow[2:]
        rows = slice(0, chunk)
        if part == 't':
            return dst.at[:, :, 0]
        if part[1] == '1':
            return dst.at[0, pl.ds(0, side - 1), 0, rows]
        return dst.at[pl.ds(0, side - 1), :, 0, rows]

    def arrived(flow):
        wait_for(flow, recv_sem, like(flow))

    def spread(name, half):
        rows = slice(half * chunk, (half + 1) * chunk)
        dst = recv[name]
        dst[py, px, core, rows] = send[name][rows]
        for d in range(1, side):
            device = at(py, px + d, core) if half == 0 else at(py + d, px, core)
            remote(name + '_' + 'ab'[half] + '1', send[name].at[rows], dst.at[py, px, core, rows], device).start()

    def relay(name, half):
        arrived(name + '_' + 'ab'[half] + '1')
        rows = slice(half * chunk, (half + 1) * chunk)
        dst = recv[name]
        for d in range(1, side):
            if half == 0:
                part, device = dst.at[py, :, core, rows], at(py + d, px, core)
            else:
                part, device = dst.at[:, px, core, rows], at(py, px + d, core)
            remote(name + '_' + 'ab'[half] + '2', part, part, device).start()

    def share(name):
        arrived(name + '_a2')
        arrived(name + '_b2')
        part = recv[name].at[:, :, core]
        remote(name + '_t', part, part, at(py, px, core + 1)).start()

    eye = one_hot(R, R, lambda r: r)

    def pair_norm(zref):
        for i in range(rl):
            xz[:, i * R:(i + 1) * R] = norm_axis(zref[i].astype(F32), 0)

    def bias_block(name, w, heads):
        bias_pack(name, w, heads)
        push(name, send[name], recv[name], False)

    def bias_pack(name, w, heads):
        got = mm(w, xz[...]).astype(BF16).astype(F32)
        got = jnp.concatenate([got[:, i * R:(i + 1) * R] for i in range(rl)], axis=0).astype(BF16)
        padded = w.shape[0]
        if padded != heads:
            pack = one_hot(rl * heads, rl * padded, lambda r: (r // heads) * padded + r % heads)
            got = mm(pack, got).astype(BF16)
        send[name][...] = got

    def bias_build(name, heads, group, dst, transpose):
        swap = swap_matrix(group * rl, heads)
        rows = group * rl

        @pl.loop(0, n // group)
        def _(g):
            got = mm(swap, recv[name][pl.ds(g * group, group)].reshape(rows * heads, R)) * LOG2E
            at = pl.ds(pl.multiple_of(g * rows, rows), rows)
            for h in range(heads):
                dst[h, at, :] = got[h * rows:(h + 1) * rows]
        if transpose:
            @pl.loop(0, heads)
            def _(h):
                dst[h] = dst[h].T

    def pair_project(w):
        got = mm(w, xz[...])
        for i in range(rl):
            qkvg[i] = got[:, i * R:(i + 1) * R].astype(BF16)

    def pair_attend(zref, wo, dst):
        scale = DT ** -0.5 * LOG2E

        @pl.loop(0, rl)
        def _(i):
            qt = qkvg[i, 0:WT]
            k = qkvg[i, WT:2 * WT].astype(F32).T.astype(BF16).reshape(R // 16, 16, WT)
            vt = qkvg[i, 2 * WT:3 * WT].reshape(WT // 16, 16, R)
            for h in range(HT):
                kh = (k * kmask[h][None]).reshape(R, WT)
                t = mm(kh, qt) * scale + biast_f[h]
                t = jnp.where(rmaskt[...] > 0, t, NEG)
                pbuf[h * R:(h + 1) * R, :] = softmax_cols(t)
                vbuf[:, h * R:(h + 1) * R] = (vt * vmask[h][None]).reshape(WT, R)
            o = mm(vbuf[...], pbuf[...])
            gated = (o * jax.nn.sigmoid(qkvg[i, 3 * WT:4 * WT].astype(F32))).astype(BF16)
            dst[i] = (zref[i].astype(F32) + mm(wo, gated)).astype(BF16)

    def pair_send(name):
        for i in range(rl):
            znb[i] = zb[i].astype(F32).T.astype(BF16)
        swap = one_hot(4 * rl * rl, 4 * rl * rl, lambda r: (r % rl) * (4 * rl) + r // rl)
        width = 4 * rl

        @pl.loop(0, n // 4)
        def _(g):
            got = znb[:, pl.ds(pl.multiple_of(g * width, width), width), :].reshape(rl * width, CZ)
            send[name][pl.ds(g * 4, 4)] = mm(swap, got).astype(BF16).reshape(4, rl * rl, CZ)
        push(name, send[name], recv[name], True)

    def pair_receive(name):
        rows = 8 * rl
        swap = one_hot(rows * rl, rows * rl, lambda r: ((r % rows) // rl) * (rl * rl) + (r // rows) * rl + r % rl)

        @pl.loop(0, n // 8)
        def _(g):
            got = mm(swap, recv[name][pl.ds(g * 8, 8)].reshape(rows * rl, CZ)).astype(BF16)
            at = pl.ds(pl.multiple_of(g * rows, rows), rows)
            for i in range(rl):
                znb[i, at, :] = got[i * rows:(i + 1) * rows]
        for i in range(rl):
            zb[i] = znb[i].astype(F32).T.astype(BF16)

    def outer_update(name, left, wo, zref, dst):
        swap = swap_matrix(4 * rl, 16)
        width = 4 * rl

        @pl.loop(0, n // 4)
        def _(g):
            for half in range(OP // 16):
                per = side // 2
                got = recv[name][g // per, pl.ds((g % per) * 2, 2)].reshape(width, OP, S)[:, half * 16:(half + 1) * 16].reshape(width * 16, S)
                perm[half * 16:(half + 1) * 16, pl.ds(pl.multiple_of(g * width, width), width), :] = mm(swap, got).astype(BF16).reshape(16, width, S)

        @pl.loop(0, OP // 2)
        def _(t):
            o = mm(left[...], perm[pl.ds(t * 2, 2)].reshape(2 * R, S), NT).astype(BF16)
            for u in range(2):
                at = pl.ds(pl.multiple_of((t * 2 + u) * OP, OP), OP)
                for i in range(rl):
                    obuf[at, i * R:(i + 1) * R] = o[i * OP:(i + 1) * OP, u * R:(u + 1) * R]
        upd = mm(wo, obuf[...])
        for i in range(rl):
            dst[i] = (zref[i].astype(F32) + upd[:, i * R:(i + 1) * R] * (1.0 / (1e-3 + norm_ref[i:i + 1, :]))).astype(BF16)

    def project(x, w, p):
        qvg[p, 0:WM] = mm(w[0:WM], x, NT).astype(BF16)
        kbuf[p] = mm(x, w[WM:2 * WM], NT).astype(BF16)
        qvg[p, WM:3 * WM] = mm(w[2 * WM:4 * WM], x, NT).astype(BF16)

    per_tile = 128 // D
    tile_lane = lax.broadcasted_iota(jnp.int32, (16, 128), 1) // D
    head_mask = [jnp.where(tile_lane == j, 1.0, 0.0).astype(BF16) for j in range(per_tile)]

    def attend(p, lo, size, mask, bias):
        scale = D ** -0.5 * LOG2E
        keys = slice(lo, lo + size)

        def logits(h, q):
            tile = (h // per_tile) * 128
            kt = kbuf[p, keys, tile:tile + 128].reshape(size // 16, 16, 128)
            kh = (kt * head_mask[h % per_tile][None]).reshape(size, 128)
            return mm(kh, qvg[p, tile:tile + 128, q:q + 128])
        blocks = [(h, q) for h in range(H) for q in range(lo, lo + size, 128)]
        ahead = logits(*blocks[0])
        for b, (h, q) in enumerate(blocks):
            t = ahead * scale
            if b + 1 < len(blocks):
                ahead = logits(*blocks[b + 1])
            if bias is not None:
                t = t + bias[h]
            t = jnp.where(mask > 0, t, NEG)
            o = mm(qvg[p, WM + h * D:WM + (h + 1) * D, keys], softmax_cols(t))
            g = qvg[p, 2 * WM + h * D:2 * WM + (h + 1) * D, q:q + 128].astype(F32)
            gbuf[h * D:(h + 1) * D, q:q + 128] = (o * jax.nn.sigmoid(g)).astype(BF16)

    def row_project(src, w):
        @pl.loop(0, sl // 2)
        def _(t):
            xf = src[pl.ds(2 * t, 2)].astype(F32).reshape(2 * R, CM)
            project(norm_axis(xf, 1), w, t)

    def row_attend(src, wo, bias, dst, lo, hi):
        @pl.loop(lo, hi)
        def _(t):
            for u in range(2):
                row = seqmask[pl.ds(2 * t + u, 1), :]
                mask = mm(eye, jnp.broadcast_to(row, (R, R)).astype(BF16), NT)
                attend(t, u * R, R, mask, bias)
            xf = src[pl.ds(2 * t, 2)].astype(F32).reshape(2 * R, CM)
            upd = mm(gbuf[...], wo[...], TN)
            dst[pl.ds(2 * t, 2)] = (xf + upd).astype(BF16).reshape(2, R, CM)

    def col_attention(load, w, wo, wp, a_dst, c_dst, after):
        @pl.loop(0, rl)
        def _(i):
            xf = load(i)
            project(norm_axis(xf, 1), w, 0)
            pick = jnp.where(lax.broadcasted_iota(jnp.int32, (R, R), 0) == me * rl + i, 1.0, 0.0).astype(BF16)
            attend(0, 0, S, mm(mcolmask[...], pick), None)
            y = (xf + mm(gbuf[...], wo[...], TN)).astype(BF16)
            mcol[i] = y
            x = norm_axis(y.astype(F32), 1)
            half = (mm(wp, x, NT) * colmask[pl.ds(i, 1), :]).astype(BF16)
            at = pl.ds(pl.multiple_of(i * OP, OP), OP)
            a_dst[at, :] = half[0:OP]
            c_dst[at, :] = half[OP:2 * OP]
            after(i)

    maskf = mask_ref[...].astype(F32).astype(BF16)
    mcolmask[...] = maskf
    seqmask[...] = mask_ref[pl.ds(pl.multiple_of(me * sl, sl), sl), :].astype(F32)
    rmaskt[...] = mm(eye, jnp.broadcast_to(rmask_ref[...].astype(F32), (R, R)).astype(BF16), NT)
    pick = jnp.where(lax.broadcasted_iota(jnp.int32, (8, R), 1) == lax.broadcasted_iota(jnp.int32, (8, R), 0) + me * rl, 1.0, 0.0).astype(BF16)
    colmask[...] = mm(pick, maskf, NT)
    norm_ref[...] = mm(colmask[...].astype(BF16), maskf)
    for h in range(HT):
        kmask[h] = jnp.where(lax.broadcasted_iota(jnp.int32, (16, WT), 1) % HT == h, 1.0, 0.0).astype(BF16)
        vmask[h] = jnp.where(lax.broadcasted_iota(jnp.int32, (16, R), 0) % HT == h, 1.0, 0.0).astype(BF16)

    pair_norm(z_ref)
    ld_wb.wait()
    pl.semaphore_wait(barrier, n - 1)
    bias_block('b1', wb[0], H)
    ld_wr.wait()
    row_project(m_ref, wr.at[0])
    ld_wro.wait()
    arrived('b1')
    bias_build('b1', H, 8, bias_f, True)

    row_attend(m_ref, wro.at[0], bias_f, mrow, 0, sl // 2)

    per = 16 // rl
    split = one_hot(16 * sl, 16 * sl, lambda r: (r % sl) * 16 + ((r // (2 * sl)) % per) * rl + (r // (2 * sl * per)) * 2 + (r // sl) % 2)

    @pl.loop(0, R // 16)
    def _(g):
        got = mrow[:, pl.ds(pl.multiple_of(g * 16, 16), 16), :].reshape(sl * 16, CM)
        got = mm(split, got).astype(BF16).reshape(2, per, 2 * sl, CM)
        for pair in range(2):
            send['m1'][pair, pl.ds(g * per, per)] = got[pair]
    for pair in range(2):
        push('m1_%d' % pair, send['m1'].at[pair], recv['m1'].at[pair], True)

    for load in (ld_wpo, ld_wsb, ld_ws, ld_wso, ld_web, ld_we, ld_weo):
        load.wait()
    swap = swap_matrix(16, 16)
    for p in range(OP // 16):
        for q in range(OP // 16):
            got = wpo[0].reshape(OP, OP, CZ)[p * 16:(p + 1) * 16, q * 16:(q + 1) * 16].reshape(256, CZ)
            wtmp[q * 16:(q + 1) * 16, p * 16:(p + 1) * 16, :] = mm(swap, got).astype(BF16).reshape(16, 16, CZ)
    wpot[0] = wtmp[...].reshape(OP * OP, CZ).astype(F32).T.astype(BF16)
    wpot[1] = wpo[1].astype(F32).T.astype(BF16)
    for b in range(2):
        wsot[b] = wso[b].astype(F32).T.astype(BF16)
        weot[b] = weo[b].astype(F32).T.astype(BF16)

    ld_wc.wait()
    ld_wco.wait()
    ld_wpi.wait()
    arrived('m1_0')

    def load_first(i):
        pl.when(i == 2)(lambda: arrived('m1_1'))
        got = recv['m1'][i // 2].astype(F32)
        return jnp.where(i % 2 == 0, got[:, 0:sl], got[:, sl:2 * sl]).reshape(S, CM)

    def after_first(i):
        pl.when(i == rl // 2 - 1)(lambda: spread('c', 0))
    col_attention(load_first, wc.at[0], wco.at[0], wpi[0], abuf, send['c'], after_first)
    spread('c', 1)
    relay('c', 0)

    def send_cols(pair):
        got = [mcol[2 * pair + u].astype(F32).reshape(n, sl, CM) for u in range(2)]
        send['m2'][pair] = jnp.concatenate(got, axis=1).astype(BF16)
        push('m2_%d' % pair, send['m2'].at[pair], recv['m2'].at[pair], True)

    def after_second(i):
        @pl.when(i == 0)
        def _():
            relay('c', 1)

        @pl.when(i == 1)
        def _():
            spread('a', 0)
            send_cols(0)

        @pl.when(i == 2)
        def _():
            share('c')
    col_attention(lambda i: mcol[i].astype(F32), wc.at[1], wco.at[1], wpi[1], send['a'], cbuf2, after_second)
    spread('a', 1)

    arrived('c_t')
    outer_update('c', abuf, wpot[0], z_ref, zb)
    pair_norm(zb)
    bias_block('s1', wsb[0], HT)
    pair_project(ws[0])
    arrived('s1')
    relay('a', 0)
    relay('a', 1)
    bias_build('s1', HT, 4, biast_f, True)
    pair_attend(zb, wsot[0], zb)
    pair_send('z1')
    pair_norm(zb)
    bias_block('e1', web[0], HT)
    share('a')
    arrived('z1')
    pair_receive('z1')
    pair_norm(zb)
    pair_project(we[0])
    arrived('e1')
    send_cols(1)
    bias_build('e1', HT, 4, biast_f, False)
    pair_attend(zb, weot[0], zb)

    pair_norm(zb)
    bias_pack('b2', wb[1], H)
    arrived('a_t')
    outer_update('a', cbuf2, wpot[1], zb, zb)
    pair_norm(zb)
    bias_block('e2', web[1], HT)
    push('b2', send['b2'], recv['b2'], False)
    pair_project(we[1])
    arrived('m2_0')
    arrived('m2_1')
    unsplit = one_hot(16 * sl, 16 * sl, lambda r: ((r % 4) // 2) * (8 * sl) + ((r % 16) // 4) * (2 * sl) + (r % 2) * sl + r // 16)

    @pl.loop(0, R // 16)
    def _(g):
        got = jnp.concatenate([recv['m2'][pair, pl.ds(g * per, per)].reshape(8 * sl, CM) for pair in range(2)], axis=0)
        mrow[:, pl.ds(pl.multiple_of(g * 16, 16), 16), :] = mm(unsplit, got).astype(BF16).reshape(sl, 16, CM)
    row_project(mrow, wr.at[1])
    arrived('e2')
    bias_build('e2', HT, 4, biast_f, True)
    pair_attend(zb, weot[1], zb)
    pair_send('z2')
    pair_norm(zb)
    bias_block('s2', wsb[1], HT)
    arrived('b2')
    bias_build('b2', H, 8, bias_f, False)
    row_attend(mrow, wro.at[1], bias_f, m_out, 0, sl // 2)
    arrived('z2')
    pair_receive('z2')
    pair_norm(zb)
    pair_project(ws[1])
    arrived('s2')
    bias_build('s2', HT, 4, biast_f, False)
    pair_attend(zb, wsot[1], z_out)
    for flow in FLOWS:
        wait_for(flow, send_sem, like(flow))


def solution(mesh):
    n = mesh.shape['dap']

    def local_step(m, z, mask, rmask, w_row_bias, w_row_in, w_row_out, w_col_in, w_col_out, w_opm_in, w_opm_out, w_ts_bias, w_ts_in, w_ts_out, w_te_bias, w_te_in, w_te_out):
        sl, R, CM = m.shape
        rl, _, CZ = z.shape
        S = mask.shape[0]
        H, D = w_row_in.shape[3:]
        HT, DT = w_ts_in.shape[3:]
        OP = w_opm_in.shape[3]
        HP = -(-H // 8) * 8
        WM, WT = H * D, HT * DT
        zt = z.transpose(0, 2, 1)
        wb = jnp.pad(w_row_bias.transpose(0, 2, 1), ((0, 0), (0, HP - H), (0, 0)))
        wr = w_row_in.transpose(0, 2, 3, 4, 1).reshape(2, 4 * WM, CM)
        wc = w_col_in.transpose(0, 2, 3, 4, 1).reshape(2, 4 * WM, CM)
        wro = w_row_out.reshape(2, WM, CM)
        wco = w_col_out.reshape(2, WM, CM)
        wpi = w_opm_in.transpose(0, 2, 3, 1).reshape(2, 2 * OP, CM)
        wpo = w_opm_out.reshape(2, OP * OP, CZ)
        wsb = w_ts_bias.transpose(0, 2, 1)
        web = w_te_bias.transpose(0, 2, 1)
        ws = w_ts_in.transpose(0, 2, 4, 3, 1).reshape(2, 4 * WT, CZ)
        we = w_te_in.transpose(0, 2, 4, 3, 1).reshape(2, 4 * WT, CZ)
        wso = w_ts_out.transpose(0, 2, 1, 3).reshape(2, WT, CZ)
        weo = w_te_out.transpose(0, 2, 1, 3).reshape(2, WT, CZ)
        weights = [wb, wr, wro, wc, wco, wpi, wpo, wsb, ws, wso, web, we, weo]

        def vm(shape, dtype=BF16):
            return pltpu.VMEM(shape, dtype)
        scratch = [vm(w.shape) for w in weights]
        scratch += [vm((OP, OP, CZ)), vm((2, CZ, OP * OP)), vm((2, CZ, WT)), vm((2, CZ, WT))]
        scratch += [vm((H, R, R), F32), vm((HT, R, R), F32)]
        scratch += [vm((CZ, rl * R)), vm((rl, 4 * WT, R)), vm((HT * R, R)), vm((WT, HT * R))]
        scratch += [vm((sl // 2, 3 * WM, S)), vm((sl // 2, S, WM)), vm((WM, S)), vm((HT, 16, WT)), vm((HT, 16, R))]
        scratch += [vm((sl, R, CM)), vm((rl, S, CM)), vm((rl, CZ, R)), vm((rl, R, CZ))]
        scratch += [vm((rl * OP, S))] * 4 + [vm((OP, R, S)), vm((OP * OP, rl * R))]
        scratch += [vm((S, R)), vm((sl, R), F32), vm((R, R), F32), vm((8, S), F32), vm((8, R), F32)]
        side = math.isqrt(n // 2)
        bias_row, bias_tri = (rl * H, R), (rl * HT, R)
        shapes = {'b1': bias_row, 'b2': bias_row, 's1': bias_tri, 'e1': bias_tri, 'e2': bias_tri, 's2': bias_tri,
                  'c': (rl * OP, S), 'a': (rl * OP, S), 'm1': (rl * sl // 2, CM), 'm2': (rl * sl // 2, CM), 'z1': (rl * rl, CZ), 'z2': (rl * rl, CZ)}
        for name in EXCHANGES:
            shape = shapes[name]
            if name in 'ac':
                scratch += [vm(shape), vm((side, side, 2) + shape)]
            elif name[0] == 'm':
                scratch += [vm((2, n) + shape), vm((2, n) + shape)]
            else:
                scratch += [vm((n,) + shape if name[0] == 'z' else shape), vm((n,) + shape)]
        scratch += [pltpu.SemaphoreType.DMA((len(FLOWS),)), pltpu.SemaphoreType.DMA((len(FLOWS),)), pltpu.SemaphoreType.DMA((len(weights),))]
        cfg = (n, sl, rl, S, R, CM, CZ, H, D, HT, DT, OP, HP)
        vmem = pl.BlockSpec(memory_space=pltpu.VMEM)
        hbm = pl.BlockSpec(memory_space=pl.ANY)
        m_new, z_new = pl.pallas_call(
            functools.partial(step_kernel, cfg),
            out_shape=[jax.ShapeDtypeStruct(m.shape, BF16), jax.ShapeDtypeStruct(zt.shape, BF16)],
            in_specs=[vmem] * 4 + [hbm] * len(weights),
            out_specs=[vmem, vmem],
            scratch_shapes=scratch,
            compiler_params=pltpu.CompilerParams(collective_id=0, has_side_effects=True, vmem_limit_bytes=60 * 2**20),
            name='evoformer',
        )(m, zt, mask, rmask.reshape(1, R), *weights)
        return m_new, z_new.transpose(0, 2, 1)

    in_specs = (P(('data', 'dap')), P(('data', 'dap')), P('data'), P('data')) + (P(),) * 13
    out_specs = (P(('data', 'dap')), P(('data', 'dap')))
    return jax.shard_map(local_step, mesh=mesh, in_specs=in_specs, out_specs=out_specs, check_vma=False)
```

```python
import functools
import math

import jax
import jax.numpy as jnp
from jax import lax
from jax.experimental import pallas as pl
from jax.experimental.pallas import tpu as pltpu
from jax.sharding import PartitionSpec as P

F32 = jnp.float32
BF16 = jnp.bfloat16
EPS = 1e-5
LOG2E = 1.4426950408889634
NEG = -1e9 * LOG2E
NN = (((1,), (0,)), ((), ()))
NT = (((1,), (1,)), ((), ()))
TN = (((0,), (0,)), ((), ()))
MESH = pl.DeviceIdType.MESH


def mm(a, b, dims=NN):
    return lax.dot_general(a, b, dims, preferred_element_type=F32)


def norm_axis(x, axis):
    mean = jnp.mean(x, axis=axis, keepdims=True)
    centered = x - mean
    var = jnp.mean(centered * centered, axis=axis, keepdims=True)
    return (centered * lax.rsqrt(var + EPS)).astype(BF16)


def one_hot(rows, cols, source):
    r = lax.broadcasted_iota(jnp.int32, (rows, cols), 0)
    c = lax.broadcasted_iota(jnp.int32, (rows, cols), 1)
    return jnp.where(c == source(r), 1.0, 0.0).astype(BF16)


def swap_matrix(a, b):
    return one_hot(a * b, a * b, lambda r: (r % a) * b + r // a)


def softmax_cols(t):
    e = jnp.exp2(t - jnp.max(t, axis=0, keepdims=True))
    return (e * (1.0 / jnp.sum(e, axis=0, keepdims=True))).astype(BF16)


EXCHANGES = ('b1', 'm1', 'c', 's1', 'z1', 'e1', 'b2', 'a', 'm2', 'e2', 'z2', 's2')
FLOWS = ('b1', 'm1_0', 'm1_1', 's1', 'z1', 'e1', 'b2', 'm2_0', 'm2_1', 'e2', 'z2', 's2',
         'c_a1', 'c_b1', 'c_a2', 'c_b2', 'c_t', 'a_a1', 'a_b1', 'a_a2', 'a_b2', 'a_t')
STRIDE = 13


def step_kernel(cfg, *refs):
    n, sl, rl, S, R, CM, CZ, H, D, HT, DT, OP, HP = cfg
    WM = H * D
    WT = HT * DT
    side = math.isqrt(n // 2)
    chunk = rl * OP // 2
    it = iter(refs)
    (m_ref, z_ref, mask_ref, rmask_ref, wb_hbm, wr_hbm, wro_hbm, wc_hbm, wco_hbm, wpi_hbm, wpo_hbm,
     wsb_hbm, ws_hbm, wso_hbm, web_hbm, we_hbm, weo_hbm) = [next(it) for _ in range(17)]
    m_out, z_out = next(it), next(it)
    wb, wr, wro, wc, wco, wpi, wpo, wsb, ws, wso, web, we, weo = weights = [next(it) for _ in range(13)]
    wtmp, wpot, wsot, weot = [next(it) for _ in range(4)]
    bias_f, biast_f = next(it), next(it)
    xz, qkvg, pbuf, vbuf = [next(it) for _ in range(4)]
    qvg, kbuf, gbuf, kmask, vmask = [next(it) for _ in range(5)]
    mrow, mcol, zb, znb = [next(it) for _ in range(4)]
    abuf, cbuf, abuf2, cbuf2, perm, obuf = [next(it) for _ in range(6)]
    mcolmask, seqmask, rmaskt, colmask, norm_ref = [next(it) for _ in range(5)]
    send = {}
    recv = {}
    for name in EXCHANGES:
        send[name] = next(it)
        recv[name] = next(it)
    send_sem, recv_sem, w_sem = next(it), next(it), next(it)
    hbm = [wb_hbm, wr_hbm, wro_hbm, wc_hbm, wco_hbm, wpi_hbm, wpo_hbm, wsb_hbm, ws_hbm, wso_hbm, web_hbm, we_hbm, weo_hbm]
    loads = [pltpu.make_async_copy(src, dst, w_sem.at[i]) for i, (src, dst) in enumerate(zip(hbm, weights))]
    for load in loads:
        load.start()
    (ld_wb, ld_wr, ld_wro, ld_wc, ld_wco, ld_wpi, ld_wpo, ld_wsb, ld_ws, ld_wso, ld_web, ld_we, ld_weo) = loads

    me = lax.axis_index('dap')
    barrier = pltpu.get_barrier_semaphore()

    @pl.loop(1, n)
    def _(k):
        pl.semaphore_signal(barrier, inc=1, device_id={'dap': lax.rem(me + k, n)}, device_id_type=MESH)

    core, px, py = me % 2, (me // 2) % side, me // (2 * side)

    def at(y, x, c):
        return {'dap': ((y % side) * side + x % side) * 2 + c % 2}

    def remote(flow, src, dst, device):
        f = FLOWS.index(flow)
        return pltpu.make_async_remote_copy(src_ref=src, dst_ref=dst, send_sem=send_sem.at[f], recv_sem=recv_sem.at[f], device_id=device, device_id_type=MESH)

    def wait_for(flow, sems, like):
        pltpu.make_async_copy(like, like, sems.at[FLOWS.index(flow)]).wait()

    def push(flow, src, dst, scatter):
        @pl.loop(1, n)
        def _(k):
            peer = lax.rem(me + k * STRIDE, n)
            remote(flow, src.at[peer] if scatter else src, dst.at[me], {'dap': peer}).start()
        dst[me] = src[me] if scatter else src[...]

    def target(flow):
        if flow[0] == 'm':
            return recv[flow[:2]].at[int(flow[3])]
        return recv[flow]

    def like(flow):
        if flow[1] != '_':
            return target(flow).at[pl.ds(0, n - 1)]
        dst, part = recv[flow[0]], flow[2:]
        rows = slice(0, chunk)
        if part == 't':
            return dst.at[:, :, 0]
        if part[1] == '1':
            return dst.at[0, pl.ds(0, side - 1), 0, rows]
        return dst.at[pl.ds(0, side - 1), :, 0, rows]

    def arrived(flow):
        wait_for(flow, recv_sem, like(flow))

    def spread(name, half):
        rows = slice(half * chunk, (half + 1) * chunk)
        dst = recv[name]
        dst[py, px, core, rows] = send[name][rows]
        for d in range(1, side):
            device = at(py, px + d, core) if half == 0 else at(py + d, px, core)
            remote(name + '_' + 'ab'[half] + '1', send[name].at[rows], dst.at[py, px, core, rows], device).start()

    def relay(name, half):
        arrived(name + '_' + 'ab'[half] + '1')
        rows = slice(half * chunk, (half + 1) * chunk)
        dst = recv[name]
        for d in range(1, side):
            if half == 0:
                part, device = dst.at[py, :, core, rows], at(py + d, px, core)
            else:
                part, device = dst.at[:, px, core, rows], at(py, px + d, core)
            remote(name + '_' + 'ab'[half] + '2', part, part, device).start()

    def share(name):
        arrived(name + '_a2')
        arrived(name + '_b2')
        part = recv[name].at[:, :, core]
        remote(name + '_t', part, part, at(py, px, core + 1)).start()

    eye = one_hot(R, R, lambda r: r)

    def pair_norm(zref):
        for i in range(rl):
            xz[:, i * R:(i + 1) * R] = norm_axis(zref[i].astype(F32), 0)

    def bias_block(name, w, heads):
        bias_pack(name, w, heads)
        push(name, send[name], recv[name], False)

    def bias_pack(name, w, heads):
        got = mm(w, xz[...]).astype(BF16).astype(F32)
        got = jnp.concatenate([got[:, i * R:(i + 1) * R] for i in range(rl)], axis=0).astype(BF16)
        padded = w.shape[0]
        if padded != heads:
            pack = one_hot(rl * heads, rl * padded, lambda r: (r // heads) * padded + r % heads)
            got = mm(pack, got).astype(BF16)
        send[name][...] = got

    def bias_build(name, heads, group, dst, transpose):
        swap = swap_matrix(group * rl, heads)
        rows = group * rl

        for g in range(n // group):
            got = mm(swap, recv[name][g * group:(g + 1) * group].reshape(rows * heads, R)) * LOG2E
            for h in range(heads):
                dst[h, g * rows:(g + 1) * rows, :] = got[h * rows:(h + 1) * rows]
        if transpose:
            for h in range(heads):
                dst[h] = dst[h].T

    def pair_project(w):
        got = mm(w, xz[...])
        for i in range(rl):
            qkvg[i] = got[:, i * R:(i + 1) * R].astype(BF16)

    def pair_attend(zref, wo, dst):
        scale = DT ** -0.5 * LOG2E

        @pl.loop(0, rl)
        def _(i):
            qt = qkvg[i, 0:WT]
            k = qkvg[i, WT:2 * WT].astype(F32).T.astype(BF16).reshape(R // 16, 16, WT)
            vt = qkvg[i, 2 * WT:3 * WT].reshape(WT // 16, 16, R)
            for h in range(HT):
                kh = (k * kmask[h][None]).reshape(R, WT)
                t = mm(kh, qt) * scale + biast_f[h]
                t = jnp.where(rmaskt[...] > 0, t, NEG)
                pbuf[h * R:(h + 1) * R, :] = softmax_cols(t)
                vbuf[:, h * R:(h + 1) * R] = (vt * vmask[h][None]).reshape(WT, R)
            o = mm(vbuf[...], pbuf[...])
            gated = (o * jax.nn.sigmoid(qkvg[i, 3 * WT:4 * WT].astype(F32))).astype(BF16)
            dst[i] = (zref[i].astype(F32) + mm(wo, gated)).astype(BF16)

    def pair_send(name):
        for i in range(rl):
            znb[i] = zb[i].astype(F32).T.astype(BF16)
        swap = one_hot(4 * rl * rl, 4 * rl * rl, lambda r: (r % rl) * (4 * rl) + r // rl)
        width = 4 * rl

        for g in range(n // 4):
            got = znb[:, g * width:(g + 1) * width, :].reshape(rl * width, CZ)
            send[name][g * 4:(g + 1) * 4] = mm(swap, got).astype(BF16).reshape(4, rl * rl, CZ)
        push(name, send[name], recv[name], True)

    def pair_receive(name):
        rows = 8 * rl
        swap = one_hot(rows * rl, rows * rl, lambda r: ((r % rows) // rl) * (rl * rl) + (r // rows) * rl + r % rl)

        for g in range(n // 8):
            got = mm(swap, recv[name][g * 8:(g + 1) * 8].reshape(rows * rl, CZ)).astype(BF16)
            for i in range(rl):
                znb[i, g * rows:(g + 1) * rows, :] = got[i * rows:(i + 1) * rows]
        for i in range(rl):
            zb[i] = znb[i].astype(F32).T.astype(BF16)

    def outer_update(name, left, wo, zref, dst):
        swap = swap_matrix(4 * rl, 16)
        width = 4 * rl

        per_y = side // 2
        for g in range(n // 4):
            for half in range(OP // 16):
                got = recv[name][g // per_y, (g % per_y) * 2:(g % per_y) * 2 + 2].reshape(width, OP, S)[:, half * 16:(half + 1) * 16].reshape(width * 16, S)
                perm[half * 16:(half + 1) * 16, g * width:(g + 1) * width, :] = mm(swap, got).astype(BF16).reshape(16, width, S)
        for t in range(OP // 2):
            o = mm(left[...], perm[t * 2:t * 2 + 2].reshape(2 * R, S), NT).astype(BF16)
            for u in range(2):
                for i in range(rl):
                    obuf[(t * 2 + u) * OP:(t * 2 + u + 1) * OP, i * R:(i + 1) * R] = o[i * OP:(i + 1) * OP, u * R:(u + 1) * R]
        upd = mm(wo, obuf[...])
        for i in range(rl):
            dst[i] = (zref[i].astype(F32) + upd[:, i * R:(i + 1) * R] * (1.0 / (1e-3 + norm_ref[i:i + 1, :]))).astype(BF16)

    def project(x, w, p):
        qvg[p, 0:WM] = mm(w[0:WM], x, NT).astype(BF16)
        kbuf[p] = mm(x, w[WM:2 * WM], NT).astype(BF16)
        qvg[p, WM:3 * WM] = mm(w[2 * WM:4 * WM], x, NT).astype(BF16)

    per_tile = 128 // D
    tile_lane = lax.broadcasted_iota(jnp.int32, (16, 128), 1) // D
    head_mask = [jnp.where(tile_lane == j, 1.0, 0.0).astype(BF16) for j in range(per_tile)]

    def attend(p, lo, size, mask, bias):
        scale = D ** -0.5 * LOG2E
        keys = slice(lo, lo + size)

        def query(h, q):
            j = h % per_tile
            parts = [qvg[p, h * D:(h + 1) * D, q:q + 128]]
            if j:
                parts.insert(0, jnp.zeros((j * D, 128), BF16))
            if j + 1 < per_tile:
                parts.append(jnp.zeros(((per_tile - 1 - j) * D, 128), BF16))
            return jnp.concatenate(parts, axis=0)

        def logits(group):
            h, q = group[0]
            tile = (h // per_tile) * 128
            if len(group) == 1:
                kt = kbuf[p, keys, tile:tile + 128].reshape(size // 16, 16, 128)
                kh = (kt * head_mask[h % per_tile][None]).reshape(size, 128)
                return mm(kh, qvg[p, tile:tile + 128, q:q + 128])
            return mm(kbuf[p, keys, tile:tile + 128], jnp.concatenate([query(h, q) for h, q in group], axis=1))
        blocks = [(h, q) for h in range(H) for q in range(lo, lo + size, 128)]
        step = size // 128
        groups = [blocks[b:b + step] for b in range(0, len(blocks), step)]
        ahead = logits(groups[0])
        for b, group in enumerate(groups):
            now = ahead
            if b + 1 < len(groups):
                ahead = logits(groups[b + 1])
            for u, (h, q) in enumerate(group):
                t = now[:, u * 128:(u + 1) * 128] * scale
                if bias is not None:
                    t = t + bias[h]
                t = jnp.where(mask > 0, t, NEG)
                o = mm(qvg[p, WM + h * D:WM + (h + 1) * D, keys], softmax_cols(t))
                g = qvg[p, 2 * WM + h * D:2 * WM + (h + 1) * D, q:q + 128].astype(F32)
                gbuf[h * D:(h + 1) * D, q:q + 128] = (o * jax.nn.sigmoid(g)).astype(BF16)

    def row_project(src, w):
        @pl.loop(0, sl // 2)
        def _(t):
            xf = src[pl.ds(2 * t, 2)].astype(F32).reshape(2 * R, CM)
            project(norm_axis(xf, 1), w, t)

    def row_attend(src, wo, bias, dst, lo, hi):
        @pl.loop(lo, hi)
        def _(t):
            for u in range(2):
                row = seqmask[pl.ds(2 * t + u, 1), :]
                mask = mm(eye, jnp.broadcast_to(row, (R, R)).astype(BF16), NT)
                attend(t, u * R, R, mask, bias)
            xf = src[pl.ds(2 * t, 2)].astype(F32).reshape(2 * R, CM)
            upd = mm(gbuf[...], wo[...], TN)
            dst[pl.ds(2 * t, 2)] = (xf + upd).astype(BF16).reshape(2, R, CM)

    def col_attention(load, w, wo, wp, a_dst, c_dst, after):
        @pl.loop(0, rl)
        def _(i):
            xf = load(i)
            project(norm_axis(xf, 1), w, 0)
            pick = jnp.where(lax.broadcasted_iota(jnp.int32, (R, R), 0) == me * rl + i, 1.0, 0.0).astype(BF16)
            attend(0, 0, S, mm(mcolmask[...], pick), None)
            y = (xf + mm(gbuf[...], wo[...], TN)).astype(BF16)
            mcol[i] = y
            x = norm_axis(y.astype(F32), 1)
            half = (mm(wp, x, NT) * colmask[pl.ds(i, 1), :]).astype(BF16)
            at = pl.ds(pl.multiple_of(i * OP, OP), OP)
            a_dst[at, :] = half[0:OP]
            c_dst[at, :] = half[OP:2 * OP]
            after(i)

    maskf = mask_ref[...].astype(F32).astype(BF16)
    mcolmask[...] = maskf
    seqmask[...] = mask_ref[pl.ds(pl.multiple_of(me * sl, sl), sl), :].astype(F32)
    rmaskt[...] = mm(eye, jnp.broadcast_to(rmask_ref[...].astype(F32), (R, R)).astype(BF16), NT)
    pick = jnp.where(lax.broadcasted_iota(jnp.int32, (8, R), 1) == lax.broadcasted_iota(jnp.int32, (8, R), 0) + me * rl, 1.0, 0.0).astype(BF16)
    colmask[...] = mm(pick, maskf, NT)
    norm_ref[...] = mm(colmask[...].astype(BF16), maskf)
    for h in range(HT):
        kmask[h] = jnp.where(lax.broadcasted_iota(jnp.int32, (16, WT), 1) % HT == h, 1.0, 0.0).astype(BF16)
        vmask[h] = jnp.where(lax.broadcasted_iota(jnp.int32, (16, R), 0) % HT == h, 1.0, 0.0).astype(BF16)

    pair_norm(z_ref)
    ld_wb.wait()
    pl.semaphore_wait(barrier, n - 1)
    bias_block('b1', wb[0], H)
    ld_wr.wait()
    row_project(m_ref, wr.at[0])
    ld_wro.wait()
    arrived('b1')
    bias_build('b1', H, 8, bias_f, True)

    row_attend(m_ref, wro.at[0], bias_f, mrow, 0, sl // 2)

    per = 16 // rl
    split = one_hot(16 * sl, 16 * sl, lambda r: (r % sl) * 16 + ((r // (2 * sl)) % per) * rl + (r // (2 * sl * per)) * 2 + (r // sl) % 2)

    for g in range(R // 16):
        got = mm(split, mrow[:, g * 16:(g + 1) * 16, :].reshape(sl * 16, CM)).astype(BF16).reshape(2, per, 2 * sl, CM)
        for pair in range(2):
            send['m1'][pair, g * per:(g + 1) * per] = got[pair]
    for pair in range(2):
        push('m1_%d' % pair, send['m1'].at[pair], recv['m1'].at[pair], True)

    for load in (ld_wpo, ld_wsb, ld_ws, ld_wso, ld_web, ld_we, ld_weo):
        load.wait()
    swap = swap_matrix(16, 16)
    for p in range(OP // 16):
        for q in range(OP // 16):
            got = wpo[0].reshape(OP, OP, CZ)[p * 16:(p + 1) * 16, q * 16:(q + 1) * 16].reshape(256, CZ)
            wtmp[q * 16:(q + 1) * 16, p * 16:(p + 1) * 16, :] = mm(swap, got).astype(BF16).reshape(16, 16, CZ)
    wpot[0] = wtmp[...].reshape(OP * OP, CZ).astype(F32).T.astype(BF16)
    wpot[1] = wpo[1].astype(F32).T.astype(BF16)
    for b in range(2):
        wsot[b] = wso[b].astype(F32).T.astype(BF16)
        weot[b] = weo[b].astype(F32).T.astype(BF16)

    ld_wc.wait()
    ld_wco.wait()
    ld_wpi.wait()
    arrived('m1_0')

    def load_first(i):
        pl.when(i == 2)(lambda: arrived('m1_1'))
        got = recv['m1'][i // 2].astype(F32)
        return jnp.where(i % 2 == 0, got[:, 0:sl], got[:, sl:2 * sl]).reshape(S, CM)

    def after_first(i):
        pl.when(i == rl // 2 - 1)(lambda: spread('c', 0))
    col_attention(load_first, wc.at[0], wco.at[0], wpi[0], abuf, send['c'], after_first)
    spread('c', 1)
    relay('c', 0)

    def send_cols(pair):
        got = [mcol[2 * pair + u].astype(F32).reshape(n, sl, CM) for u in range(2)]
        send['m2'][pair] = jnp.concatenate(got, axis=1).astype(BF16)
        push('m2_%d' % pair, send['m2'].at[pair], recv['m2'].at[pair], True)

    def after_second(i):
        @pl.when(i == 0)
        def _():
            relay('c', 1)

        @pl.when(i == 1)
        def _():
            spread('a', 0)
            send_cols(0)

        @pl.when(i == 2)
        def _():
            share('c')
    col_attention(lambda i: mcol[i].astype(F32), wc.at[1], wco.at[1], wpi[1], send['a'], cbuf2, after_second)
    spread('a', 1)

    arrived('c_t')
    outer_update('c', abuf, wpot[0], z_ref, zb)
    pair_norm(zb)
    bias_block('s1', wsb[0], HT)
    pair_project(ws[0])
    arrived('s1')
    relay('a', 0)
    relay('a', 1)
    bias_build('s1', HT, 4, biast_f, True)
    pair_attend(zb, wsot[0], zb)
    pair_send('z1')
    pair_norm(zb)
    bias_block('e1', web[0], HT)
    share('a')
    arrived('z1')
    pair_receive('z1')
    pair_norm(zb)
    pair_project(we[0])
    arrived('e1')
    send_cols(1)
    bias_build('e1', HT, 4, biast_f, False)
    pair_attend(zb, weot[0], zb)

    pair_norm(zb)
    bias_pack('b2', wb[1], H)
    arrived('a_t')
    outer_update('a', cbuf2, wpot[1], zb, zb)
    pair_norm(zb)
    bias_block('e2', web[1], HT)
    push('b2', send['b2'], recv['b2'], False)
    pair_project(we[1])
    arrived('m2_0')
    arrived('m2_1')
    unsplit = one_hot(16 * sl, 16 * sl, lambda r: ((r % 4) // 2) * (8 * sl) + ((r % 16) // 4) * (2 * sl) + (r % 2) * sl + r // 16)

    for g in range(R // 16):
        got = jnp.concatenate([recv['m2'][pair, g * per:(g + 1) * per].reshape(8 * sl, CM) for pair in range(2)], axis=0)
        mrow[:, g * 16:(g + 1) * 16, :] = mm(unsplit, got).astype(BF16).reshape(sl, 16, CM)
    row_project(mrow, wr.at[1])
    arrived('e2')
    bias_build('e2', HT, 4, biast_f, True)
    pair_attend(zb, weot[1], zb)
    pair_send('z2')
    pair_norm(zb)
    bias_block('s2', wsb[1], HT)
    arrived('b2')
    bias_build('b2', H, 8, bias_f, False)
    row_attend(mrow, wro.at[1], bias_f, m_out, 0, sl // 2)
    arrived('z2')
    pair_receive('z2')
    pair_norm(zb)
    pair_project(ws[1])
    arrived('s2')
    bias_build('s2', HT, 4, biast_f, False)
    pair_attend(zb, wsot[1], z_out)
    for flow in FLOWS:
        wait_for(flow, send_sem, like(flow))


def solution(mesh):
    n = mesh.shape['dap']

    def local_step(m, z, mask, rmask, w_row_bias, w_row_in, w_row_out, w_col_in, w_col_out, w_opm_in, w_opm_out, w_ts_bias, w_ts_in, w_ts_out, w_te_bias, w_te_in, w_te_out):
        sl, R, CM = m.shape
        rl, _, CZ = z.shape
        S = mask.shape[0]
        H, D = w_row_in.shape[3:]
        HT, DT = w_ts_in.shape[3:]
        OP = w_opm_in.shape[3]
        HP = -(-H // 8) * 8
        WM, WT = H * D, HT * DT
        zt = z.transpose(0, 2, 1)
        wb = jnp.pad(w_row_bias.transpose(0, 2, 1), ((0, 0), (0, HP - H), (0, 0)))
        wr = w_row_in.transpose(0, 2, 3, 4, 1).reshape(2, 4 * WM, CM)
        wc = w_col_in.transpose(0, 2, 3, 4, 1).reshape(2, 4 * WM, CM)
        wro = w_row_out.reshape(2, WM, CM)
        wco = w_col_out.reshape(2, WM, CM)
        wpi = w_opm_in.transpose(0, 2, 3, 1).reshape(2, 2 * OP, CM)
        wpo = w_opm_out.reshape(2, OP * OP, CZ)
        wsb = w_ts_bias.transpose(0, 2, 1)
        web = w_te_bias.transpose(0, 2, 1)
        ws = w_ts_in.transpose(0, 2, 4, 3, 1).reshape(2, 4 * WT, CZ)
        we = w_te_in.transpose(0, 2, 4, 3, 1).reshape(2, 4 * WT, CZ)
        wso = w_ts_out.transpose(0, 2, 1, 3).reshape(2, WT, CZ)
        weo = w_te_out.transpose(0, 2, 1, 3).reshape(2, WT, CZ)
        weights = [wb, wr, wro, wc, wco, wpi, wpo, wsb, ws, wso, web, we, weo]

        def vm(shape, dtype=BF16):
            return pltpu.VMEM(shape, dtype)
        scratch = [vm(w.shape) for w in weights]
        scratch += [vm((OP, OP, CZ)), vm((2, CZ, OP * OP)), vm((2, CZ, WT)), vm((2, CZ, WT))]
        scratch += [vm((H, R, R), F32), vm((HT, R, R), F32)]
        scratch += [vm((CZ, rl * R)), vm((rl, 4 * WT, R)), vm((HT * R, R)), vm((WT, HT * R))]
        scratch += [vm((sl // 2, 3 * WM, S)), vm((sl // 2, S, WM)), vm((WM, S)), vm((HT, 16, WT)), vm((HT, 16, R))]
        scratch += [vm((sl, R, CM)), vm((rl, S, CM)), vm((rl, CZ, R)), vm((rl, R, CZ))]
        scratch += [vm((rl * OP, S))] * 4 + [vm((OP, R, S)), vm((OP * OP, rl * R))]
        scratch += [vm((S, R)), vm((sl, R), F32), vm((R, R), F32), vm((8, S), F32), vm((8, R), F32)]
        side = math.isqrt(n // 2)
        bias_row, bias_tri = (rl * H, R), (rl * HT, R)
        shapes = {'b1': bias_row, 'b2': bias_row, 's1': bias_tri, 'e1': bias_tri, 'e2': bias_tri, 's2': bias_tri,
                  'c': (rl * OP, S), 'a': (rl * OP, S), 'm1': (rl * sl // 2, CM), 'm2': (rl * sl // 2, CM), 'z1': (rl * rl, CZ), 'z2': (rl * rl, CZ)}
        for name in EXCHANGES:
            shape = shapes[name]
            if name in 'ac':
                scratch += [vm(shape), vm((side, side, 2) + shape)]
            elif name[0] == 'm':
                scratch += [vm((2, n) + shape), vm((2, n) + shape)]
            else:
                scratch += [vm((n,) + shape if name[0] == 'z' else shape), vm((n,) + shape)]
        scratch += [pltpu.SemaphoreType.DMA((len(FLOWS),)), pltpu.SemaphoreType.DMA((len(FLOWS),)), pltpu.SemaphoreType.DMA((len(weights),))]
        cfg = (n, sl, rl, S, R, CM, CZ, H, D, HT, DT, OP, HP)
        vmem = pl.BlockSpec(memory_space=pltpu.VMEM)
        hbm = pl.BlockSpec(memory_space=pl.ANY)
        m_new, z_new = pl.pallas_call(
            functools.partial(step_kernel, cfg),
            out_shape=[jax.ShapeDtypeStruct(m.shape, BF16), jax.ShapeDtypeStruct(zt.shape, BF16)],
            in_specs=[vmem] * 4 + [hbm] * len(weights),
            out_specs=[vmem, vmem],
            scratch_shapes=scratch,
            compiler_params=pltpu.CompilerParams(collective_id=0, has_side_effects=True, vmem_limit_bytes=60 * 2**20),
            name='evoformer',
        )(m, zt, mask, rmask.reshape(1, R), *weights)
        return m_new, z_new.transpose(0, 2, 1)

    in_specs = (P(('data', 'dap')), P(('data', 'dap')), P('data'), P('data')) + (P(),) * 13
    out_specs = (P(('data', 'dap')), P(('data', 'dap')))
    return jax.shard_map(local_step, mesh=mesh, in_specs=in_specs, out_specs=out_specs, check_vma=False)
```

```python
import functools
import math

import jax
import jax.numpy as jnp
from jax import lax
from jax.experimental import pallas as pl
from jax.experimental.pallas import tpu as pltpu
from jax.sharding import PartitionSpec as P

F32 = jnp.float32
BF16 = jnp.bfloat16
EPS = 1e-5
LOG2E = 1.4426950408889634
NEG = -1e9 * LOG2E
NN = (((1,), (0,)), ((), ()))
NT = (((1,), (1,)), ((), ()))
TN = (((0,), (0,)), ((), ()))
MESH = pl.DeviceIdType.MESH


def mm(a, b, dims=NN):
    return lax.dot_general(a, b, dims, preferred_element_type=F32)


def norm_axis(x, axis):
    mean = jnp.mean(x, axis=axis, keepdims=True)
    centered = x - mean
    var = jnp.mean(centered * centered, axis=axis, keepdims=True)
    return (centered * lax.rsqrt(var + EPS)).astype(BF16)


def one_hot(rows, cols, source):
    r = lax.broadcasted_iota(jnp.int32, (rows, cols), 0)
    c = lax.broadcasted_iota(jnp.int32, (rows, cols), 1)
    return jnp.where(c == source(r), 1.0, 0.0).astype(BF16)


def swap_matrix(a, b):
    return one_hot(a * b, a * b, lambda r: (r % a) * b + r // a)


def softmax_cols(t):
    e = jnp.exp2(t - jnp.max(t, axis=0, keepdims=True))
    return (e * (1.0 / jnp.sum(e, axis=0, keepdims=True))).astype(BF16)


EXCHANGES = ('b1', 'm1', 'c', 's1', 'z1', 'e1', 'b2', 'a', 'm2', 'e2', 'z2', 's2')
FLOWS = ('b1', 'm1_0', 'm1_1', 's1', 'z1', 'e1', 'b2', 'm2_0', 'm2_1', 'e2', 'z2', 's2',
         'c_a1', 'c_b1', 'c_a2', 'c_b2', 'c_t', 'a_a1', 'a_b1', 'a_a2', 'a_b2', 'a_t')
STRIDE = 13


def step_kernel(cfg, *refs):
    n, sl, rl, S, R, CM, CZ, H, D, HT, DT, OP, HP = cfg
    WM = H * D
    WT = HT * DT
    DP = -(-DT // 16) * 16
    WP = HT * DP
    side = math.isqrt(n // 2)
    chunk = rl * OP // 2
    it = iter(refs)
    (m_ref, z_ref, mask_ref, rmask_ref, wb_hbm, wr_hbm, wro_hbm, wc_hbm, wco_hbm, wpi_hbm, wpo_hbm,
     wsb_hbm, ws_hbm, wso_hbm, web_hbm, we_hbm, weo_hbm) = [next(it) for _ in range(17)]
    m_out, z_out = next(it), next(it)
    wb, wr, wro, wc, wco, wpi, wpo, wsb, ws, wso, web, we, weo = weights = [next(it) for _ in range(13)]
    wtmp, wpot, wsot, weot = [next(it) for _ in range(4)]
    bias_f, biast_f = next(it), next(it)
    xz, qkvg, gpair, wsp, wep = [next(it) for _ in range(5)]
    qvg, kbuf, gbuf = [next(it) for _ in range(3)]
    mrow, mcol, zb, znb = [next(it) for _ in range(4)]
    abuf, cbuf, abuf2, cbuf2, perm, obuf = [next(it) for _ in range(6)]
    mcolmask, seqmask, rmaskt, colmask, norm_ref = [next(it) for _ in range(5)]
    send = {}
    recv = {}
    for name in EXCHANGES:
        send[name] = next(it)
        recv[name] = next(it)
    send_sem, recv_sem, w_sem = next(it), next(it), next(it)
    hbm = [wb_hbm, wr_hbm, wro_hbm, wc_hbm, wco_hbm, wpi_hbm, wpo_hbm, wsb_hbm, ws_hbm, wso_hbm, web_hbm, we_hbm, weo_hbm]
    loads = [pltpu.make_async_copy(src, dst, w_sem.at[i]) for i, (src, dst) in enumerate(zip(hbm, weights))]
    for load in loads:
        load.start()
    (ld_wb, ld_wr, ld_wro, ld_wc, ld_wco, ld_wpi, ld_wpo, ld_wsb, ld_ws, ld_wso, ld_web, ld_we, ld_weo) = loads

    me = lax.axis_index('dap')
    barrier = pltpu.get_barrier_semaphore()

    @pl.loop(1, n)
    def _(k):
        pl.semaphore_signal(barrier, inc=1, device_id={'dap': lax.rem(me + k, n)}, device_id_type=MESH)

    core, px, py = me % 2, (me // 2) % side, me // (2 * side)

    def at(y, x, c):
        return {'dap': ((y % side) * side + x % side) * 2 + c % 2}

    def remote(flow, src, dst, device):
        f = FLOWS.index(flow)
        return pltpu.make_async_remote_copy(src_ref=src, dst_ref=dst, send_sem=send_sem.at[f], recv_sem=recv_sem.at[f], device_id=device, device_id_type=MESH)

    def wait_for(flow, sems, like):
        pltpu.make_async_copy(like, like, sems.at[FLOWS.index(flow)]).wait()

    def push(flow, src, dst, scatter):
        @pl.loop(1, n)
        def _(k):
            peer = lax.rem(me + k * STRIDE, n)
            remote(flow, src.at[peer] if scatter else src, dst.at[me], {'dap': peer}).start()
        dst[me] = src[me] if scatter else src[...]

    def target(flow):
        if flow[0] == 'm':
            return recv[flow[:2]].at[int(flow[3])]
        return recv[flow]

    def like(flow):
        if flow[1] != '_':
            return target(flow).at[pl.ds(0, n - 1)]
        dst, part = recv[flow[0]], flow[2:]
        rows = slice(0, chunk)
        if part == 't':
            return dst.at[:, :, 0]
        if part[1] == '1':
            return dst.at[0, pl.ds(0, side - 1), 0, rows]
        return dst.at[pl.ds(0, side - 1), :, 0, rows]

    def arrived(flow):
        wait_for(flow, recv_sem, like(flow))

    def spread(name, half):
        rows = slice(half * chunk, (half + 1) * chunk)
        dst = recv[name]
        dst[py, px, core, rows] = send[name][rows]
        for d in range(1, side):
            device = at(py, px + d, core) if half == 0 else at(py + d, px, core)
            remote(name + '_' + 'ab'[half] + '1', send[name].at[rows], dst.at[py, px, core, rows], device).start()

    def relay(name, half):
        arrived(name + '_' + 'ab'[half] + '1')
        rows = slice(half * chunk, (half + 1) * chunk)
        dst = recv[name]
        for d in range(1, side):
            if half == 0:
                part, device = dst.at[py, :, core, rows], at(py + d, px, core)
            else:
                part, device = dst.at[:, px, core, rows], at(py, px + d, core)
            remote(name + '_' + 'ab'[half] + '2', part, part, device).start()

    def share(name):
        arrived(name + '_a2')
        arrived(name + '_b2')
        part = recv[name].at[:, :, core]
        remote(name + '_t', part, part, at(py, px, core + 1)).start()

    eye = one_hot(R, R, lambda r: r)

    def pair_norm(zref):
        for i in range(rl):
            xz[:, i * R:(i + 1) * R] = norm_axis(zref[i].astype(F32), 0)

    def bias_block(name, w, heads):
        bias_pack(name, w, heads)
        push(name, send[name], recv[name], False)

    def bias_pack(name, w, heads):
        got = mm(w, xz[...]).astype(BF16).astype(F32)
        got = jnp.concatenate([got[:, i * R:(i + 1) * R] for i in range(rl)], axis=0).astype(BF16)
        padded = w.shape[0]
        if padded != heads:
            pack = one_hot(rl * heads, rl * padded, lambda r: (r // heads) * padded + r % heads)
            got = mm(pack, got).astype(BF16)
        send[name][...] = got

    def bias_build(name, heads, group, dst, transpose):
        swap = swap_matrix(group * rl, heads)
        rows = group * rl

        for g in range(n // group):
            got = mm(swap, recv[name][g * group:(g + 1) * group].reshape(rows * heads, R)) * LOG2E
            for h in range(heads):
                dst[h, g * rows:(g + 1) * rows, :] = got[h * rows:(h + 1) * rows]
        if transpose:
            for h in range(heads):
                dst[h] = dst[h].T

    def pair_project(w):
        got = mm(w, xz[...])
        for i in range(rl):
            qkvg[i] = got[:, i * R:(i + 1) * R].astype(BF16)

    def pair_attend(zref, wo, dst):
        scale = DT ** -0.5 * LOG2E

        @pl.loop(0, rl)
        def _(i):
            def part(f, h):
                return qkvg[i, f * WP + h * DP:f * WP + (h + 1) * DP]

            def logits(h):
                return mm(part(1, h).astype(F32).T.astype(BF16), part(0, h))
            ahead = logits(0)
            for h in range(HT):
                t = ahead * scale + biast_f[h]
                if h + 1 < HT:
                    ahead = logits(h + 1)
                t = jnp.where(rmaskt[...] > 0, t, NEG)
                o = mm(part(2, h), softmax_cols(t))
                gpair[h * DP:(h + 1) * DP, :] = (o * jax.nn.sigmoid(part(3, h).astype(F32))).astype(BF16)
            dst[i] = (zref[i].astype(F32) + mm(wo, gpair[...])).astype(BF16)

    def pair_send(name):
        for i in range(rl):
            znb[i] = zb[i].astype(F32).T.astype(BF16)
        swap = one_hot(4 * rl * rl, 4 * rl * rl, lambda r: (r % rl) * (4 * rl) + r // rl)
        width = 4 * rl

        for g in range(n // 4):
            got = znb[:, g * width:(g + 1) * width, :].reshape(rl * width, CZ)
            send[name][g * 4:(g + 1) * 4] = mm(swap, got).astype(BF16).reshape(4, rl * rl, CZ)
        push(name, send[name], recv[name], True)

    def pair_receive(name):
        rows = 8 * rl
        swap = one_hot(rows * rl, rows * rl, lambda r: ((r % rows) // rl) * (rl * rl) + (r // rows) * rl + r % rl)

        for g in range(n // 8):
            got = mm(swap, recv[name][g * 8:(g + 1) * 8].reshape(rows * rl, CZ)).astype(BF16)
            for i in range(rl):
                znb[i, g * rows:(g + 1) * rows, :] = got[i * rows:(i + 1) * rows]
        for i in range(rl):
            zb[i] = znb[i].astype(F32).T.astype(BF16)

    def outer_update(name, left, wo, zref, dst):
        swap = swap_matrix(4 * rl, 16)
        width = 4 * rl

        per_y = side // 2
        for g in range(n // 4):
            for half in range(OP // 16):
                got = recv[name][g // per_y, (g % per_y) * 2:(g % per_y) * 2 + 2].reshape(width, OP, S)[:, half * 16:(half + 1) * 16].reshape(width * 16, S)
                perm[half * 16:(half + 1) * 16, g * width:(g + 1) * width, :] = mm(swap, got).astype(BF16).reshape(16, width, S)
        for t in range(OP // 2):
            o = mm(left[...], perm[t * 2:t * 2 + 2].reshape(2 * R, S), NT).astype(BF16)
            for u in range(2):
                for i in range(rl):
                    obuf[(t * 2 + u) * OP:(t * 2 + u + 1) * OP, i * R:(i + 1) * R] = o[i * OP:(i + 1) * OP, u * R:(u + 1) * R]
        upd = mm(wo, obuf[...])
        for i in range(rl):
            dst[i] = (zref[i].astype(F32) + upd[:, i * R:(i + 1) * R] * (1.0 / (1e-3 + norm_ref[i:i + 1, :]))).astype(BF16)

    def project(x, w, p):
        qvg[p, 0:WM] = mm(w[0:WM], x, NT).astype(BF16)
        kbuf[p] = mm(x, w[WM:2 * WM], NT).astype(BF16)
        qvg[p, WM:3 * WM] = mm(w[2 * WM:4 * WM], x, NT).astype(BF16)

    per_tile = 128 // D
    tile_lane = lax.broadcasted_iota(jnp.int32, (16, 128), 1) // D
    head_mask = [jnp.where(tile_lane == j, 1.0, 0.0).astype(BF16) for j in range(per_tile)]

    def attend(p, lo, size, mask, bias):
        scale = D ** -0.5 * LOG2E
        keys = slice(lo, lo + size)

        def query(h, q):
            j = h % per_tile
            parts = [qvg[p, h * D:(h + 1) * D, q:q + 128]]
            if j:
                parts.insert(0, jnp.zeros((j * D, 128), BF16))
            if j + 1 < per_tile:
                parts.append(jnp.zeros(((per_tile - 1 - j) * D, 128), BF16))
            return jnp.concatenate(parts, axis=0)

        def logits(group):
            h, q = group[0]
            tile = (h // per_tile) * 128
            if len(group) == 1:
                kt = kbuf[p, keys, tile:tile + 128].reshape(size // 16, 16, 128)
                kh = (kt * head_mask[h % per_tile][None]).reshape(size, 128)
                return mm(kh, qvg[p, tile:tile + 128, q:q + 128])
            return mm(kbuf[p, keys, tile:tile + 128], jnp.concatenate([query(h, q) for h, q in group], axis=1))
        blocks = [(h, q) for h in range(H) for q in range(lo, lo + size, 128)]
        step = size // 128
        groups = [blocks[b:b + step] for b in range(0, len(blocks), step)]
        ahead = logits(groups[0])
        for b, group in enumerate(groups):
            now = ahead
            if b + 1 < len(groups):
                ahead = logits(groups[b + 1])
            for u, (h, q) in enumerate(group):
                t = now[:, u * 128:(u + 1) * 128] * scale
                if bias is not None:
                    t = t + bias[h]
                t = jnp.where(mask > 0, t, NEG)
                o = mm(qvg[p, WM + h * D:WM + (h + 1) * D, keys], softmax_cols(t))
                g = qvg[p, 2 * WM + h * D:2 * WM + (h + 1) * D, q:q + 128].astype(F32)
                gbuf[h * D:(h + 1) * D, q:q + 128] = (o * jax.nn.sigmoid(g)).astype(BF16)

    def row_project(src, w):
        @pl.loop(0, sl // 2)
        def _(t):
            xf = src[pl.ds(2 * t, 2)].astype(F32).reshape(2 * R, CM)
            project(norm_axis(xf, 1), w, t)

    def row_attend(src, wo, bias, dst, lo, hi):
        @pl.loop(lo, hi)
        def _(t):
            for u in range(2):
                row = seqmask[pl.ds(2 * t + u, 1), :]
                mask = mm(eye, jnp.broadcast_to(row, (R, R)).astype(BF16), NT)
                attend(t, u * R, R, mask, bias)
            xf = src[pl.ds(2 * t, 2)].astype(F32).reshape(2 * R, CM)
            upd = mm(gbuf[...], wo[...], TN)
            dst[pl.ds(2 * t, 2)] = (xf + upd).astype(BF16).reshape(2, R, CM)

    def col_attention(load, w, wo, wp, a_dst, c_dst, after):
        @pl.loop(0, rl)
        def _(i):
            xf = load(i)
            project(norm_axis(xf, 1), w, 0)
            pick = jnp.where(lax.broadcasted_iota(jnp.int32, (R, R), 0) == me * rl + i, 1.0, 0.0).astype(BF16)
            attend(0, 0, S, mm(mcolmask[...], pick), None)
            y = (xf + mm(gbuf[...], wo[...], TN)).astype(BF16)
            mcol[i] = y
            x = norm_axis(y.astype(F32), 1)
            half = (mm(wp, x, NT) * colmask[pl.ds(i, 1), :]).astype(BF16)
            at = pl.ds(pl.multiple_of(i * OP, OP), OP)
            a_dst[at, :] = half[0:OP]
            c_dst[at, :] = half[OP:2 * OP]
            after(i)

    maskf = mask_ref[...].astype(F32).astype(BF16)
    mcolmask[...] = maskf
    seqmask[...] = mask_ref[pl.ds(pl.multiple_of(me * sl, sl), sl), :].astype(F32)
    rmaskt[...] = mm(eye, jnp.broadcast_to(rmask_ref[...].astype(F32), (R, R)).astype(BF16), NT)
    pick = jnp.where(lax.broadcasted_iota(jnp.int32, (8, R), 1) == lax.broadcasted_iota(jnp.int32, (8, R), 0) + me * rl, 1.0, 0.0).astype(BF16)
    colmask[...] = mm(pick, maskf, NT)
    norm_ref[...] = mm(colmask[...].astype(BF16), maskf)

    pair_norm(z_ref)
    ld_wb.wait()
    pl.semaphore_wait(barrier, n - 1)
    bias_block('b1', wb[0], H)
    ld_wr.wait()
    row_project(m_ref, wr.at[0])
    ld_wro.wait()
    ld_wpo.wait()
    swap = swap_matrix(16, 16)
    for p in range(OP // 16):
        for q in range(OP // 16):
            got = wpo[0].reshape(OP, OP, CZ)[p * 16:(p + 1) * 16, q * 16:(q + 1) * 16].reshape(256, CZ)
            wtmp[q * 16:(q + 1) * 16, p * 16:(p + 1) * 16, :] = mm(swap, got).astype(BF16).reshape(16, 16, CZ)
    wpot[0] = wtmp[...].reshape(OP * OP, CZ).astype(F32).T.astype(BF16)
    wpot[1] = wpo[1].astype(F32).T.astype(BF16)
    arrived('b1')
    bias_build('b1', H, 8, bias_f, True)

    row_attend(m_ref, wro.at[0], bias_f, mrow, 0, sl // 2)

    per = 16 // rl
    split = one_hot(16 * sl, 16 * sl, lambda r: (r % sl) * 16 + ((r // (2 * sl)) % per) * rl + (r // (2 * sl * per)) * 2 + (r // sl) % 2)

    for g in range(R // 16):
        got = mm(split, mrow[:, g * 16:(g + 1) * 16, :].reshape(sl * 16, CM)).astype(BF16).reshape(2, per, 2 * sl, CM)
        for pair in range(2):
            send['m1'][pair, g * per:(g + 1) * per] = got[pair]
    for pair in range(2):
        push('m1_%d' % pair, send['m1'].at[pair], recv['m1'].at[pair], True)

    for load in (ld_wsb, ld_ws, ld_wso, ld_web, ld_we, ld_weo):
        load.wait()
    heads = one_hot(WP, WT, lambda r: jnp.where(r % DP < DT, (r % DP) * HT + r // DP, -1))
    for raw, out, turned, dst in ((ws, wso, wsp, wsot), (we, weo, wep, weot)):
        for b in range(2):
            for f in range(4):
                turned[b, f * WP:(f + 1) * WP] = mm(heads, raw[b, f * WT:(f + 1) * WT]).astype(BF16)
            dst[b] = mm(heads, out[b]).T.astype(BF16)

    ld_wc.wait()
    ld_wco.wait()
    ld_wpi.wait()
    arrived('m1_0')

    def load_first(i):
        pl.when(i == 2)(lambda: arrived('m1_1'))
        got = recv['m1'][i // 2].astype(F32)
        return jnp.where(i % 2 == 0, got[:, 0:sl], got[:, sl:2 * sl]).reshape(S, CM)

    def after_first(i):
        pl.when(i == rl // 2 - 1)(lambda: spread('c', 0))
    col_attention(load_first, wc.at[0], wco.at[0], wpi[0], abuf, send['c'], after_first)
    spread('c', 1)
    relay('c', 0)

    def send_cols(pair):
        got = [mcol[2 * pair + u].astype(F32).reshape(n, sl, CM) for u in range(2)]
        send['m2'][pair] = jnp.concatenate(got, axis=1).astype(BF16)
        push('m2_%d' % pair, send['m2'].at[pair], recv['m2'].at[pair], True)

    def after_second(i):
        @pl.when(i == 0)
        def _():
            relay('c', 1)

        @pl.when(i == 1)
        def _():
            spread('a', 0)
            send_cols(0)

        @pl.when(i == 2)
        def _():
            share('c')
    col_attention(lambda i: mcol[i].astype(F32), wc.at[1], wco.at[1], wpi[1], send['a'], cbuf2, after_second)
    spread('a', 1)

    arrived('c_t')
    outer_update('c', abuf, wpot[0], z_ref, zb)
    pair_norm(zb)
    bias_block('s1', wsb[0], HT)
    pair_project(wsp[0])
    arrived('s1')
    relay('a', 0)
    relay('a', 1)
    bias_build('s1', HT, 4, biast_f, True)
    pair_attend(zb, wsot[0], zb)
    pair_send('z1')
    pair_norm(zb)
    bias_block('e1', web[0], HT)
    share('a')
    arrived('z1')
    pair_receive('z1')
    pair_norm(zb)
    pair_project(wep[0])
    arrived('e1')
    send_cols(1)
    bias_build('e1', HT, 4, biast_f, False)
    pair_attend(zb, weot[0], zb)

    pair_norm(zb)
    bias_pack('b2', wb[1], H)
    arrived('a_t')
    outer_update('a', cbuf2, wpot[1], zb, zb)
    pair_norm(zb)
    bias_block('e2', web[1], HT)
    push('b2', send['b2'], recv['b2'], False)
    pair_project(wep[1])
    arrived('m2_0')
    arrived('m2_1')
    unsplit = one_hot(16 * sl, 16 * sl, lambda r: ((r % 4) // 2) * (8 * sl) + ((r % 16) // 4) * (2 * sl) + (r % 2) * sl + r // 16)

    for g in range(R // 16):
        got = jnp.concatenate([recv['m2'][pair, g * per:(g + 1) * per].reshape(8 * sl, CM) for pair in range(2)], axis=0)
        mrow[:, g * 16:(g + 1) * 16, :] = mm(unsplit, got).astype(BF16).reshape(sl, 16, CM)
    row_project(mrow, wr.at[1])
    arrived('e2')
    bias_build('e2', HT, 4, biast_f, True)
    pair_attend(zb, weot[1], zb)
    pair_send('z2')
    pair_norm(zb)
    bias_block('s2', wsb[1], HT)
    arrived('b2')
    bias_build('b2', H, 8, bias_f, False)
    row_attend(mrow, wro.at[1], bias_f, m_out, 0, sl // 2)
    arrived('z2')
    pair_receive('z2')
    pair_norm(zb)
    pair_project(wsp[1])
    arrived('s2')
    bias_build('s2', HT, 4, biast_f, False)
    pair_attend(zb, wsot[1], z_out)
    for flow in FLOWS:
        wait_for(flow, send_sem, like(flow))


def solution(mesh):
    n = mesh.shape['dap']

    def local_step(m, z, mask, rmask, w_row_bias, w_row_in, w_row_out, w_col_in, w_col_out, w_opm_in, w_opm_out, w_ts_bias, w_ts_in, w_ts_out, w_te_bias, w_te_in, w_te_out):
        sl, R, CM = m.shape
        rl, _, CZ = z.shape
        S = mask.shape[0]
        H, D = w_row_in.shape[3:]
        HT, DT = w_ts_in.shape[3:]
        OP = w_opm_in.shape[3]
        HP = -(-H // 8) * 8
        WM, WT = H * D, HT * DT
        WP = HT * -(-DT // 16) * 16
        zt = z.transpose(0, 2, 1)
        wb = jnp.pad(w_row_bias.transpose(0, 2, 1), ((0, 0), (0, HP - H), (0, 0)))
        wr = w_row_in.transpose(0, 2, 3, 4, 1).reshape(2, 4 * WM, CM)
        wc = w_col_in.transpose(0, 2, 3, 4, 1).reshape(2, 4 * WM, CM)
        wro = w_row_out.reshape(2, WM, CM)
        wco = w_col_out.reshape(2, WM, CM)
        wpi = w_opm_in.transpose(0, 2, 3, 1).reshape(2, 2 * OP, CM)
        wpo = w_opm_out.reshape(2, OP * OP, CZ)
        wsb = w_ts_bias.transpose(0, 2, 1)
        web = w_te_bias.transpose(0, 2, 1)
        ws = w_ts_in.transpose(0, 2, 4, 3, 1).reshape(2, 4 * WT, CZ)
        we = w_te_in.transpose(0, 2, 4, 3, 1).reshape(2, 4 * WT, CZ)
        wso = w_ts_out.transpose(0, 2, 1, 3).reshape(2, WT, CZ)
        weo = w_te_out.transpose(0, 2, 1, 3).reshape(2, WT, CZ)
        weights = [wb, wr, wro, wc, wco, wpi, wpo, wsb, ws, wso, web, we, weo]

        def vm(shape, dtype=BF16):
            return pltpu.VMEM(shape, dtype)
        scratch = [vm(w.shape) for w in weights]
        scratch += [vm((OP, OP, CZ)), vm((2, CZ, OP * OP)), vm((2, CZ, WP)), vm((2, CZ, WP))]
        scratch += [vm((H, R, R), F32), vm((HT, R, R), F32)]
        scratch += [vm((CZ, rl * R)), vm((rl, 4 * WP, R)), vm((WP, R)), vm((2, 4 * WP, CZ)), vm((2, 4 * WP, CZ))]
        scratch += [vm((sl // 2, 3 * WM, S)), vm((sl // 2, S, WM)), vm((WM, S))]
        scratch += [vm((sl, R, CM)), vm((rl, S, CM)), vm((rl, CZ, R)), vm((rl, R, CZ))]
        scratch += [vm((rl * OP, S))] * 4 + [vm((OP, R, S)), vm((OP * OP, rl * R))]
        scratch += [vm((S, R)), vm((sl, R), F32), vm((R, R), F32), vm((8, S), F32), vm((8, R), F32)]
        side = math.isqrt(n // 2)
        bias_row, bias_tri = (rl * H, R), (rl * HT, R)
        shapes = {'b1': bias_row, 'b2': bias_row, 's1': bias_tri, 'e1': bias_tri, 'e2': bias_tri, 's2': bias_tri,
                  'c': (rl * OP, S), 'a': (rl * OP, S), 'm1': (rl * sl // 2, CM), 'm2': (rl * sl // 2, CM), 'z1': (rl * rl, CZ), 'z2': (rl * rl, CZ)}
        for name in EXCHANGES:
            shape = shapes[name]
            if name in 'ac':
                scratch += [vm(shape), vm((side, side, 2) + shape)]
            elif name[0] == 'm':
                scratch += [vm((2, n) + shape), vm((2, n) + shape)]
            else:
                scratch += [vm((n,) + shape if name[0] == 'z' else shape), vm((n,) + shape)]
        scratch += [pltpu.SemaphoreType.DMA((len(FLOWS),)), pltpu.SemaphoreType.DMA((len(FLOWS),)), pltpu.SemaphoreType.DMA((len(weights),))]
        cfg = (n, sl, rl, S, R, CM, CZ, H, D, HT, DT, OP, HP)
        vmem = pl.BlockSpec(memory_space=pltpu.VMEM)
        hbm = pl.BlockSpec(memory_space=pl.ANY)
        m_new, z_new = pl.pallas_call(
            functools.partial(step_kernel, cfg),
            out_shape=[jax.ShapeDtypeStruct(m.shape, BF16), jax.ShapeDtypeStruct(zt.shape, BF16)],
            in_specs=[vmem] * 4 + [hbm] * len(weights),
            out_specs=[vmem, vmem],
            scratch_shapes=scratch,
            compiler_params=pltpu.CompilerParams(collective_id=0, has_side_effects=True, vmem_limit_bytes=60 * 2**20),
            name='evoformer',
        )(m, zt, mask, rmask.reshape(1, R), *weights)
        return m_new, z_new.transpose(0, 2, 1)

    in_specs = (P(('data', 'dap')), P(('data', 'dap')), P('data'), P('data')) + (P(),) * 13
    out_specs = (P(('data', 'dap')), P(('data', 'dap')))
    return jax.shard_map(local_step, mesh=mesh, in_specs=in_specs, out_specs=out_specs, check_vma=False)
```

```python
import functools
import math

import jax
import jax.numpy as jnp
from jax import lax
from jax.experimental import pallas as pl
from jax.experimental.pallas import tpu as pltpu
from jax.sharding import PartitionSpec as P

F32 = jnp.float32
BF16 = jnp.bfloat16
EPS = 1e-5
LOG2E = 1.4426950408889634
NEG = -1e9 * LOG2E
NN = (((1,), (0,)), ((), ()))
NT = (((1,), (1,)), ((), ()))
TN = (((0,), (0,)), ((), ()))
MESH = pl.DeviceIdType.MESH


def mm(a, b, dims=NN):
    return lax.dot_general(a, b, dims, preferred_element_type=F32)


def norm_axis(x, axis):
    mean = jnp.mean(x, axis=axis, keepdims=True)
    centered = x - mean
    var = jnp.mean(centered * centered, axis=axis, keepdims=True)
    return (centered * lax.rsqrt(var + EPS)).astype(BF16)


def one_hot(rows, cols, source):
    r = lax.broadcasted_iota(jnp.int32, (rows, cols), 0)
    c = lax.broadcasted_iota(jnp.int32, (rows, cols), 1)
    return jnp.where(c == source(r), 1.0, 0.0).astype(BF16)


def swap_matrix(a, b):
    return one_hot(a * b, a * b, lambda r: (r % a) * b + r // a)


def softmax_cols(t):
    e = jnp.exp2(t - jnp.max(t, axis=0, keepdims=True))
    return (e * (1.0 / jnp.sum(e, axis=0, keepdims=True))).astype(BF16)


EXCHANGES = ('b1', 'm1', 'c', 's1', 'z1', 'e1', 'b2', 'a', 'm2', 'e2', 'z2', 's2')
FLOWS = ('b1', 'm1_0', 'm1_1', 's1', 'z1', 'e1', 'b2', 'm2_0', 'm2_1', 'e2', 'z2', 's2',
         'c_a1', 'c_b1', 'c_a2', 'c_b2', 'c_t', 'a_a1', 'a_b1', 'a_a2', 'a_b2', 'a_t')
STRIDE = 13


def step_kernel(cfg, *refs):
    n, sl, rl, S, R, CM, CZ, H, D, HT, DT, OP, HP = cfg
    WM = H * D
    WT = HT * DT
    DP = -(-DT // 16) * 16
    WP = HT * DP
    side = math.isqrt(n // 2)
    chunk = rl * OP // 2
    it = iter(refs)
    (m_ref, z_ref, mask_ref, rmask_ref, wb_hbm, wr_hbm, wro_hbm, wc_hbm, wco_hbm, wpi_hbm, wpo_hbm,
     wsb_hbm, ws_hbm, wso_hbm, web_hbm, we_hbm, weo_hbm) = [next(it) for _ in range(17)]
    m_out, z_out = next(it), next(it)
    wb, wr, wro, wc, wco, wpi, wpo, wsb, ws, wso, web, we, weo = weights = [next(it) for _ in range(13)]
    wtmp, wpot, wsot, weot = [next(it) for _ in range(4)]
    bias_f, biast_f = next(it), next(it)
    xz, qkvg, gpair, wsp, wep = [next(it) for _ in range(5)]
    qvg, kbuf, gbuf = [next(it) for _ in range(3)]
    mrow, mcol, zb, znb = [next(it) for _ in range(4)]
    abuf, cbuf, abuf2, cbuf2, perm, obuf = [next(it) for _ in range(6)]
    mcolmask, seqmask, rmaskt, colmask, norm_ref = [next(it) for _ in range(5)]
    send = {}
    recv = {}
    for name in EXCHANGES:
        send[name] = next(it)
        recv[name] = next(it)
    send_sem, recv_sem, w_sem = next(it), next(it), next(it)
    hbm = [wb_hbm, wr_hbm, wro_hbm, wc_hbm, wco_hbm, wpi_hbm, wpo_hbm, wsb_hbm, ws_hbm, wso_hbm, web_hbm, we_hbm, weo_hbm]
    loads = [pltpu.make_async_copy(src, dst, w_sem.at[i]) for i, (src, dst) in enumerate(zip(hbm, weights))]
    for load in loads:
        load.start()
    (ld_wb, ld_wr, ld_wro, ld_wc, ld_wco, ld_wpi, ld_wpo, ld_wsb, ld_ws, ld_wso, ld_web, ld_we, ld_weo) = loads

    me = lax.axis_index('dap')
    barrier = pltpu.get_barrier_semaphore()

    @pl.loop(1, n)
    def _(k):
        pl.semaphore_signal(barrier, inc=1, device_id={'dap': lax.rem(me + k, n)}, device_id_type=MESH)

    core, px, py = me % 2, (me // 2) % side, me // (2 * side)

    def at(y, x, c):
        return {'dap': ((y % side) * side + x % side) * 2 + c % 2}

    def remote(flow, src, dst, device):
        f = FLOWS.index(flow)
        return pltpu.make_async_remote_copy(src_ref=src, dst_ref=dst, send_sem=send_sem.at[f], recv_sem=recv_sem.at[f], device_id=device, device_id_type=MESH)

    def wait_for(flow, sems, like):
        pltpu.make_async_copy(like, like, sems.at[FLOWS.index(flow)]).wait()

    def push(flow, src, dst, scatter):
        @pl.loop(1, n)
        def _(k):
            peer = lax.rem(me + k * STRIDE, n)
            remote(flow, src.at[peer] if scatter else src, dst.at[me], {'dap': peer}).start()
        dst[me] = src[me] if scatter else src[...]

    def target(flow):
        if flow[0] == 'm':
            return recv[flow[:2]].at[int(flow[3])]
        return recv[flow]

    def like(flow):
        if flow[1] != '_':
            return target(flow).at[pl.ds(0, n - 1)]
        dst, part = recv[flow[0]], flow[2:]
        rows = slice(0, chunk)
        if part == 't':
            return dst.at[:, :, 0]
        if part[1] == '1':
            return dst.at[0, pl.ds(0, side - 1), 0, rows]
        return dst.at[pl.ds(0, side - 1), :, 0, rows]

    def arrived(flow):
        wait_for(flow, recv_sem, like(flow))

    def spread(name, half):
        rows = slice(half * chunk, (half + 1) * chunk)
        dst = recv[name]
        dst[py, px, core, rows] = send[name][rows]
        for d in range(1, side):
            device = at(py, px + d, core) if half == 0 else at(py + d, px, core)
            remote(name + '_' + 'ab'[half] + '1', send[name].at[rows], dst.at[py, px, core, rows], device).start()

    def relay(name, half):
        arrived(name + '_' + 'ab'[half] + '1')
        rows = slice(half * chunk, (half + 1) * chunk)
        dst = recv[name]
        for d in range(1, side):
            if half == 0:
                part, device = dst.at[py, :, core, rows], at(py + d, px, core)
            else:
                part, device = dst.at[:, px, core, rows], at(py, px + d, core)
            remote(name + '_' + 'ab'[half] + '2', part, part, device).start()

    def share(name):
        arrived(name + '_a2')
        arrived(name + '_b2')
        part = recv[name].at[:, :, core]
        remote(name + '_t', part, part, at(py, px, core + 1)).start()

    eye = one_hot(R, R, lambda r: r)

    def pair_norm(zref):
        for i in range(rl):
            xz[:, i * R:(i + 1) * R] = norm_axis(zref[i].astype(F32), 0)

    def bias_block(name, w, heads):
        bias_pack(name, w, heads)
        push(name, send[name], recv[name], False)

    def bias_pack(name, w, heads):
        got = mm(w, xz[...]).astype(BF16).astype(F32)
        got = jnp.concatenate([got[:, i * R:(i + 1) * R] for i in range(rl)], axis=0).astype(BF16)
        padded = w.shape[0]
        if padded != heads:
            pack = one_hot(rl * heads, rl * padded, lambda r: (r // heads) * padded + r % heads)
            got = mm(pack, got).astype(BF16)
        send[name][...] = got

    def bias_build(name, heads, group, dst, transpose):
        swap = swap_matrix(group * rl, heads)
        rows = group * rl

        for g in range(n // group):
            got = mm(swap, recv[name][g * group:(g + 1) * group].reshape(rows * heads, R)) * LOG2E
            for h in range(heads):
                dst[h, g * rows:(g + 1) * rows, :] = got[h * rows:(h + 1) * rows]
        if transpose:
            for h in range(heads):
                dst[h] = dst[h].T

    def pair_project(w):
        got = mm(w, xz[...])
        for i in range(rl):
            qkvg[i] = got[:, i * R:(i + 1) * R].astype(BF16)

    def pair_attend(zref, wo, dst):
        scale = DT ** -0.5 * LOG2E

        def row(i, u):
            def part(f, h):
                return qkvg[i, f * WP + h * DP:f * WP + (h + 1) * DP]

            def logits(h):
                return mm(part(1, h).astype(F32).T.astype(BF16), part(0, h))
            ahead = logits(0)
            for h in range(HT):
                t = ahead * scale + biast_f[h]
                if h + 1 < HT:
                    ahead = logits(h + 1)
                t = jnp.where(rmaskt[...] > 0, t, NEG)
                o = mm(part(2, h), softmax_cols(t))
                gpair[u, h * DP:(h + 1) * DP, :] = (o * jax.nn.sigmoid(part(3, h).astype(F32))).astype(BF16)
            dst[i] = (zref[i].astype(F32) + mm(wo, gpair[u])).astype(BF16)

        @pl.loop(0, rl // 2)
        def _(t):
            row(2 * t, 0)
            row(2 * t + 1, 1)

    def pair_send(name):
        for i in range(rl):
            znb[i] = zb[i].astype(F32).T.astype(BF16)
        swap = one_hot(4 * rl * rl, 4 * rl * rl, lambda r: (r % rl) * (4 * rl) + r // rl)
        width = 4 * rl

        for g in range(n // 4):
            got = znb[:, g * width:(g + 1) * width, :].reshape(rl * width, CZ)
            send[name][g * 4:(g + 1) * 4] = mm(swap, got).astype(BF16).reshape(4, rl * rl, CZ)
        push(name, send[name], recv[name], True)

    def pair_receive(name):
        rows = 8 * rl
        swap = one_hot(rows * rl, rows * rl, lambda r: ((r % rows) // rl) * (rl * rl) + (r // rows) * rl + r % rl)

        for g in range(n // 8):
            got = mm(swap, recv[name][g * 8:(g + 1) * 8].reshape(rows * rl, CZ)).astype(BF16)
            for i in range(rl):
                znb[i, g * rows:(g + 1) * rows, :] = got[i * rows:(i + 1) * rows]
        for i in range(rl):
            zb[i] = znb[i].astype(F32).T.astype(BF16)

    def outer_update(name, left, wo, zref, dst):
        swap = swap_matrix(4 * rl, 16)
        width = 4 * rl

        per_y = side // 2
        for g in range(n // 4):
            for half in range(OP // 16):
                got = recv[name][g // per_y, (g % per_y) * 2:(g % per_y) * 2 + 2].reshape(width, OP, S)[:, half * 16:(half + 1) * 16].reshape(width * 16, S)
                perm[half * 16:(half + 1) * 16, g * width:(g + 1) * width, :] = mm(swap, got).astype(BF16).reshape(16, width, S)
        for t in range(OP // 2):
            o = mm(left[...], perm[t * 2:t * 2 + 2].reshape(2 * R, S), NT).astype(BF16)
            for u in range(2):
                for i in range(rl):
                    obuf[(t * 2 + u) * OP:(t * 2 + u + 1) * OP, i * R:(i + 1) * R] = o[i * OP:(i + 1) * OP, u * R:(u + 1) * R]
        upd = mm(wo, obuf[...])
        for i in range(rl):
            dst[i] = (zref[i].astype(F32) + upd[:, i * R:(i + 1) * R] * (1.0 / (1e-3 + norm_ref[i:i + 1, :]))).astype(BF16)

    def row_bias_weight(b):
        got = wb[:, b, :].astype(F32)
        return jnp.concatenate([got, jnp.zeros((HP - H, CZ), F32)], axis=0).astype(BF16)

    def project(x, w, p):
        qvg[p, 0:WM] = mm(w[0:WM], x, NT).astype(BF16)
        kbuf[p] = mm(x, w[WM:2 * WM], NT).astype(BF16)
        qvg[p, WM:3 * WM] = mm(w[2 * WM:4 * WM], x, NT).astype(BF16)

    per_tile = 128 // D
    tile_lane = lax.broadcasted_iota(jnp.int32, (16, 128), 1) // D
    head_mask = [jnp.where(tile_lane == j, 1.0, 0.0).astype(BF16) for j in range(per_tile)]

    def attend(p, lo, size, mask, bias):
        scale = D ** -0.5 * LOG2E
        keys = slice(lo, lo + size)

        def query(h, q):
            j = h % per_tile
            parts = [qvg[p, h * D:(h + 1) * D, q:q + 128]]
            if j:
                parts.insert(0, jnp.zeros((j * D, 128), BF16))
            if j + 1 < per_tile:
                parts.append(jnp.zeros(((per_tile - 1 - j) * D, 128), BF16))
            return jnp.concatenate(parts, axis=0)

        def logits(group):
            h, q = group[0]
            tile = (h // per_tile) * 128
            if len(group) == 1:
                kt = kbuf[p, keys, tile:tile + 128].reshape(size // 16, 16, 128)
                kh = (kt * head_mask[h % per_tile][None]).reshape(size, 128)
                return mm(kh, qvg[p, tile:tile + 128, q:q + 128])
            return mm(kbuf[p, keys, tile:tile + 128], jnp.concatenate([query(h, q) for h, q in group], axis=1))
        blocks = [(h, q) for h in range(H) for q in range(lo, lo + size, 128)]
        step = size // 128
        groups = [blocks[b:b + step] for b in range(0, len(blocks), step)]
        ahead = logits(groups[0])
        for b, group in enumerate(groups):
            now = ahead
            if b + 1 < len(groups):
                ahead = logits(groups[b + 1])
            for u, (h, q) in enumerate(group):
                t = now[:, u * 128:(u + 1) * 128] * scale
                if bias is not None:
                    t = t + bias[h]
                t = jnp.where(mask > 0, t, NEG)
                o = mm(qvg[p, WM + h * D:WM + (h + 1) * D, keys], softmax_cols(t))
                g = qvg[p, 2 * WM + h * D:2 * WM + (h + 1) * D, q:q + 128].astype(F32)
                gbuf[h * D:(h + 1) * D, q:q + 128] = (o * jax.nn.sigmoid(g)).astype(BF16)

    def row_project(src, w):
        @pl.loop(0, sl // 2)
        def _(t):
            xf = src[pl.ds(2 * t, 2)].astype(F32).reshape(2 * R, CM)
            project(norm_axis(xf, 1), w, t)

    def row_attend(src, wo, bias, dst, lo, hi):
        @pl.loop(lo, hi)
        def _(t):
            for u in range(2):
                row = seqmask[pl.ds(2 * t + u, 1), :]
                mask = mm(eye, jnp.broadcast_to(row, (R, R)).astype(BF16), NT)
                attend(t, u * R, R, mask, bias)
            xf = src[pl.ds(2 * t, 2)].astype(F32).reshape(2 * R, CM)
            upd = mm(gbuf[...], wo[...], TN)
            dst[pl.ds(2 * t, 2)] = (xf + upd).astype(BF16).reshape(2, R, CM)

    def col_attention(load, w, wo, wp, a_dst, c_dst, after):
        @pl.loop(0, rl)
        def _(i):
            xf = load(i)
            project(norm_axis(xf, 1), w, 0)
            pick = jnp.where(lax.broadcasted_iota(jnp.int32, (R, R), 0) == me * rl + i, 1.0, 0.0).astype(BF16)
            attend(0, 0, S, mm(mcolmask[...], pick), None)
            y = (xf + mm(gbuf[...], wo[...], TN)).astype(BF16)
            mcol[i] = y
            x = norm_axis(y.astype(F32), 1)
            half = (mm(wp, x, NT) * colmask[pl.ds(i, 1), :]).astype(BF16)
            at = pl.ds(pl.multiple_of(i * OP, OP), OP)
            a_dst[at, :] = half[0:OP]
            c_dst[at, :] = half[OP:2 * OP]
            after(i)

    maskf = mask_ref[...].astype(F32).astype(BF16)
    mcolmask[...] = maskf
    seqmask[...] = mask_ref[pl.ds(pl.multiple_of(me * sl, sl), sl), :].astype(F32)
    rmaskt[...] = mm(eye, jnp.broadcast_to(rmask_ref[...].astype(F32), (R, R)).astype(BF16), NT)
    pick = jnp.where(lax.broadcasted_iota(jnp.int32, (8, R), 1) == lax.broadcasted_iota(jnp.int32, (8, R), 0) + me * rl, 1.0, 0.0).astype(BF16)
    colmask[...] = mm(pick, maskf, NT)
    norm_ref[...] = mm(colmask[...].astype(BF16), maskf)

    pair_norm(z_ref)
    ld_wb.wait()
    pl.semaphore_wait(barrier, n - 1)
    bias_block('b1', row_bias_weight(0), H)
    ld_wr.wait()
    row_project(m_ref, wr.at[0])
    ld_wro.wait()
    ld_wpo.wait()
    swap = swap_matrix(16, 16)
    for p in range(OP // 16):
        for q in range(OP // 16):
            got = wpo[0].reshape(OP, OP, CZ)[p * 16:(p + 1) * 16, q * 16:(q + 1) * 16].reshape(256, CZ)
            wtmp[q * 16:(q + 1) * 16, p * 16:(p + 1) * 16, :] = mm(swap, got).astype(BF16).reshape(16, 16, CZ)
    wpot[0] = wtmp[...].reshape(OP * OP, CZ).astype(F32).T.astype(BF16)
    wpot[1] = wpo[1].astype(F32).T.astype(BF16)
    arrived('b1')
    bias_build('b1', H, 8, bias_f, True)

    row_attend(m_ref, wro.at[0], bias_f, mrow, 0, sl // 2)

    per = 16 // rl
    split = one_hot(16 * sl, 16 * sl, lambda r: (r % sl) * 16 + ((r // (2 * sl)) % per) * rl + (r // (2 * sl * per)) * 2 + (r // sl) % 2)

    for g in range(R // 16):
        got = mm(split, mrow[:, g * 16:(g + 1) * 16, :].reshape(sl * 16, CM)).astype(BF16).reshape(2, per, 2 * sl, CM)
        for pair in range(2):
            send['m1'][pair, g * per:(g + 1) * per] = got[pair]
    for pair in range(2):
        push('m1_%d' % pair, send['m1'].at[pair], recv['m1'].at[pair], True)

    for load in (ld_wsb, ld_ws, ld_wso, ld_web, ld_we, ld_weo):
        load.wait()
    heads = one_hot(WP, WT, lambda r: jnp.where(r % DP < DT, (r % DP) * HT + r // DP, -1))
    for raw, out, turned, dst in ((ws, wso, wsp, wsot), (we, weo, wep, weot)):
        for b in range(2):
            for f in range(4):
                turned[b, f * WP:(f + 1) * WP] = mm(heads, raw[b, f * WT:(f + 1) * WT]).astype(BF16)
            dst[b] = mm(heads, out[b]).T.astype(BF16)

    ld_wc.wait()
    ld_wco.wait()
    ld_wpi.wait()
    arrived('m1_0')

    def load_first(i):
        pl.when(i == 2)(lambda: arrived('m1_1'))
        got = recv['m1'][i // 2].astype(F32)
        return jnp.where(i % 2 == 0, got[:, 0:sl], got[:, sl:2 * sl]).reshape(S, CM)

    def after_first(i):
        pl.when(i == rl // 2 - 1)(lambda: spread('c', 0))
    col_attention(load_first, wc.at[0], wco.at[0], wpi[0], abuf, send['c'], after_first)
    spread('c', 1)
    relay('c', 0)

    def send_cols(pair):
        got = [mcol[2 * pair + u].astype(F32).reshape(n, sl, CM) for u in range(2)]
        send['m2'][pair] = jnp.concatenate(got, axis=1).astype(BF16)
        push('m2_%d' % pair, send['m2'].at[pair], recv['m2'].at[pair], True)

    def after_second(i):
        @pl.when(i == 0)
        def _():
            relay('c', 1)

        @pl.when(i == 1)
        def _():
            spread('a', 0)
            send_cols(0)

        @pl.when(i == 2)
        def _():
            share('c')
    col_attention(lambda i: mcol[i].astype(F32), wc.at[1], wco.at[1], wpi[1], send['a'], cbuf2, after_second)
    spread('a', 1)

    arrived('c_t')
    outer_update('c', abuf, wpot[0], z_ref, zb)
    pair_norm(zb)
    bias_block('s1', wsb[0], HT)
    pair_project(wsp[0])
    arrived('s1')
    relay('a', 0)
    relay('a', 1)
    bias_build('s1', HT, 4, biast_f, True)
    pair_attend(zb, wsot[0], zb)
    pair_send('z1')
    pair_norm(zb)
    bias_block('e1', web[0], HT)
    share('a')
    arrived('z1')
    pair_receive('z1')
    pair_norm(zb)
    pair_project(wep[0])
    arrived('e1')
    send_cols(1)
    bias_build('e1', HT, 4, biast_f, False)
    pair_attend(zb, weot[0], zb)

    pair_norm(zb)
    bias_pack('b2', row_bias_weight(1), H)
    arrived('a_t')
    outer_update('a', cbuf2, wpot[1], zb, zb)
    pair_norm(zb)
    bias_block('e2', web[1], HT)
    push('b2', send['b2'], recv['b2'], False)
    pair_project(wep[1])
    arrived('m2_0')
    arrived('m2_1')
    unsplit = one_hot(16 * sl, 16 * sl, lambda r: ((r % 4) // 2) * (8 * sl) + ((r % 16) // 4) * (2 * sl) + (r % 2) * sl + r // 16)

    for g in range(R // 16):
        got = jnp.concatenate([recv['m2'][pair, g * per:(g + 1) * per].reshape(8 * sl, CM) for pair in range(2)], axis=0)
        mrow[:, g * 16:(g + 1) * 16, :] = mm(unsplit, got).astype(BF16).reshape(sl, 16, CM)
    row_project(mrow, wr.at[1])
    arrived('e2')
    bias_build('e2', HT, 4, biast_f, True)
    pair_attend(zb, weot[1], zb)
    pair_send('z2')
    pair_norm(zb)
    bias_block('s2', wsb[1], HT)
    arrived('b2')
    bias_build('b2', H, 8, bias_f, False)
    row_attend(mrow, wro.at[1], bias_f, m_out, 0, sl // 2)
    arrived('z2')
    pair_receive('z2')
    pair_norm(zb)
    pair_project(wsp[1])
    arrived('s2')
    bias_build('s2', HT, 4, biast_f, False)
    pair_attend(zb, wsot[1], z_out)
    for flow in FLOWS:
        wait_for(flow, send_sem, like(flow))


def solution(mesh):
    n = mesh.shape['dap']

    def local_step(m, z, mask, rmask, w_row_bias, w_row_in, w_row_out, w_col_in, w_col_out, w_opm_in, w_opm_out, w_ts_bias, w_ts_in, w_ts_out, w_te_bias, w_te_in, w_te_out):
        sl, R, CM = m.shape
        rl, _, CZ = z.shape
        S = mask.shape[0]
        H, D = w_row_in.shape[3:]
        HT, DT = w_ts_in.shape[3:]
        OP = w_opm_in.shape[3]
        HP = -(-H // 8) * 8
        WM, WT = H * D, HT * DT
        WP = HT * -(-DT // 16) * 16
        zt = z.transpose(0, 2, 1)
        wb = w_row_bias.transpose(2, 0, 1)
        wr = w_row_in.transpose(0, 2, 3, 4, 1).reshape(2, 4 * WM, CM)
        wc = w_col_in.transpose(0, 2, 3, 4, 1).reshape(2, 4 * WM, CM)
        wro = w_row_out.reshape(2, WM, CM)
        wco = w_col_out.reshape(2, WM, CM)
        wpi = w_opm_in.transpose(0, 2, 3, 1).reshape(2, 2 * OP, CM)
        wpo = w_opm_out.reshape(2, OP * OP, CZ)
        wsb = w_ts_bias.transpose(0, 2, 1)
        web = w_te_bias.transpose(0, 2, 1)
        ws = w_ts_in.transpose(0, 2, 4, 3, 1).reshape(2, 4 * WT, CZ)
        we = w_te_in.transpose(0, 2, 4, 3, 1).reshape(2, 4 * WT, CZ)
        wso = w_ts_out.transpose(0, 2, 1, 3).reshape(2, WT, CZ)
        weo = w_te_out.transpose(0, 2, 1, 3).reshape(2, WT, CZ)
        weights = [wb, wr, wro, wc, wco, wpi, wpo, wsb, ws, wso, web, we, weo]

        def vm(shape, dtype=BF16):
            return pltpu.VMEM(shape, dtype)
        scratch = [vm(w.shape) for w in weights]
        scratch += [vm((OP, OP, CZ)), vm((2, CZ, OP * OP)), vm((2, CZ, WP)), vm((2, CZ, WP))]
        scratch += [vm((H, R, R), F32), vm((HT, R, R), F32)]
        scratch += [vm((CZ, rl * R)), vm((rl, 4 * WP, R)), vm((2, WP, R)), vm((2, 4 * WP, CZ)), vm((2, 4 * WP, CZ))]
        scratch += [vm((sl // 2, 3 * WM, S)), vm((sl // 2, S, WM)), vm((WM, S))]
        scratch += [vm((sl, R, CM)), vm((rl, S, CM)), vm((rl, CZ, R)), vm((rl, R, CZ))]
        scratch += [vm((rl * OP, S))] * 4 + [vm((OP, R, S)), vm((OP * OP, rl * R))]
        scratch += [vm((S, R)), vm((sl, R), F32), vm((R, R), F32), vm((8, S), F32), vm((8, R), F32)]
        side = math.isqrt(n // 2)
        bias_row, bias_tri = (rl * H, R), (rl * HT, R)
        shapes = {'b1': bias_row, 'b2': bias_row, 's1': bias_tri, 'e1': bias_tri, 'e2': bias_tri, 's2': bias_tri,
                  'c': (rl * OP, S), 'a': (rl * OP, S), 'm1': (rl * sl // 2, CM), 'm2': (rl * sl // 2, CM), 'z1': (rl * rl, CZ), 'z2': (rl * rl, CZ)}
        for name in EXCHANGES:
            shape = shapes[name]
            if name in 'ac':
                scratch += [vm(shape), vm((side, side, 2) + shape)]
            elif name[0] == 'm':
                scratch += [vm((2, n) + shape), vm((2, n) + shape)]
            else:
                scratch += [vm((n,) + shape if name[0] == 'z' else shape), vm((n,) + shape)]
        scratch += [pltpu.SemaphoreType.DMA((len(FLOWS),)), pltpu.SemaphoreType.DMA((len(FLOWS),)), pltpu.SemaphoreType.DMA((len(weights),))]
        cfg = (n, sl, rl, S, R, CM, CZ, H, D, HT, DT, OP, HP)
        vmem = pl.BlockSpec(memory_space=pltpu.VMEM)
        hbm = pl.BlockSpec(memory_space=pl.ANY)
        m_new, z_new = pl.pallas_call(
            functools.partial(step_kernel, cfg),
            out_shape=[jax.ShapeDtypeStruct(m.shape, BF16), jax.ShapeDtypeStruct(zt.shape, BF16)],
            in_specs=[vmem] * 4 + [hbm] * len(weights),
            out_specs=[vmem, vmem],
            scratch_shapes=scratch,
            compiler_params=pltpu.CompilerParams(collective_id=0, has_side_effects=True, vmem_limit_bytes=60 * 2**20),
            name='evoformer',
        )(m, zt, mask, rmask.reshape(1, R), *weights)
        return m_new, z_new.transpose(0, 2, 1)

    in_specs = (P(('data', 'dap')), P(('data', 'dap')), P('data'), P('data')) + (P(),) * 13
    out_specs = (P(('data', 'dap')), P(('data', 'dap')))
    return jax.shard_map(local_step, mesh=mesh, in_specs=in_specs, out_specs=out_specs, check_vma=False)
```

```python
import functools
import itertools
import math

import jax
import jax.numpy as jnp
from jax import lax
from jax.experimental import pallas as pl
from jax.experimental.pallas import tpu as pltpu
from jax.sharding import PartitionSpec as P

F32 = jnp.float32
BF16 = jnp.bfloat16
EPS = 1e-5
LOG2E = 1.4426950408889634
NEG = -1e9 * LOG2E
NN = (((1,), (0,)), ((), ()))
NT = (((1,), (1,)), ((), ()))
TN = (((0,), (0,)), ((), ()))
MESH = pl.DeviceIdType.MESH


def mm(a, b, dims=NN):
    return lax.dot_general(a, b, dims, preferred_element_type=F32)


def norm_axis(x, axis):
    mean = jnp.mean(x, axis=axis, keepdims=True)
    centered = x - mean
    var = jnp.mean(centered * centered, axis=axis, keepdims=True)
    return (centered * lax.rsqrt(var + EPS)).astype(BF16)


def one_hot(rows, cols, source):
    r = lax.broadcasted_iota(jnp.int32, (rows, cols), 0)
    c = lax.broadcasted_iota(jnp.int32, (rows, cols), 1)
    return jnp.where(c == source(r), 1.0, 0.0).astype(BF16)


def swap_matrix(a, b):
    return one_hot(a * b, a * b, lambda r: (r % a) * b + r // a)


def softmax_cols(t):
    e = jnp.exp2(t - jnp.max(t, axis=0, keepdims=True))
    return (e * (1.0 / jnp.sum(e, axis=0, keepdims=True))).astype(BF16)


EXCHANGES = ('b1', 'm1', 'c', 's1', 'z1', 'e1', 'b2', 'a', 'm2', 'e2', 'z2', 's2')
FLOWS = ('b1', 'm1_0', 'm1_1', 's1', 'z1', 'e1', 'b2', 'm2_0', 'm2_1', 'e2', 'z2', 's2',
         'c_a1', 'c_b1', 'c_a2', 'c_b2', 'c_t', 'a_a1', 'a_b1', 'a_a2', 'a_b2', 'a_t')


def step_kernel(cfg, *refs):
    n, sl, rl, S, R, CM, CZ, H, D, HT, DT, OP, HP = cfg
    WM = H * D
    WT = HT * DT
    DP = -(-DT // 16) * 16
    WP = HT * DP
    side = math.isqrt(n // 2)
    chunk = rl * OP // 2
    it = iter(refs)
    (m_ref, z_ref, mask_ref, rmask_ref, wb_hbm, wr_hbm, wro_hbm, wc_hbm, wco_hbm, wpi_hbm, wpo_hbm,
     wsb_hbm, ws_hbm, wso_hbm, web_hbm, we_hbm, weo_hbm) = [next(it) for _ in range(17)]
    m_out, z_out = next(it), next(it)
    wb, wr, wro, wc, wco, wpi, wpo, wsb, ws, wso, web, we, weo = weights = [next(it) for _ in range(13)]
    wtmp, wpot, wsot, weot = [next(it) for _ in range(4)]
    bias_f, biast_f = next(it), next(it)
    xz, qkvg, gpair, wsp, wep = [next(it) for _ in range(5)]
    qvg, kbuf, gbuf = [next(it) for _ in range(3)]
    mrow, mcol, zb, znb, mfinal = [next(it) for _ in range(5)]
    abuf, cbuf, abuf2, cbuf2, perm, obuf = [next(it) for _ in range(6)]
    mcolmask, seqmask, rmaskt, colmask, norm_ref = [next(it) for _ in range(5)]
    send = {}
    recv = {}
    for name in EXCHANGES:
        send[name] = next(it)
        recv[name] = next(it)
    send_sem, recv_sem, w_sem = next(it), next(it), next(it)
    hbm = [wb_hbm, wr_hbm, wro_hbm, wc_hbm, wco_hbm, wpi_hbm, wpo_hbm, wsb_hbm, ws_hbm, wso_hbm, web_hbm, we_hbm, weo_hbm]
    loads = [pltpu.make_async_copy(src, dst, w_sem.at[i]) for i, (src, dst) in enumerate(zip(hbm, weights))]
    for load in loads:
        load.start()
    (ld_wb, ld_wr, ld_wro, ld_wc, ld_wco, ld_wpi, ld_wpo, ld_wsb, ld_ws, ld_wso, ld_web, ld_we, ld_weo) = loads

    me = lax.axis_index('dap')
    barrier = pltpu.get_barrier_semaphore()

    @pl.loop(1, n)
    def _(k):
        pl.semaphore_signal(barrier, inc=1, device_id={'dap': lax.rem(me + k, n)}, device_id_type=MESH)

    core, px, py = me % 2, (me // 2) % side, me // (2 * side)

    rows_of = [(py + d) % side * (2 * side) for d in range(side)]
    chips_of = [(px + d) % side * 2 for d in range(side)]
    cores_of = [core, 1 - core]

    def hops(offset):
        return sum(min(d, side - d) for d in offset[:2])
    offsets = sorted(itertools.product(range(side), range(side), range(2)), key=hops)[:0:-1]

    def at(y, x, c):
        return {'dap': ((y % side) * side + x % side) * 2 + c % 2}

    def remote(flow, src, dst, device):
        f = FLOWS.index(flow)
        return pltpu.make_async_remote_copy(src_ref=src, dst_ref=dst, send_sem=send_sem.at[f], recv_sem=recv_sem.at[f], device_id=device, device_id_type=MESH)

    def wait_for(flow, sems, like):
        pltpu.make_async_copy(like, like, sems.at[FLOWS.index(flow)]).wait()

    def push(flow, src, dst, scatter):
        for dy, dx, dc in offsets:
            peer = rows_of[dy] + chips_of[dx] + cores_of[dc]
            remote(flow, src.at[peer] if scatter else src, dst.at[me], {'dap': peer}).start()
        dst[me] = src[me] if scatter else src[...]

    def target(flow):
        if flow[0] == 'm':
            return recv[flow[:2]].at[int(flow[3])]
        return recv[flow]

    def like(flow):
        if flow[1] != '_':
            return target(flow).at[pl.ds(0, n - 1)]
        dst, part = recv[flow[0]], flow[2:]
        rows = slice(0, chunk)
        if part == 't':
            return dst.at[:, :, 0]
        if part[1] == '1':
            return dst.at[0, pl.ds(0, side - 1), 0, rows]
        return dst.at[pl.ds(0, side - 1), :, 0, rows]

    def arrived(flow):
        wait_for(flow, recv_sem, like(flow))

    def spread(name, half):
        rows = slice(half * chunk, (half + 1) * chunk)
        dst = recv[name]
        dst[py, px, core, rows] = send[name][rows]
        for d in range(1, side):
            device = at(py, px + d, core) if half == 0 else at(py + d, px, core)
            remote(name + '_' + 'ab'[half] + '1', send[name].at[rows], dst.at[py, px, core, rows], device).start()

    def relay(name, half):
        arrived(name + '_' + 'ab'[half] + '1')
        rows = slice(half * chunk, (half + 1) * chunk)
        dst = recv[name]
        for d in range(1, side):
            if half == 0:
                part, device = dst.at[py, :, core, rows], at(py + d, px, core)
            else:
                part, device = dst.at[:, px, core, rows], at(py, px + d, core)
            remote(name + '_' + 'ab'[half] + '2', part, part, device).start()

    def share(name):
        arrived(name + '_a2')
        arrived(name + '_b2')
        part = recv[name].at[:, :, core]
        remote(name + '_t', part, part, at(py, px, core + 1)).start()

    eye = one_hot(R, R, lambda r: r)

    def pair_norm(zref):
        for i in range(rl):
            xz[:, i * R:(i + 1) * R] = norm_axis(zref[i].astype(F32), 0)

    def bias_block(name, w, heads):
        bias_pack(name, w, heads)
        push(name, send[name], recv[name], False)

    def bias_pack(name, w, heads):
        got = mm(w, xz[...]).astype(BF16).astype(F32)
        got = jnp.concatenate([got[:, i * R:(i + 1) * R] for i in range(rl)], axis=0).astype(BF16)
        padded = w.shape[0]
        if padded != heads:
            pack = one_hot(rl * heads, rl * padded, lambda r: (r // heads) * padded + r % heads)
            got = mm(pack, got).astype(BF16)
        send[name][...] = got

    def bias_build(name, heads, group, dst, transpose):
        swap = swap_matrix(group * rl, heads)
        rows = group * rl

        for g in range(n // group):
            got = mm(swap, recv[name][g * group:(g + 1) * group].reshape(rows * heads, R)) * LOG2E
            for h in range(heads):
                dst[h, g * rows:(g + 1) * rows, :] = got[h * rows:(h + 1) * rows]
        if transpose:
            for h in range(heads):
                dst[h] = dst[h].T

    def pair_project(w):
        got = mm(w, xz[...])
        for i in range(rl):
            qkvg[i] = got[:, i * R:(i + 1) * R].astype(BF16)

    def pair_attend(zref, wo, dst):
        scale = DT ** -0.5 * LOG2E

        def row(i, u):
            def part(f, h):
                return qkvg[i, f * WP + h * DP:f * WP + (h + 1) * DP]

            def logits(h):
                return mm(part(1, h).astype(F32).T.astype(BF16), part(0, h))
            ahead = logits(0)
            for h in range(HT):
                t = ahead * scale + biast_f[h]
                if h + 1 < HT:
                    ahead = logits(h + 1)
                t = jnp.where(rmaskt[...] > 0, t, NEG)
                o = mm(part(2, h), softmax_cols(t))
                gpair[u, h * DP:(h + 1) * DP, :] = (o * jax.nn.sigmoid(part(3, h).astype(F32))).astype(BF16)
            dst[i] = (zref[i].astype(F32) + mm(wo, gpair[u])).astype(dst.dtype)

        @pl.loop(0, rl // 2)
        def _(t):
            row(2 * t, 0)
            row(2 * t + 1, 1)

    def pair_send(name):
        for i in range(rl):
            znb[i] = zb[i].astype(F32).T.astype(BF16)
        swap = one_hot(4 * rl * rl, 4 * rl * rl, lambda r: (r % rl) * (4 * rl) + r // rl)
        width = 4 * rl

        for g in range(n // 4):
            got = znb[:, g * width:(g + 1) * width, :].reshape(rl * width, CZ)
            send[name][g * 4:(g + 1) * 4] = mm(swap, got).astype(BF16).reshape(4, rl * rl, CZ)
        push(name, send[name], recv[name], True)

    def pair_receive(name):
        rows = 8 * rl
        swap = one_hot(rows * rl, rows * rl, lambda r: ((r % rows) // rl) * (rl * rl) + (r // rows) * rl + r % rl)

        for g in range(n // 8):
            got = mm(swap, recv[name][g * 8:(g + 1) * 8].reshape(rows * rl, CZ)).astype(BF16)
            for i in range(rl):
                znb[i, g * rows:(g + 1) * rows, :] = got[i * rows:(i + 1) * rows]
        for i in range(rl):
            zb[i] = znb[i].astype(F32).T.astype(BF16)

    def outer_update(name, left, wo, zref, dst):
        swap = swap_matrix(4 * rl, 16)
        width = 4 * rl

        per_y = side // 2
        for g in range(n // 4):
            for half in range(OP // 16):
                got = recv[name][g // per_y, (g % per_y) * 2:(g % per_y) * 2 + 2].reshape(width, OP, S)[:, half * 16:(half + 1) * 16].reshape(width * 16, S)
                perm[half * 16:(half + 1) * 16, g * width:(g + 1) * width, :] = mm(swap, got).astype(BF16).reshape(16, width, S)
        for t in range(OP // 2):
            o = mm(left[...], perm[t * 2:t * 2 + 2].reshape(2 * R, S), NT).astype(BF16)
            for u in range(2):
                for i in range(rl):
                    obuf[(t * 2 + u) * OP:(t * 2 + u + 1) * OP, i * R:(i + 1) * R] = o[i * OP:(i + 1) * OP, u * R:(u + 1) * R]
        upd = mm(wo, obuf[...])
        for i in range(rl):
            dst[i] = (zref[i].astype(F32) + upd[:, i * R:(i + 1) * R] * (1.0 / (1e-3 + norm_ref[i:i + 1, :]))).astype(BF16)

    def row_bias_weight(b):
        got = wb[:, b, :].astype(F32)
        return jnp.concatenate([got, jnp.zeros((HP - H, CZ), F32)], axis=0).astype(BF16)

    def project(x, w, p):
        qvg[p, 0:WM] = mm(w[0:WM], x, NT).astype(BF16)
        kbuf[p] = mm(x, w[WM:2 * WM], NT).astype(BF16)
        qvg[p, WM:3 * WM] = mm(w[2 * WM:4 * WM], x, NT).astype(BF16)

    per_tile = 128 // D
    tile_lane = lax.broadcasted_iota(jnp.int32, (16, 128), 1) // D
    head_mask = [jnp.where(tile_lane == j, 1.0, 0.0).astype(BF16) for j in range(per_tile)]

    def attend(p, lo, size, mask, bias):
        scale = D ** -0.5 * LOG2E
        keys = slice(lo, lo + size)

        def query(h, q):
            j = h % per_tile
            parts = [qvg[p, h * D:(h + 1) * D, q:q + 128]]
            if j:
                parts.insert(0, jnp.zeros((j * D, 128), BF16))
            if j + 1 < per_tile:
                parts.append(jnp.zeros(((per_tile - 1 - j) * D, 128), BF16))
            return jnp.concatenate(parts, axis=0)

        def logits(group):
            h, q = group[0]
            tile = (h // per_tile) * 128
            if len(group) == 1:
                kt = kbuf[p, keys, tile:tile + 128].reshape(size // 16, 16, 128)
                kh = (kt * head_mask[h % per_tile][None]).reshape(size, 128)
                return mm(kh, qvg[p, tile:tile + 128, q:q + 128])
            return mm(kbuf[p, keys, tile:tile + 128], jnp.concatenate([query(h, q) for h, q in group], axis=1))
        blocks = [(h, q) for h in range(H) for q in range(lo, lo + size, 128)]
        step = size // 128
        groups = [blocks[b:b + step] for b in range(0, len(blocks), step)]
        ahead = logits(groups[0])
        for b, group in enumerate(groups):
            now = ahead
            if b + 1 < len(groups):
                ahead = logits(groups[b + 1])
            for u, (h, q) in enumerate(group):
                t = now[:, u * 128:(u + 1) * 128] * scale
                if bias is not None:
                    t = t + bias[h]
                t = jnp.where(mask > 0, t, NEG)
                o = mm(qvg[p, WM + h * D:WM + (h + 1) * D, keys], softmax_cols(t))
                g = qvg[p, 2 * WM + h * D:2 * WM + (h + 1) * D, q:q + 128].astype(F32)
                gbuf[h * D:(h + 1) * D, q:q + 128] = (o * jax.nn.sigmoid(g)).astype(BF16)

    def row_project(src, w):
        @pl.loop(0, sl // 2)
        def _(t):
            xf = src[pl.ds(2 * t, 2)].astype(F32).reshape(2 * R, CM)
            project(norm_axis(xf, 1), w, t)

    def row_attend(src, wo, bias, dst, lo, hi):
        @pl.loop(lo, hi)
        def _(t):
            for u in range(2):
                row = seqmask[pl.ds(2 * t + u, 1), :]
                mask = mm(eye, jnp.broadcast_to(row, (R, R)).astype(BF16), NT)
                attend(t, u * R, R, mask, bias)
            xf = src[pl.ds(2 * t, 2)].astype(F32).reshape(2 * R, CM)
            upd = mm(gbuf[...], wo[...], TN)
            dst[pl.ds(2 * t, 2)] = (xf + upd).astype(dst.dtype).reshape(2, R, CM)

    def col_attention(load, w, wo, wp, a_dst, c_dst, after):
        @pl.loop(0, rl)
        def _(i):
            xf = load(i)
            project(norm_axis(xf, 1), w, 0)
            pick = jnp.where(lax.broadcasted_iota(jnp.int32, (R, R), 0) == me * rl + i, 1.0, 0.0).astype(BF16)
            attend(0, 0, S, mm(mcolmask[...], pick), None)
            y = (xf + mm(gbuf[...], wo[...], TN)).astype(BF16)
            mcol[i] = y
            x = norm_axis(y.astype(F32), 1)
            half = (mm(wp, x, NT) * colmask[pl.ds(i, 1), :]).astype(BF16)
            at = pl.ds(pl.multiple_of(i * OP, OP), OP)
            a_dst[at, :] = half[0:OP]
            c_dst[at, :] = half[OP:2 * OP]
            after(i)

    maskf = mask_ref[...].astype(F32).astype(BF16)
    mcolmask[...] = maskf
    seqmask[...] = mask_ref[pl.ds(pl.multiple_of(me * sl, sl), sl), :].astype(F32)
    rmaskt[...] = mm(eye, jnp.broadcast_to(rmask_ref[...].astype(F32), (R, R)).astype(BF16), NT)
    pick = jnp.where(lax.broadcasted_iota(jnp.int32, (8, R), 1) == lax.broadcasted_iota(jnp.int32, (8, R), 0) + me * rl, 1.0, 0.0).astype(BF16)
    colmask[...] = mm(pick, maskf, NT)
    norm_ref[...] = mm(colmask[...].astype(BF16), maskf)

    pair_norm(z_ref)
    ld_wb.wait()
    pl.semaphore_wait(barrier, n - 1)
    bias_block('b1', row_bias_weight(0), H)
    ld_wr.wait()
    row_project(m_ref, wr.at[0])
    ld_wro.wait()
    ld_wpo.wait()
    swap = swap_matrix(16, 16)
    for p in range(OP // 16):
        for q in range(OP // 16):
            got = wpo[0].reshape(OP, OP, CZ)[p * 16:(p + 1) * 16, q * 16:(q + 1) * 16].reshape(256, CZ)
            wtmp[q * 16:(q + 1) * 16, p * 16:(p + 1) * 16, :] = mm(swap, got).astype(BF16).reshape(16, 16, CZ)
    wpot[0] = wtmp[...].reshape(OP * OP, CZ).astype(F32).T.astype(BF16)
    wpot[1] = wpo[1].astype(F32).T.astype(BF16)
    arrived('b1')
    bias_build('b1', H, 8, bias_f, True)

    row_attend(m_ref, wro.at[0], bias_f, mrow, 0, sl // 2)

    per = 16 // rl
    split = one_hot(16 * sl, 16 * sl, lambda r: (r % sl) * 16 + ((r // (2 * sl)) % per) * rl + (r // (2 * sl * per)) * 2 + (r // sl) % 2)

    for g in range(R // 16):
        got = mm(split, mrow[:, g * 16:(g + 1) * 16, :].reshape(sl * 16, CM)).astype(BF16).reshape(2, per, 2 * sl, CM)
        for pair in range(2):
            send['m1'][pair, g * per:(g + 1) * per] = got[pair]
    for pair in range(2):
        push('m1_%d' % pair, send['m1'].at[pair], recv['m1'].at[pair], True)

    for load in (ld_wsb, ld_ws, ld_wso, ld_web, ld_we, ld_weo):
        load.wait()
    heads = one_hot(WP, WT, lambda r: jnp.where(r % DP < DT, (r % DP) * HT + r // DP, -1))
    for raw, out, turned, dst in ((ws, wso, wsp, wsot), (we, weo, wep, weot)):
        for b in range(2):
            for f in range(4):
                turned[b, f * WP:(f + 1) * WP] = mm(heads, raw[b, f * WT:(f + 1) * WT]).astype(BF16)
            dst[b] = mm(heads, out[b]).T.astype(BF16)

    ld_wc.wait()
    ld_wco.wait()
    ld_wpi.wait()
    arrived('m1_0')

    def load_first(i):
        pl.when(i == 2)(lambda: arrived('m1_1'))
        got = recv['m1'][i // 2].astype(F32)
        return jnp.where(i % 2 == 0, got[:, 0:sl], got[:, sl:2 * sl]).reshape(S, CM)

    def after_first(i):
        pl.when(i == rl // 2 - 1)(lambda: spread('c', 0))
    col_attention(load_first, wc.at[0], wco.at[0], wpi[0], abuf, send['c'], after_first)
    spread('c', 1)
    relay('c', 0)

    def send_cols(pair):
        got = [mcol[2 * pair + u].astype(F32).reshape(n, sl, CM) for u in range(2)]
        send['m2'][pair] = jnp.concatenate(got, axis=1).astype(BF16)
        push('m2_%d' % pair, send['m2'].at[pair], recv['m2'].at[pair], True)

    def after_second(i):
        @pl.when(i == 0)
        def _():
            relay('c', 1)

        @pl.when(i == 1)
        def _():
            spread('a', 0)
            send_cols(0)

        @pl.when(i == 2)
        def _():
            share('c')
    col_attention(lambda i: mcol[i].astype(F32), wc.at[1], wco.at[1], wpi[1], send['a'], cbuf2, after_second)
    spread('a', 1)

    arrived('c_t')
    outer_update('c', abuf, wpot[0], z_ref, zb)
    pair_norm(zb)
    bias_block('s1', wsb[0], HT)
    pair_project(wsp[0])
    arrived('s1')
    relay('a', 0)
    relay('a', 1)
    bias_build('s1', HT, 4, biast_f, True)
    pair_attend(zb, wsot[0], zb)
    pair_send('z1')
    pair_norm(zb)
    bias_block('e1', web[0], HT)
    share('a')
    arrived('z1')
    pair_receive('z1')
    pair_norm(zb)
    pair_project(wep[0])
    arrived('e1')
    send_cols(1)
    bias_build('e1', HT, 4, biast_f, False)
    pair_attend(zb, weot[0], zb)

    pair_norm(zb)
    bias_pack('b2', row_bias_weight(1), H)
    arrived('a_t')
    outer_update('a', cbuf2, wpot[1], zb, zb)
    pair_norm(zb)
    bias_block('e2', web[1], HT)
    push('b2', send['b2'], recv['b2'], False)
    pair_project(wep[1])
    arrived('m2_0')
    arrived('m2_1')
    unsplit = one_hot(16 * sl, 16 * sl, lambda r: ((r % 4) // 2) * (8 * sl) + ((r % 16) // 4) * (2 * sl) + (r % 2) * sl + r // 16)

    for g in range(R // 16):
        got = jnp.concatenate([recv['m2'][pair, g * per:(g + 1) * per].reshape(8 * sl, CM) for pair in range(2)], axis=0)
        mrow[:, g * 16:(g + 1) * 16, :] = mm(unsplit, got).astype(BF16).reshape(sl, 16, CM)
    row_project(mrow, wr.at[1])
    arrived('e2')
    bias_build('e2', HT, 4, biast_f, True)
    pair_attend(zb, weot[1], zb)
    pair_send('z2')
    pair_norm(zb)
    bias_block('s2', wsb[1], HT)
    arrived('b2')
    bias_build('b2', H, 8, bias_f, False)
    row_attend(mrow, wro.at[1], bias_f, mfinal, 0, sl // 2)
    store = pltpu.make_async_copy(mfinal, m_out, w_sem.at[0])
    store.start()
    arrived('z2')
    pair_receive('z2')
    pair_norm(zb)
    pair_project(wsp[1])
    arrived('s2')
    bias_build('s2', HT, 4, biast_f, False)
    pair_attend(zb, wsot[1], z_out)
    store.wait()
    for flow in FLOWS:
        wait_for(flow, send_sem, like(flow))


def solution(mesh):
    n = mesh.shape['dap']

    def local_step(m, z, mask, rmask, w_row_bias, w_row_in, w_row_out, w_col_in, w_col_out, w_opm_in, w_opm_out, w_ts_bias, w_ts_in, w_ts_out, w_te_bias, w_te_in, w_te_out):
        sl, R, CM = m.shape
        rl, _, CZ = z.shape
        S = mask.shape[0]
        H, D = w_row_in.shape[3:]
        HT, DT = w_ts_in.shape[3:]
        OP = w_opm_in.shape[3]
        HP = -(-H // 8) * 8
        WM, WT = H * D, HT * DT
        WP = HT * -(-DT // 16) * 16
        zt = z.transpose(0, 2, 1)
        wb = w_row_bias.transpose(2, 0, 1)
        wr = w_row_in.transpose(0, 2, 3, 4, 1).reshape(2, 4 * WM, CM)
        wc = w_col_in.transpose(0, 2, 3, 4, 1).reshape(2, 4 * WM, CM)
        wro = w_row_out.reshape(2, WM, CM)
        wco = w_col_out.reshape(2, WM, CM)
        wpi = w_opm_in.transpose(0, 2, 3, 1).reshape(2, 2 * OP, CM)
        wpo = w_opm_out.reshape(2, OP * OP, CZ)
        wsb = w_ts_bias.transpose(0, 2, 1)
        web = w_te_bias.transpose(0, 2, 1)
        ws = w_ts_in.transpose(0, 2, 4, 3, 1).reshape(2, 4 * WT, CZ)
        we = w_te_in.transpose(0, 2, 4, 3, 1).reshape(2, 4 * WT, CZ)
        wso = w_ts_out.transpose(0, 2, 1, 3).reshape(2, WT, CZ)
        weo = w_te_out.transpose(0, 2, 1, 3).reshape(2, WT, CZ)
        weights = [wb, wr, wro, wc, wco, wpi, wpo, wsb, ws, wso, web, we, weo]

        def vm(shape, dtype=BF16):
            return pltpu.VMEM(shape, dtype)
        scratch = [vm(w.shape) for w in weights]
        scratch += [vm((OP, OP, CZ)), vm((2, CZ, OP * OP)), vm((2, CZ, WP)), vm((2, CZ, WP))]
        scratch += [vm((H, R, R), F32), vm((HT, R, R), F32)]
        scratch += [vm((CZ, rl * R)), vm((rl, 4 * WP, R)), vm((2, WP, R)), vm((2, 4 * WP, CZ)), vm((2, 4 * WP, CZ))]
        scratch += [vm((sl // 2, 3 * WM, S)), vm((sl // 2, S, WM)), vm((WM, S))]
        scratch += [vm((sl, R, CM)), vm((rl, S, CM)), vm((rl, CZ, R)), vm((rl, R, CZ)), vm((sl, R, CM), F32)]
        scratch += [vm((rl * OP, S))] * 4 + [vm((OP, R, S)), vm((OP * OP, rl * R))]
        scratch += [vm((S, R)), vm((sl, R), F32), vm((R, R), F32), vm((8, S), F32), vm((8, R), F32)]
        side = math.isqrt(n // 2)
        bias_row, bias_tri = (rl * H, R), (rl * HT, R)
        shapes = {'b1': bias_row, 'b2': bias_row, 's1': bias_tri, 'e1': bias_tri, 'e2': bias_tri, 's2': bias_tri,
                  'c': (rl * OP, S), 'a': (rl * OP, S), 'm1': (rl * sl // 2, CM), 'm2': (rl * sl // 2, CM), 'z1': (rl * rl, CZ), 'z2': (rl * rl, CZ)}
        for name in EXCHANGES:
            shape = shapes[name]
            if name in 'ac':
                scratch += [vm(shape), vm((side, side, 2) + shape)]
            elif name[0] == 'm':
                scratch += [vm((2, n) + shape), vm((2, n) + shape)]
            else:
                scratch += [vm((n,) + shape if name[0] == 'z' else shape), vm((n,) + shape)]
        scratch += [pltpu.SemaphoreType.DMA((len(FLOWS),)), pltpu.SemaphoreType.DMA((len(FLOWS),)), pltpu.SemaphoreType.DMA((len(weights),))]
        cfg = (n, sl, rl, S, R, CM, CZ, H, D, HT, DT, OP, HP)
        vmem = pl.BlockSpec(memory_space=pltpu.VMEM)
        hbm = pl.BlockSpec(memory_space=pl.ANY)
        m_new, z_new = pl.pallas_call(
            functools.partial(step_kernel, cfg),
            out_shape=[jax.ShapeDtypeStruct(m.shape, F32), jax.ShapeDtypeStruct(zt.shape, F32)],
            in_specs=[vmem] * 4 + [hbm] * len(weights),
            out_specs=[hbm, vmem],
            scratch_shapes=scratch,
            compiler_params=pltpu.CompilerParams(collective_id=0, has_side_effects=True, vmem_limit_bytes=60 * 2**20),
            name='evoformer',
        )(m, zt, mask, rmask.reshape(1, R), *weights)
        return m_new.astype(BF16), z_new.transpose(0, 2, 1).astype(BF16)

    in_specs = (P(('data', 'dap')), P(('data', 'dap')), P('data'), P('data')) + (P(),) * 13
    out_specs = (P(('data', 'dap')), P(('data', 'dap')))
    return jax.shard_map(local_step, mesh=mesh, in_specs=in_specs, out_specs=out_specs, check_vma=False)
```

```python
import functools
import math

import jax
import jax.numpy as jnp
from jax import lax
from jax.experimental import pallas as pl
from jax.experimental.pallas import tpu as pltpu
from jax.sharding import PartitionSpec as P

F32 = jnp.float32
BF16 = jnp.bfloat16
EPS = 1e-5
LOG2E = 1.4426950408889634
NEG = -1e9 * LOG2E
NN = (((1,), (0,)), ((), ()))
NT = (((1,), (1,)), ((), ()))
TN = (((0,), (0,)), ((), ()))
MESH = pl.DeviceIdType.MESH


def mm(a, b, dims=NN):
    return lax.dot_general(a, b, dims, preferred_element_type=F32)


def norm_axis(x, axis):
    mean = jnp.mean(x, axis=axis, keepdims=True)
    centered = x - mean
    var = jnp.mean(centered * centered, axis=axis, keepdims=True)
    return (centered * lax.rsqrt(var + EPS)).astype(BF16)


def one_hot(rows, cols, source):
    r = lax.broadcasted_iota(jnp.int32, (rows, cols), 0)
    c = lax.broadcasted_iota(jnp.int32, (rows, cols), 1)
    return jnp.where(c == source(r), 1.0, 0.0).astype(BF16)


def swap_matrix(a, b):
    return one_hot(a * b, a * b, lambda r: (r % a) * b + r // a)


def softmax_cols(t):
    e = jnp.exp2(t - jnp.max(t, axis=0, keepdims=True))
    return e.astype(BF16), 1.0 / jnp.sum(e, axis=0, keepdims=True)


EXCHANGES = ('b1', 'm1', 'c', 's1', 'z1', 'e1', 'b2', 'a', 'm2', 'e2', 'z2', 's2')
FLOWS = ('b1', 'm1_0', 'm1_1', 's1', 'z1', 'e1', 'b2', 'm2_0', 'm2_1', 'e2', 'z2', 's2',
         'c_a1', 'c_b1', 'c_a2', 'c_b2', 'c_t', 'a_a1', 'a_b1', 'a_a2', 'a_b2', 'a_t')
STRIDE = 13


def step_kernel(cfg, *refs):
    n, sl, rl, S, R, CM, CZ, H, D, HT, DT, OP, HP = cfg
    WM = H * D
    WT = HT * DT
    DP = -(-DT // 16) * 16
    WP = HT * DP
    side = math.isqrt(n // 2)
    chunk = rl * OP // 2
    it = iter(refs)
    (m_ref, z_ref, mask_ref, rmask_ref, wb_hbm, wr_hbm, wro_hbm, wc_hbm, wco_hbm, wpi_hbm, wpo_hbm,
     wsb_hbm, ws_hbm, wso_hbm, web_hbm, we_hbm, weo_hbm) = [next(it) for _ in range(17)]
    m_out, z_out = next(it), next(it)
    wb, wr, wro, wc, wco, wpi, wpo, wsb, ws, wso, web, we, weo = weights = [next(it) for _ in range(13)]
    wtmp, wpot, wsot, weot = [next(it) for _ in range(4)]
    bias_f, biast_f = next(it), next(it)
    xz, qkvg, gpair, wsp, wep = [next(it) for _ in range(5)]
    qvg, kbuf, gbuf = [next(it) for _ in range(3)]
    mrow, mcol, zb, znb = [next(it) for _ in range(4)]
    abuf, cbuf, abuf2, cbuf2, perm, obuf = [next(it) for _ in range(6)]
    mcolmask, seqmask, rmaskt, colmask, norm_ref = [next(it) for _ in range(5)]
    send = {}
    recv = {}
    for name in EXCHANGES:
        send[name] = next(it)
        recv[name] = next(it)
    send_sem, recv_sem, w_sem = next(it), next(it), next(it)
    hbm = [wb_hbm, wr_hbm, wro_hbm, wc_hbm, wco_hbm, wpi_hbm, wpo_hbm, wsb_hbm, ws_hbm, wso_hbm, web_hbm, we_hbm, weo_hbm]
    loads = [pltpu.make_async_copy(src, dst, w_sem.at[i]) for i, (src, dst) in enumerate(zip(hbm, weights))]
    for load in loads:
        load.start()
    (ld_wb, ld_wr, ld_wro, ld_wc, ld_wco, ld_wpi, ld_wpo, ld_wsb, ld_ws, ld_wso, ld_web, ld_we, ld_weo) = loads

    me = lax.axis_index('dap')
    barrier = pltpu.get_barrier_semaphore()

    @pl.loop(1, n)
    def _(k):
        pl.semaphore_signal(barrier, inc=1, device_id={'dap': lax.rem(me + k, n)}, device_id_type=MESH)

    core, px, py = me % 2, (me // 2) % side, me // (2 * side)

    def at(y, x, c):
        return {'dap': ((y % side) * side + x % side) * 2 + c % 2}

    def remote(flow, src, dst, device):
        f = FLOWS.index(flow)
        return pltpu.make_async_remote_copy(src_ref=src, dst_ref=dst, send_sem=send_sem.at[f], recv_sem=recv_sem.at[f], device_id=device, device_id_type=MESH)

    def wait_for(flow, sems, like):
        pltpu.make_async_copy(like, like, sems.at[FLOWS.index(flow)]).wait()

    def push(flow, src, dst, scatter):
        @pl.loop(1, n)
        def _(k):
            peer = lax.rem(me + k * STRIDE, n)
            remote(flow, src.at[peer] if scatter else src, dst.at[me], {'dap': peer}).start()
        dst[me] = src[me] if scatter else src[...]

    def target(flow):
        if flow[0] == 'm':
            return recv[flow[:2]].at[int(flow[3])]
        return recv[flow]

    def like(flow):
        if flow[1] != '_':
            return target(flow).at[pl.ds(0, n - 1)]
        dst, part = recv[flow[0]], flow[2:]
        rows = slice(0, chunk)
        if part == 't':
            return dst.at[:, :, 0]
        if part[1] == '1':
            return dst.at[0, pl.ds(0, side - 1), 0, rows]
        return dst.at[pl.ds(0, side - 1), :, 0, rows]

    def arrived(flow):
        wait_for(flow, recv_sem, like(flow))

    def spread(name, half):
        rows = slice(half * chunk, (half + 1) * chunk)
        dst = recv[name]
        dst[py, px, core, rows] = send[name][rows]
        for d in range(1, side):
            device = at(py, px + d, core) if half == 0 else at(py + d, px, core)
            remote(name + '_' + 'ab'[half] + '1', send[name].at[rows], dst.at[py, px, core, rows], device).start()

    def relay(name, half):
        arrived(name + '_' + 'ab'[half] + '1')
        rows = slice(half * chunk, (half + 1) * chunk)
        dst = recv[name]
        for d in range(1, side):
            if half == 0:
                part, device = dst.at[py, :, core, rows], at(py + d, px, core)
            else:
                part, device = dst.at[:, px, core, rows], at(py, px + d, core)
            remote(name + '_' + 'ab'[half] + '2', part, part, device).start()

    def share(name):
        arrived(name + '_a2')
        arrived(name + '_b2')
        part = recv[name].at[:, :, core]
        remote(name + '_t', part, part, at(py, px, core + 1)).start()

    eye = one_hot(R, R, lambda r: r)

    def pair_norm(zref):
        for i in range(rl):
            xz[:, i * R:(i + 1) * R] = norm_axis(zref[i].astype(F32), 0)

    def bias_block(name, w, heads):
        bias_pack(name, w, heads)
        push(name, send[name], recv[name], False)

    def bias_pack(name, w, heads):
        got = mm(w, xz[...]).astype(BF16).astype(F32)
        got = jnp.concatenate([got[:, i * R:(i + 1) * R] for i in range(rl)], axis=0).astype(BF16)
        padded = w.shape[0]
        if padded != heads:
            pack = one_hot(rl * heads, rl * padded, lambda r: (r // heads) * padded + r % heads)
            got = mm(pack, got).astype(BF16)
        send[name][...] = got

    def bias_build(name, heads, group, dst, transpose):
        swap = swap_matrix(group * rl, heads)
        rows = group * rl

        for g in range(n // group):
            got = mm(swap, recv[name][g * group:(g + 1) * group].reshape(rows * heads, R)) * LOG2E
            for h in range(heads):
                dst[h, g * rows:(g + 1) * rows, :] = got[h * rows:(h + 1) * rows]
        if transpose:
            for h in range(heads):
                dst[h] = dst[h].T

    def pair_project(w):
        got = mm(w, xz[...])
        for i in range(rl):
            qkvg[i] = got[:, i * R:(i + 1) * R].astype(BF16)

    def pair_attend(zref, wo, dst):
        scale = DT ** -0.5 * LOG2E

        def row(i, u):
            def part(f, h):
                return qkvg[i, f * WP + h * DP:f * WP + (h + 1) * DP]

            def logits(h):
                return mm(part(1, h).astype(F32).T.astype(BF16), part(0, h))
            ahead = logits(0)
            for h in range(HT):
                t = ahead * scale + biast_f[h]
                if h + 1 < HT:
                    ahead = logits(h + 1)
                t = jnp.where(rmaskt[...] > 0, t, NEG)
                e, inverse = softmax_cols(t)
                o = mm(part(2, h), e) * inverse
                gpair[u, h * DP:(h + 1) * DP, :] = (o * jax.nn.sigmoid(part(3, h).astype(F32))).astype(BF16)
            dst[i] = (zref[i].astype(F32) + mm(wo, gpair[u])).astype(BF16)

        @pl.loop(0, rl // 2)
        def _(t):
            row(2 * t, 0)
            row(2 * t + 1, 1)

    def pair_send(name):
        for i in range(rl):
            znb[i] = zb[i].astype(F32).T.astype(BF16)
        swap = one_hot(4 * rl * rl, 4 * rl * rl, lambda r: (r % rl) * (4 * rl) + r // rl)
        width = 4 * rl

        for g in range(n // 4):
            got = znb[:, g * width:(g + 1) * width, :].reshape(rl * width, CZ)
            send[name][g * 4:(g + 1) * 4] = mm(swap, got).astype(BF16).reshape(4, rl * rl, CZ)
        push(name, send[name], recv[name], True)

    def pair_receive(name):
        rows = 8 * rl
        swap = one_hot(rows * rl, rows * rl, lambda r: ((r % rows) // rl) * (rl * rl) + (r // rows) * rl + r % rl)

        for g in range(n // 8):
            got = mm(swap, recv[name][g * 8:(g + 1) * 8].reshape(rows * rl, CZ)).astype(BF16)
            for i in range(rl):
                znb[i, g * rows:(g + 1) * rows, :] = got[i * rows:(i + 1) * rows]
        for i in range(rl):
            zb[i] = znb[i].astype(F32).T.astype(BF16)

    def outer_update(name, left, wo, zref, dst):
        swap = swap_matrix(4 * rl, 16)
        width = 4 * rl

        per_y = side // 2
        for g in range(n // 4):
            for half in range(OP // 16):
                got = recv[name][g // per_y, (g % per_y) * 2:(g % per_y) * 2 + 2].reshape(width, OP, S)[:, half * 16:(half + 1) * 16].reshape(width * 16, S)
                perm[half * 16:(half + 1) * 16, g * width:(g + 1) * width, :] = mm(swap, got).astype(BF16).reshape(16, width, S)
        for t in range(OP // 2):
            o = mm(left[...], perm[t * 2:t * 2 + 2].reshape(2 * R, S), NT).astype(BF16)
            for u in range(2):
                for i in range(rl):
                    obuf[(t * 2 + u) * OP:(t * 2 + u + 1) * OP, i * R:(i + 1) * R] = o[i * OP:(i + 1) * OP, u * R:(u + 1) * R]
        upd = mm(wo, obuf[...])
        for i in range(rl):
            dst[i] = (zref[i].astype(F32) + upd[:, i * R:(i + 1) * R] * (1.0 / (1e-3 + norm_ref[i:i + 1, :]))).astype(BF16)

    def row_bias_weight(b):
        got = wb[:, b, :].astype(F32)
        return jnp.concatenate([got, jnp.zeros((HP - H, CZ), F32)], axis=0).astype(BF16)

    def project(x, w, p):
        qvg[p, 0:WM] = mm(w[0:WM], x, NT).astype(BF16)
        kbuf[p] = mm(x, w[WM:2 * WM], NT).astype(BF16)
        qvg[p, WM:3 * WM] = mm(w[2 * WM:4 * WM], x, NT).astype(BF16)

    per_tile = 128 // D
    tile_lane = lax.broadcasted_iota(jnp.int32, (16, 128), 1) // D
    head_mask = [jnp.where(tile_lane == j, 1.0, 0.0).astype(BF16) for j in range(per_tile)]

    def attend(p, lo, size, mask, bias):
        scale = D ** -0.5 * LOG2E
        keys = slice(lo, lo + size)

        def query(h, q):
            j = h % per_tile
            parts = [qvg[p, h * D:(h + 1) * D, q:q + 128]]
            if j:
                parts.insert(0, jnp.zeros((j * D, 128), BF16))
            if j + 1 < per_tile:
                parts.append(jnp.zeros(((per_tile - 1 - j) * D, 128), BF16))
            return jnp.concatenate(parts, axis=0)

        def logits(group):
            h, q = group[0]
            tile = (h // per_tile) * 128
            if len(group) == 1:
                kt = kbuf[p, keys, tile:tile + 128].reshape(size // 16, 16, 128)
                kh = (kt * head_mask[h % per_tile][None]).reshape(size, 128)
                return mm(kh, qvg[p, tile:tile + 128, q:q + 128])
            return mm(kbuf[p, keys, tile:tile + 128], jnp.concatenate([query(h, q) for h, q in group], axis=1))
        blocks = [(h, q) for h in range(H) for q in range(lo, lo + size, 128)]
        step = size // 128
        groups = [blocks[b:b + step] for b in range(0, len(blocks), step)]
        ahead = logits(groups[0])
        for b, group in enumerate(groups):
            now = ahead
            if b + 1 < len(groups):
                ahead = logits(groups[b + 1])
            for u, (h, q) in enumerate(group):
                t = now[:, u * 128:(u + 1) * 128] * scale
                if bias is not None:
                    t = t + bias[h]
                t = jnp.where(mask > 0, t, NEG)
                e, inverse = softmax_cols(t)
                o = mm(qvg[p, WM + h * D:WM + (h + 1) * D, keys], e) * inverse
                g = qvg[p, 2 * WM + h * D:2 * WM + (h + 1) * D, q:q + 128].astype(F32)
                gbuf[h * D:(h + 1) * D, q:q + 128] = (o * jax.nn.sigmoid(g)).astype(BF16)

    def row_project(src, w):
        @pl.loop(0, sl // 2)
        def _(t):
            xf = src[pl.ds(2 * t, 2)].astype(F32).reshape(2 * R, CM)
            project(norm_axis(xf, 1), w, t)

    def row_attend(src, wo, bias, dst, lo, hi):
        @pl.loop(lo, hi)
        def _(t):
            for u in range(2):
                row = seqmask[pl.ds(2 * t + u, 1), :]
                mask = mm(eye, jnp.broadcast_to(row, (R, R)).astype(BF16), NT)
                attend(t, u * R, R, mask, bias)
            xf = src[pl.ds(2 * t, 2)].astype(F32).reshape(2 * R, CM)
            upd = mm(gbuf[...], wo[...], TN)
            dst[pl.ds(2 * t, 2)] = (xf + upd).astype(BF16).reshape(2, R, CM)

    def col_attention(load, w, wo, wp, a_dst, c_dst, after):
        @pl.loop(0, rl)
        def _(i):
            xf = load(i)
            project(norm_axis(xf, 1), w, 0)
            pick = jnp.where(lax.broadcasted_iota(jnp.int32, (R, R), 0) == me * rl + i, 1.0, 0.0).astype(BF16)
            attend(0, 0, S, mm(mcolmask[...], pick), None)
            y = (xf + mm(gbuf[...], wo[...], TN)).astype(BF16)
            mcol[i] = y
            x = norm_axis(y.astype(F32), 1)
            half = (mm(wp, x, NT) * colmask[pl.ds(i, 1), :]).astype(BF16)
            at = pl.ds(pl.multiple_of(i * OP, OP), OP)
            a_dst[at, :] = half[0:OP]
            c_dst[at, :] = half[OP:2 * OP]
            after(i)

    maskf = mask_ref[...].astype(F32).astype(BF16)
    mcolmask[...] = maskf
    seqmask[...] = mask_ref[pl.ds(pl.multiple_of(me * sl, sl), sl), :].astype(F32)
    rmaskt[...] = mm(eye, jnp.broadcast_to(rmask_ref[...].astype(F32), (R, R)).astype(BF16), NT)
    pick = jnp.where(lax.broadcasted_iota(jnp.int32, (8, R), 1) == lax.broadcasted_iota(jnp.int32, (8, R), 0) + me * rl, 1.0, 0.0).astype(BF16)
    colmask[...] = mm(pick, maskf, NT)
    norm_ref[...] = mm(colmask[...].astype(BF16), maskf)

    pair_norm(z_ref)
    ld_wb.wait()
    pl.semaphore_wait(barrier, n - 1)
    bias_block('b1', row_bias_weight(0), H)
    ld_wr.wait()
    row_project(m_ref, wr.at[0])
    ld_wro.wait()
    ld_wpo.wait()
    swap = swap_matrix(16, 16)
    for p in range(OP // 16):
        for q in range(OP // 16):
            got = wpo[0].reshape(OP, OP, CZ)[p * 16:(p + 1) * 16, q * 16:(q + 1) * 16].reshape(256, CZ)
            wtmp[q * 16:(q + 1) * 16, p * 16:(p + 1) * 16, :] = mm(swap, got).astype(BF16).reshape(16, 16, CZ)
    wpot[0] = wtmp[...].reshape(OP * OP, CZ).astype(F32).T.astype(BF16)
    wpot[1] = wpo[1].astype(F32).T.astype(BF16)
    arrived('b1')
    bias_build('b1', H, 8, bias_f, True)

    row_attend(m_ref, wro.at[0], bias_f, mrow, 0, sl // 2)

    per = 16 // rl
    split = one_hot(16 * sl, 16 * sl, lambda r: (r % sl) * 16 + ((r // (2 * sl)) % per) * rl + (r // (2 * sl * per)) * 2 + (r // sl) % 2)

    for g in range(R // 16):
        got = mm(split, mrow[:, g * 16:(g + 1) * 16, :].reshape(sl * 16, CM)).astype(BF16).reshape(2, per, 2 * sl, CM)
        for pair in range(2):
            send['m1'][pair, g * per:(g + 1) * per] = got[pair]
    for pair in range(2):
        push('m1_%d' % pair, send['m1'].at[pair], recv['m1'].at[pair], True)

    for load in (ld_wsb, ld_ws, ld_wso, ld_web, ld_we, ld_weo):
        load.wait()
    heads = one_hot(WP, WT, lambda r: jnp.where(r % DP < DT, (r % DP) * HT + r // DP, -1))
    for raw, out, turned, dst in ((ws, wso, wsp, wsot), (we, weo, wep, weot)):
        for b in range(2):
            for f in range(4):
                turned[b, f * WP:(f + 1) * WP] = mm(heads, raw[b, f * WT:(f + 1) * WT]).astype(BF16)
            dst[b] = mm(heads, out[b]).T.astype(BF16)

    ld_wc.wait()
    ld_wco.wait()
    ld_wpi.wait()
    arrived('m1_0')

    def load_first(i):
        pl.when(i == 2)(lambda: arrived('m1_1'))
        got = recv['m1'][i // 2].astype(F32)
        return jnp.where(i % 2 == 0, got[:, 0:sl], got[:, sl:2 * sl]).reshape(S, CM)

    def after_first(i):
        pl.when(i == rl // 2 - 1)(lambda: spread('c', 0))
    col_attention(load_first, wc.at[0], wco.at[0], wpi[0], abuf, send['c'], after_first)
    spread('c', 1)
    relay('c', 0)

    def send_cols(pair):
        got = [mcol[2 * pair + u].astype(F32).reshape(n, sl, CM) for u in range(2)]
        send['m2'][pair] = jnp.concatenate(got, axis=1).astype(BF16)
        push('m2_%d' % pair, send['m2'].at[pair], recv['m2'].at[pair], True)

    def after_second(i):
        @pl.when(i == 0)
        def _():
            relay('c', 1)

        @pl.when(i == 1)
        def _():
            spread('a', 0)
            send_cols(0)

        @pl.when(i == 2)
        def _():
            share('c')
    col_attention(lambda i: mcol[i].astype(F32), wc.at[1], wco.at[1], wpi[1], send['a'], cbuf2, after_second)
    spread('a', 1)

    arrived('c_t')
    outer_update('c', abuf, wpot[0], z_ref, zb)
    pair_norm(zb)
    bias_block('s1', wsb[0], HT)
    pair_project(wsp[0])
    arrived('s1')
    relay('a', 0)
    relay('a', 1)
    bias_build('s1', HT, 4, biast_f, True)
    pair_attend(zb, wsot[0], zb)
    pair_send('z1')
    pair_norm(zb)
    bias_block('e1', web[0], HT)
    share('a')
    arrived('z1')
    pair_receive('z1')
    pair_norm(zb)
    pair_project(wep[0])
    arrived('e1')
    send_cols(1)
    bias_build('e1', HT, 4, biast_f, False)
    pair_attend(zb, weot[0], zb)

    pair_norm(zb)
    bias_pack('b2', row_bias_weight(1), H)
    arrived('a_t')
    outer_update('a', cbuf2, wpot[1], zb, zb)
    pair_norm(zb)
    bias_block('e2', web[1], HT)
    push('b2', send['b2'], recv['b2'], False)
    pair_project(wep[1])
    arrived('m2_0')
    arrived('m2_1')
    unsplit = one_hot(16 * sl, 16 * sl, lambda r: ((r % 4) // 2) * (8 * sl) + ((r % 16) // 4) * (2 * sl) + (r % 2) * sl + r // 16)

    for g in range(R // 16):
        got = jnp.concatenate([recv['m2'][pair, g * per:(g + 1) * per].reshape(8 * sl, CM) for pair in range(2)], axis=0)
        mrow[:, g * 16:(g + 1) * 16, :] = mm(unsplit, got).astype(BF16).reshape(sl, 16, CM)
    row_project(mrow, wr.at[1])
    arrived('e2')
    bias_build('e2', HT, 4, biast_f, True)
    pair_attend(zb, weot[1], zb)
    pair_send('z2')
    pair_norm(zb)
    bias_block('s2', wsb[1], HT)
    arrived('b2')
    bias_build('b2', H, 8, bias_f, False)
    row_attend(mrow, wro.at[1], bias_f, m_out, 0, sl // 2)
    arrived('z2')
    pair_receive('z2')
    pair_norm(zb)
    pair_project(wsp[1])
    arrived('s2')
    bias_build('s2', HT, 4, biast_f, False)
    pair_attend(zb, wsot[1], z_out)
    for flow in FLOWS:
        wait_for(flow, send_sem, like(flow))


def solution(mesh):
    n = mesh.shape['dap']

    def local_step(m, z, mask, rmask, w_row_bias, w_row_in, w_row_out, w_col_in, w_col_out, w_opm_in, w_opm_out, w_ts_bias, w_ts_in, w_ts_out, w_te_bias, w_te_in, w_te_out):
        sl, R, CM = m.shape
        rl, _, CZ = z.shape
        S = mask.shape[0]
        H, D = w_row_in.shape[3:]
        HT, DT = w_ts_in.shape[3:]
        OP = w_opm_in.shape[3]
        HP = -(-H // 8) * 8
        WM, WT = H * D, HT * DT
        WP = HT * -(-DT // 16) * 16
        zt = z.transpose(0, 2, 1)
        wb = w_row_bias.transpose(2, 0, 1)
        wr = w_row_in.transpose(0, 2, 3, 4, 1).reshape(2, 4 * WM, CM)
        wc = w_col_in.transpose(0, 2, 3, 4, 1).reshape(2, 4 * WM, CM)
        wro = w_row_out.reshape(2, WM, CM)
        wco = w_col_out.reshape(2, WM, CM)
        wpi = w_opm_in.transpose(0, 2, 3, 1).reshape(2, 2 * OP, CM)
        wpo = w_opm_out.reshape(2, OP * OP, CZ)
        wsb = w_ts_bias.transpose(0, 2, 1)
        web = w_te_bias.transpose(0, 2, 1)
        ws = w_ts_in.transpose(0, 2, 4, 3, 1).reshape(2, 4 * WT, CZ)
        we = w_te_in.transpose(0, 2, 4, 3, 1).reshape(2, 4 * WT, CZ)
        wso = w_ts_out.transpose(0, 2, 1, 3).reshape(2, WT, CZ)
        weo = w_te_out.transpose(0, 2, 1, 3).reshape(2, WT, CZ)
        weights = [wb, wr, wro, wc, wco, wpi, wpo, wsb, ws, wso, web, we, weo]

        def vm(shape, dtype=BF16):
            return pltpu.VMEM(shape, dtype)
        scratch = [vm(w.shape) for w in weights]
        scratch += [vm((OP, OP, CZ)), vm((2, CZ, OP * OP)), vm((2, CZ, WP)), vm((2, CZ, WP))]
        scratch += [vm((H, R, R), F32), vm((HT, R, R), F32)]
        scratch += [vm((CZ, rl * R)), vm((rl, 4 * WP, R)), vm((2, WP, R)), vm((2, 4 * WP, CZ)), vm((2, 4 * WP, CZ))]
        scratch += [vm((sl // 2, 3 * WM, S)), vm((sl // 2, S, WM)), vm((WM, S))]
        scratch += [vm((sl, R, CM)), vm((rl, S, CM)), vm((rl, CZ, R)), vm((rl, R, CZ))]
        scratch += [vm((rl * OP, S))] * 4 + [vm((OP, R, S)), vm((OP * OP, rl * R))]
        scratch += [vm((S, R)), vm((sl, R), F32), vm((R, R), F32), vm((8, S), F32), vm((8, R), F32)]
        side = math.isqrt(n // 2)
        bias_row, bias_tri = (rl * H, R), (rl * HT, R)
        shapes = {'b1': bias_row, 'b2': bias_row, 's1': bias_tri, 'e1': bias_tri, 'e2': bias_tri, 's2': bias_tri,
                  'c': (rl * OP, S), 'a': (rl * OP, S), 'm1': (rl * sl // 2, CM), 'm2': (rl * sl // 2, CM), 'z1': (rl * rl, CZ), 'z2': (rl * rl, CZ)}
        for name in EXCHANGES:
            shape = shapes[name]
            if name in 'ac':
                scratch += [vm(shape), vm((side, side, 2) + shape)]
            elif name[0] == 'm':
                scratch += [vm((2, n) + shape), vm((2, n) + shape)]
            else:
                scratch += [vm((n,) + shape if name[0] == 'z' else shape), vm((n,) + shape)]
        scratch += [pltpu.SemaphoreType.DMA((len(FLOWS),)), pltpu.SemaphoreType.DMA((len(FLOWS),)), pltpu.SemaphoreType.DMA((len(weights),))]
        cfg = (n, sl, rl, S, R, CM, CZ, H, D, HT, DT, OP, HP)
        vmem = pl.BlockSpec(memory_space=pltpu.VMEM)
        hbm = pl.BlockSpec(memory_space=pl.ANY)
        m_new, z_new = pl.pallas_call(
            functools.partial(step_kernel, cfg),
            out_shape=[jax.ShapeDtypeStruct(m.shape, BF16), jax.ShapeDtypeStruct(zt.shape, BF16)],
            in_specs=[vmem] * 4 + [hbm] * len(weights),
            out_specs=[vmem, vmem],
            scratch_shapes=scratch,
            compiler_params=pltpu.CompilerParams(collective_id=0, has_side_effects=True, vmem_limit_bytes=60 * 2**20),
            name='evoformer',
        )(m, zt, mask, rmask.reshape(1, R), *weights)
        return m_new, z_new.transpose(0, 2, 1)

    in_specs = (P(('data', 'dap')), P(('data', 'dap')), P('data'), P('data')) + (P(),) * 13
    out_specs = (P(('data', 'dap')), P(('data', 'dap')))
    return jax.shard_map(local_step, mesh=mesh, in_specs=in_specs, out_specs=out_specs, check_vma=False)
```

```python
import functools
import math

import jax
import jax.numpy as jnp
from jax import lax
from jax.experimental import pallas as pl
from jax.experimental.pallas import tpu as pltpu
from jax.sharding import PartitionSpec as P

F32 = jnp.float32
BF16 = jnp.bfloat16
EPS = 1e-5
LOG2E = 1.4426950408889634
NEG = -1e9 * LOG2E
NN = (((1,), (0,)), ((), ()))
NT = (((1,), (1,)), ((), ()))
TN = (((0,), (0,)), ((), ()))
MESH = pl.DeviceIdType.MESH


def mm(a, b, dims=NN):
    return lax.dot_general(a, b, dims, preferred_element_type=F32)


def norm_axis(x, axis):
    mean = jnp.mean(x, axis=axis, keepdims=True)
    centered = x - mean
    var = jnp.mean(centered * centered, axis=axis, keepdims=True)
    return (centered * lax.rsqrt(var + EPS)).astype(BF16)


def one_hot(rows, cols, source):
    r = lax.broadcasted_iota(jnp.int32, (rows, cols), 0)
    c = lax.broadcasted_iota(jnp.int32, (rows, cols), 1)
    return jnp.where(c == source(r), 1.0, 0.0).astype(BF16)


def swap_matrix(a, b):
    return one_hot(a * b, a * b, lambda r: (r % a) * b + r // a)


def softmax_cols(t):
    e = jnp.exp2(t - jnp.max(t, axis=0, keepdims=True))
    return e.astype(BF16), 1.0 / jnp.sum(e, axis=0, keepdims=True)


EXCHANGES = ('b1', 'm1', 'c', 's1', 'z1', 'e1', 'b2', 'a', 'm2', 'e2', 'z2', 's2')
FLOWS = ('b1', 'm1_0', 'm1_1', 's1', 'z1', 'e1', 'b2', 'm2_0', 'm2_1', 'e2', 'z2', 's2',
         'c_a1', 'c_b1', 'c_a2', 'c_b2', 'c_t', 'a_a1', 'a_b1', 'a_a2', 'a_b2', 'a_t')
STRIDE = 13


def step_kernel(cfg, *refs):
    n, sl, rl, S, R, CM, CZ, H, D, HT, DT, OP, HP = cfg
    WM = H * D
    WT = HT * DT
    DP = -(-DT // 16) * 16
    WP = HT * DP
    side = math.isqrt(n // 2)
    chunk = rl * OP // 2
    it = iter(refs)
    (m_hbm, z_hbm, mask_hbm, rmask_hbm, wb_hbm, wr_hbm, wro_hbm, wc_hbm, wco_hbm, wpi_hbm, wpo_hbm,
     wsb_hbm, ws_hbm, wso_hbm, web_hbm, we_hbm, weo_hbm) = [next(it) for _ in range(17)]
    m_out, z_out = next(it), next(it)
    wb, wr, wro, wc, wco, wpi, wpo, wsb, ws, wso, web, we, weo = weights = [next(it) for _ in range(13)]
    wtmp, wpot, wsot, weot = [next(it) for _ in range(4)]
    bias_f, biast_f = next(it), next(it)
    xz, qkvg, gpair, wsp, wep = [next(it) for _ in range(5)]
    qvg, kbuf, gbuf = [next(it) for _ in range(3)]
    mrow, mcol, zb, znb = [next(it) for _ in range(4)]
    abuf, cbuf, abuf2, cbuf2, perm, obuf = [next(it) for _ in range(6)]
    mcolmask, seqmask, rmaskt, colmask, norm_ref = [next(it) for _ in range(5)]
    send = {}
    recv = {}
    for name in EXCHANGES:
        send[name] = next(it)
        recv[name] = next(it)
    send_sem, recv_sem, w_sem = next(it), next(it), next(it)
    m_ref, z_ref, mask_ref, rmask_ref, mfinal, in_sem = [next(it) for _ in range(6)]
    inputs = [pltpu.make_async_copy(src, dst, in_sem.at[i]) for i, (src, dst) in enumerate(
        [(mask_hbm, mask_ref), (rmask_hbm, rmask_ref), (z_hbm, z_ref), (m_hbm, m_ref)])]
    for load in inputs:
        load.start()
    hbm = [wb_hbm, wr_hbm, wro_hbm, wc_hbm, wco_hbm, wpi_hbm, wpo_hbm, wsb_hbm, ws_hbm, wso_hbm, web_hbm, we_hbm, weo_hbm]
    loads = [pltpu.make_async_copy(src, dst, w_sem.at[i]) for i, (src, dst) in enumerate(zip(hbm, weights))]
    for load in loads:
        load.start()
    (ld_wb, ld_wr, ld_wro, ld_wc, ld_wco, ld_wpi, ld_wpo, ld_wsb, ld_ws, ld_wso, ld_web, ld_we, ld_weo) = loads

    me = lax.axis_index('dap')
    barrier = pltpu.get_barrier_semaphore()

    @pl.loop(1, n)
    def _(k):
        pl.semaphore_signal(barrier, inc=1, device_id={'dap': lax.rem(me + k, n)}, device_id_type=MESH)

    core, px, py = me % 2, (me // 2) % side, me // (2 * side)

    def at(y, x, c):
        return {'dap': ((y % side) * side + x % side) * 2 + c % 2}

    def remote(flow, src, dst, device):
        f = FLOWS.index(flow)
        return pltpu.make_async_remote_copy(src_ref=src, dst_ref=dst, send_sem=send_sem.at[f], recv_sem=recv_sem.at[f], device_id=device, device_id_type=MESH)

    def wait_for(flow, sems, like):
        pltpu.make_async_copy(like, like, sems.at[FLOWS.index(flow)]).wait()

    def push(flow, src, dst, scatter):
        for k in range(1, n):
            peer = lax.rem(me + k * STRIDE % n, n)
            remote(flow, src.at[peer] if scatter else src, dst.at[me], {'dap': peer}).start()
        dst[me] = src[me] if scatter else src[...]

    def target(flow):
        if flow[0] == 'm':
            return recv[flow[:2]].at[int(flow[3])]
        return recv[flow]

    def like(flow):
        if flow[1] != '_':
            return target(flow).at[pl.ds(0, n - 1)]
        dst, part = recv[flow[0]], flow[2:]
        rows = slice(0, chunk)
        if part == 't':
            return dst.at[:, :, 0]
        if part[1] == '1':
            return dst.at[0, pl.ds(0, side - 1), 0, rows]
        return dst.at[pl.ds(0, side - 1), :, 0, rows]

    def arrived(flow):
        wait_for(flow, recv_sem, like(flow))

    def spread(name, half):
        rows = slice(half * chunk, (half + 1) * chunk)
        dst = recv[name]
        dst[py, px, core, rows] = send[name][rows]
        for d in range(1, side):
            device = at(py, px + d, core) if half == 0 else at(py + d, px, core)
            remote(name + '_' + 'ab'[half] + '1', send[name].at[rows], dst.at[py, px, core, rows], device).start()

    def relay(name, half):
        arrived(name + '_' + 'ab'[half] + '1')
        rows = slice(half * chunk, (half + 1) * chunk)
        dst = recv[name]
        for d in range(1, side):
            if half == 0:
                part, device = dst.at[py, :, core, rows], at(py + d, px, core)
            else:
                part, device = dst.at[:, px, core, rows], at(py, px + d, core)
            remote(name + '_' + 'ab'[half] + '2', part, part, device).start()

    def share(name):
        arrived(name + '_a2')
        arrived(name + '_b2')
        part = recv[name].at[:, :, core]
        remote(name + '_t', part, part, at(py, px, core + 1)).start()

    eye = one_hot(R, R, lambda r: r)

    def pair_norm(zref):
        for i in range(rl):
            xz[:, i * R:(i + 1) * R] = norm_axis(zref[i].astype(F32), 0)

    def bias_block(name, w, heads):
        bias_pack(name, w, heads)
        push(name, send[name], recv[name], False)

    def bias_pack(name, w, heads):
        got = mm(w, xz[...]).astype(BF16).astype(F32)
        got = jnp.concatenate([got[:, i * R:(i + 1) * R] for i in range(rl)], axis=0).astype(BF16)
        padded = w.shape[0]
        if padded != heads:
            pack = one_hot(rl * heads, rl * padded, lambda r: (r // heads) * padded + r % heads)
            got = mm(pack, got).astype(BF16)
        send[name][...] = got

    def bias_build(name, heads, group, dst, transpose):
        swap = swap_matrix(group * rl, heads)
        rows = group * rl

        for g in range(n // group):
            got = mm(swap, recv[name][g * group:(g + 1) * group].reshape(rows * heads, R)) * LOG2E
            for h in range(heads):
                dst[h, g * rows:(g + 1) * rows, :] = got[h * rows:(h + 1) * rows]
        if transpose:
            for h in range(heads):
                dst[h] = dst[h].T

    def pair_project(w):
        got = mm(w, xz[...])
        for i in range(rl):
            qkvg[i] = got[:, i * R:(i + 1) * R].astype(BF16)

    def pair_attend(zref, wo, dst):
        scale = DT ** -0.5 * LOG2E

        def row(i, u):
            def part(f, h):
                return qkvg[i, f * WP + h * DP:f * WP + (h + 1) * DP]

            def logits(h):
                return mm(part(1, h).astype(F32).T.astype(BF16), part(0, h))
            ahead = logits(0)
            for h in range(HT):
                t = ahead * scale + biast_f[h]
                if h + 1 < HT:
                    ahead = logits(h + 1)
                t = jnp.where(rmaskt[...] > 0, t, NEG)
                e, inverse = softmax_cols(t)
                o = mm(part(2, h), e) * inverse
                gpair[u, h * DP:(h + 1) * DP, :] = (o * jax.nn.sigmoid(part(3, h).astype(F32))).astype(BF16)
            dst[i] = (zref[i].astype(F32) + mm(wo, gpair[u])).astype(BF16)

        @pl.loop(0, rl // 2)
        def _(t):
            row(2 * t, 0)
            row(2 * t + 1, 1)

    def pair_send(name):
        for i in range(rl):
            znb[i] = zb[i].astype(F32).T.astype(BF16)
        swap = one_hot(4 * rl * rl, 4 * rl * rl, lambda r: (r % rl) * (4 * rl) + r // rl)
        width = 4 * rl

        for g in range(n // 4):
            got = znb[:, g * width:(g + 1) * width, :].reshape(rl * width, CZ)
            send[name][g * 4:(g + 1) * 4] = mm(swap, got).astype(BF16).reshape(4, rl * rl, CZ)
        push(name, send[name], recv[name], True)

    def pair_receive(name):
        rows = 8 * rl
        swap = one_hot(rows * rl, rows * rl, lambda r: ((r % rows) // rl) * (rl * rl) + (r // rows) * rl + r % rl)

        for g in range(n // 8):
            got = mm(swap, recv[name][g * 8:(g + 1) * 8].reshape(rows * rl, CZ)).astype(BF16)
            for i in range(rl):
                znb[i, g * rows:(g + 1) * rows, :] = got[i * rows:(i + 1) * rows]
        for i in range(rl):
            zb[i] = znb[i].astype(F32).T.astype(BF16)

    def outer_update(name, left, wo, zref, dst):
        swap = swap_matrix(4 * rl, 16)
        width = 4 * rl

        per_y = side // 2
        for g in range(n // 4):
            for half in range(OP // 16):
                got = recv[name][g // per_y, (g % per_y) * 2:(g % per_y) * 2 + 2].reshape(width, OP, S)[:, half * 16:(half + 1) * 16].reshape(width * 16, S)
                perm[half * 16:(half + 1) * 16, g * width:(g + 1) * width, :] = mm(swap, got).astype(BF16).reshape(16, width, S)
        for t in range(OP // 2):
            o = mm(left[...], perm[t * 2:t * 2 + 2].reshape(2 * R, S), NT).astype(BF16)
            for u in range(2):
                for i in range(rl):
                    obuf[(t * 2 + u) * OP:(t * 2 + u + 1) * OP, i * R:(i + 1) * R] = o[i * OP:(i + 1) * OP, u * R:(u + 1) * R]
        upd = mm(wo, obuf[...])
        for i in range(rl):
            dst[i] = (zref[i].astype(F32) + upd[:, i * R:(i + 1) * R] * (1.0 / (1e-3 + norm_ref[i:i + 1, :]))).astype(BF16)

    def row_bias_weight(b):
        got = wb[:, b, :].astype(F32)
        return jnp.concatenate([got, jnp.zeros((HP - H, CZ), F32)], axis=0).astype(BF16)

    def project(x, w, p):
        qvg[p, 0:WM] = mm(w[0:WM], x, NT).astype(BF16)
        kbuf[p] = mm(x, w[WM:2 * WM], NT).astype(BF16)
        qvg[p, WM:3 * WM] = mm(w[2 * WM:4 * WM], x, NT).astype(BF16)

    per_tile = 128 // D
    tile_lane = lax.broadcasted_iota(jnp.int32, (16, 128), 1) // D
    head_mask = [jnp.where(tile_lane == j, 1.0, 0.0).astype(BF16) for j in range(per_tile)]

    def attend(p, lo, size, mask, bias):
        scale = D ** -0.5 * LOG2E
        keys = slice(lo, lo + size)

        def query(h, q):
            j = h % per_tile
            parts = [qvg[p, h * D:(h + 1) * D, q:q + 128]]
            if j:
                parts.insert(0, jnp.zeros((j * D, 128), BF16))
            if j + 1 < per_tile:
                parts.append(jnp.zeros(((per_tile - 1 - j) * D, 128), BF16))
            return jnp.concatenate(parts, axis=0)

        def logits(group):
            h, q = group[0]
            tile = (h // per_tile) * 128
            if len(group) == 1:
                kt = kbuf[p, keys, tile:tile + 128].reshape(size // 16, 16, 128)
                kh = (kt * head_mask[h % per_tile][None]).reshape(size, 128)
                return mm(kh, qvg[p, tile:tile + 128, q:q + 128])
            return mm(kbuf[p, keys, tile:tile + 128], jnp.concatenate([query(h, q) for h, q in group], axis=1))
        blocks = [(h, q) for h in range(H) for q in range(lo, lo + size, 128)]
        step = size // 128
        groups = [blocks[b:b + step] for b in range(0, len(blocks), step)]
        ahead = logits(groups[0])
        for b, group in enumerate(groups):
            now = ahead
            if b + 1 < len(groups):
                ahead = logits(groups[b + 1])
            for u, (h, q) in enumerate(group):
                t = now[:, u * 128:(u + 1) * 128] * scale
                if bias is not None:
                    t = t + bias[h]
                t = jnp.where(mask > 0, t, NEG)
                e, inverse = softmax_cols(t)
                o = mm(qvg[p, WM + h * D:WM + (h + 1) * D, keys], e) * inverse
                g = qvg[p, 2 * WM + h * D:2 * WM + (h + 1) * D, q:q + 128].astype(F32)
                gbuf[h * D:(h + 1) * D, q:q + 128] = (o * jax.nn.sigmoid(g)).astype(BF16)

    def row_project(src, w):
        @pl.loop(0, sl // 2)
        def _(t):
            xf = src[pl.ds(2 * t, 2)].astype(F32).reshape(2 * R, CM)
            project(norm_axis(xf, 1), w, t)

    def row_attend(src, wo, bias, dst, lo, hi):
        @pl.loop(lo, hi)
        def _(t):
            for u in range(2):
                row = seqmask[pl.ds(2 * t + u, 1), :]
                mask = mm(eye, jnp.broadcast_to(row, (R, R)).astype(BF16), NT)
                attend(t, u * R, R, mask, bias)
            xf = src[pl.ds(2 * t, 2)].astype(F32).reshape(2 * R, CM)
            upd = mm(gbuf[...], wo[...], TN)
            dst[pl.ds(2 * t, 2)] = (xf + upd).astype(BF16).reshape(2, R, CM)

    def col_attention(load, w, wo, wp, a_dst, c_dst, after):
        @pl.loop(0, rl)
        def _(i):
            xf = load(i)
            project(norm_axis(xf, 1), w, 0)
            pick = jnp.where(lax.broadcasted_iota(jnp.int32, (R, R), 0) == me * rl + i, 1.0, 0.0).astype(BF16)
            attend(0, 0, S, mm(mcolmask[...], pick), None)
            y = (xf + mm(gbuf[...], wo[...], TN)).astype(BF16)
            mcol[i] = y
            x = norm_axis(y.astype(F32), 1)
            half = (mm(wp, x, NT) * colmask[pl.ds(i, 1), :]).astype(BF16)
            at = pl.ds(pl.multiple_of(i * OP, OP), OP)
            a_dst[at, :] = half[0:OP]
            c_dst[at, :] = half[OP:2 * OP]
            after(i)

    for load in inputs:
        load.wait()
    maskf = mask_ref[...].astype(F32).astype(BF16)
    mcolmask[...] = maskf
    seqmask[...] = mask_ref[pl.ds(pl.multiple_of(me * sl, sl), sl), :].astype(F32)
    rmaskt[...] = mm(eye, jnp.broadcast_to(rmask_ref[...].astype(F32), (R, R)).astype(BF16), NT)
    pick = jnp.where(lax.broadcasted_iota(jnp.int32, (8, R), 1) == lax.broadcasted_iota(jnp.int32, (8, R), 0) + me * rl, 1.0, 0.0).astype(BF16)
    colmask[...] = mm(pick, maskf, NT)
    norm_ref[...] = mm(colmask[...].astype(BF16), maskf)

    pair_norm(z_ref)
    ld_wb.wait()
    pl.semaphore_wait(barrier, n - 1)
    bias_block('b1', row_bias_weight(0), H)
    ld_wr.wait()
    row_project(m_ref, wr.at[0])
    ld_wro.wait()
    ld_wpo.wait()
    swap = swap_matrix(16, 16)
    for p in range(OP // 16):
        for q in range(OP // 16):
            got = wpo[0].reshape(OP, OP, CZ)[p * 16:(p + 1) * 16, q * 16:(q + 1) * 16].reshape(256, CZ)
            wtmp[q * 16:(q + 1) * 16, p * 16:(p + 1) * 16, :] = mm(swap, got).astype(BF16).reshape(16, 16, CZ)
    wpot[0] = wtmp[...].reshape(OP * OP, CZ).astype(F32).T.astype(BF16)
    wpot[1] = wpo[1].astype(F32).T.astype(BF16)
    arrived('b1')
    bias_build('b1', H, 8, bias_f, True)

    row_attend(m_ref, wro.at[0], bias_f, mrow, 0, sl // 2)

    per = 16 // rl
    split = one_hot(16 * sl, 16 * sl, lambda r: (r % sl) * 16 + ((r // (2 * sl)) % per) * rl + (r // (2 * sl * per)) * 2 + (r // sl) % 2)

    for g in range(R // 16):
        got = mm(split, mrow[:, g * 16:(g + 1) * 16, :].reshape(sl * 16, CM)).astype(BF16).reshape(2, per, 2 * sl, CM)
        for pair in range(2):
            send['m1'][pair, g * per:(g + 1) * per] = got[pair]
    for pair in range(2):
        push('m1_%d' % pair, send['m1'].at[pair], recv['m1'].at[pair], True)

    for load in (ld_wsb, ld_ws, ld_wso, ld_web, ld_we, ld_weo):
        load.wait()
    heads = one_hot(WP, WT, lambda r: jnp.where(r % DP < DT, (r % DP) * HT + r // DP, -1))
    for raw, out, turned, dst in ((ws, wso, wsp, wsot), (we, weo, wep, weot)):
        for b in range(2):
            for f in range(4):
                turned[b, f * WP:(f + 1) * WP] = mm(heads, raw[b, f * WT:(f + 1) * WT]).astype(BF16)
            dst[b] = mm(heads, out[b]).T.astype(BF16)

    ld_wc.wait()
    ld_wco.wait()
    ld_wpi.wait()
    arrived('m1_0')

    def load_first(i):
        pl.when(i == 2)(lambda: arrived('m1_1'))
        got = recv['m1'][i // 2].astype(F32)
        return jnp.where(i % 2 == 0, got[:, 0:sl], got[:, sl:2 * sl]).reshape(S, CM)

    def after_first(i):
        pl.when(i == rl // 2 - 1)(lambda: spread('c', 0))
    col_attention(load_first, wc.at[0], wco.at[0], wpi[0], abuf, send['c'], after_first)
    spread('c', 1)
    relay('c', 0)

    def send_cols(pair):
        got = [mcol[2 * pair + u].astype(F32).reshape(n, sl, CM) for u in range(2)]
        send['m2'][pair] = jnp.concatenate(got, axis=1).astype(BF16)
        push('m2_%d' % pair, send['m2'].at[pair], recv['m2'].at[pair], True)

    def after_second(i):
        @pl.when(i == 0)
        def _():
            relay('c', 1)

        @pl.when(i == 1)
        def _():
            spread('a', 0)
            send_cols(0)

        @pl.when(i == 2)
        def _():
            share('c')
    col_attention(lambda i: mcol[i].astype(F32), wc.at[1], wco.at[1], wpi[1], send['a'], cbuf2, after_second)
    spread('a', 1)

    arrived('c_t')
    outer_update('c', abuf, wpot[0], z_ref, zb)
    pair_norm(zb)
    bias_block('s1', wsb[0], HT)
    pair_project(wsp[0])
    arrived('s1')
    relay('a', 0)
    relay('a', 1)
    bias_build('s1', HT, 4, biast_f, True)
    pair_attend(zb, wsot[0], zb)
    pair_send('z1')
    pair_norm(zb)
    bias_block('e1', web[0], HT)
    share('a')
    arrived('z1')
    pair_receive('z1')
    pair_norm(zb)
    pair_project(wep[0])
    arrived('e1')
    send_cols(1)
    bias_build('e1', HT, 4, biast_f, False)
    pair_attend(zb, weot[0], zb)

    pair_norm(zb)
    bias_pack('b2', row_bias_weight(1), H)
    arrived('a_t')
    outer_update('a', cbuf2, wpot[1], zb, zb)
    pair_norm(zb)
    bias_block('e2', web[1], HT)
    push('b2', send['b2'], recv['b2'], False)
    pair_project(wep[1])
    arrived('m2_0')
    arrived('m2_1')
    unsplit = one_hot(16 * sl, 16 * sl, lambda r: ((r % 4) // 2) * (8 * sl) + ((r % 16) // 4) * (2 * sl) + (r % 2) * sl + r // 16)

    for g in range(R // 16):
        got = jnp.concatenate([recv['m2'][pair, g * per:(g + 1) * per].reshape(8 * sl, CM) for pair in range(2)], axis=0)
        mrow[:, g * 16:(g + 1) * 16, :] = mm(unsplit, got).astype(BF16).reshape(sl, 16, CM)
    row_project(mrow, wr.at[1])
    arrived('e2')
    bias_build('e2', HT, 4, biast_f, True)
    pair_attend(zb, weot[1], zb)
    pair_send('z2')
    pair_norm(zb)
    bias_block('s2', wsb[1], HT)
    arrived('b2')
    bias_build('b2', H, 8, bias_f, False)
    row_attend(mrow, wro.at[1], bias_f, mfinal, 0, sl // 2)
    store = pltpu.make_async_copy(mfinal, m_out, in_sem.at[0])
    store.start()
    arrived('z2')
    pair_receive('z2')
    pair_norm(zb)
    pair_project(wsp[1])
    arrived('s2')
    bias_build('s2', HT, 4, biast_f, False)
    pair_attend(zb, wsot[1], z_out)
    store.wait()
    for flow in FLOWS:
        wait_for(flow, send_sem, like(flow))


def solution(mesh):
    n = mesh.shape['dap']

    def local_step(m, z, mask, rmask, w_row_bias, w_row_in, w_row_out, w_col_in, w_col_out, w_opm_in, w_opm_out, w_ts_bias, w_ts_in, w_ts_out, w_te_bias, w_te_in, w_te_out):
        sl, R, CM = m.shape
        rl, _, CZ = z.shape
        S = mask.shape[0]
        H, D = w_row_in.shape[3:]
        HT, DT = w_ts_in.shape[3:]
        OP = w_opm_in.shape[3]
        HP = -(-H // 8) * 8
        WM, WT = H * D, HT * DT
        WP = HT * -(-DT // 16) * 16
        zt = z.transpose(0, 2, 1)
        wb = w_row_bias.transpose(2, 0, 1)
        wr = w_row_in.transpose(0, 2, 3, 4, 1).reshape(2, 4 * WM, CM)
        wc = w_col_in.transpose(0, 2, 3, 4, 1).reshape(2, 4 * WM, CM)
        wro = w_row_out.reshape(2, WM, CM)
        wco = w_col_out.reshape(2, WM, CM)
        wpi = w_opm_in.transpose(0, 2, 3, 1).reshape(2, 2 * OP, CM)
        wpo = w_opm_out.reshape(2, OP * OP, CZ)
        wsb = w_ts_bias.transpose(0, 2, 1)
        web = w_te_bias.transpose(0, 2, 1)
        ws = w_ts_in.transpose(0, 2, 4, 3, 1).reshape(2, 4 * WT, CZ)
        we = w_te_in.transpose(0, 2, 4, 3, 1).reshape(2, 4 * WT, CZ)
        wso = w_ts_out.transpose(0, 2, 1, 3).reshape(2, WT, CZ)
        weo = w_te_out.transpose(0, 2, 1, 3).reshape(2, WT, CZ)
        weights = [wb, wr, wro, wc, wco, wpi, wpo, wsb, ws, wso, web, we, weo]

        def vm(shape, dtype=BF16):
            return pltpu.VMEM(shape, dtype)
        scratch = [vm(w.shape) for w in weights]
        scratch += [vm((OP, OP, CZ)), vm((2, CZ, OP * OP)), vm((2, CZ, WP)), vm((2, CZ, WP))]
        scratch += [vm((H, R, R), F32), vm((HT, R, R), F32)]
        scratch += [vm((CZ, rl * R)), vm((rl, 4 * WP, R)), vm((2, WP, R)), vm((2, 4 * WP, CZ)), vm((2, 4 * WP, CZ))]
        scratch += [vm((sl // 2, 3 * WM, S)), vm((sl // 2, S, WM)), vm((WM, S))]
        scratch += [vm((sl, R, CM)), vm((rl, S, CM)), vm((rl, CZ, R)), vm((rl, R, CZ))]
        scratch += [vm((rl * OP, S))] * 4 + [vm((OP, R, S)), vm((OP * OP, rl * R))]
        scratch += [vm((S, R)), vm((sl, R), F32), vm((R, R), F32), vm((8, S), F32), vm((8, R), F32)]
        side = math.isqrt(n // 2)
        bias_row, bias_tri = (rl * H, R), (rl * HT, R)
        shapes = {'b1': bias_row, 'b2': bias_row, 's1': bias_tri, 'e1': bias_tri, 'e2': bias_tri, 's2': bias_tri,
                  'c': (rl * OP, S), 'a': (rl * OP, S), 'm1': (rl * sl // 2, CM), 'm2': (rl * sl // 2, CM), 'z1': (rl * rl, CZ), 'z2': (rl * rl, CZ)}
        for name in EXCHANGES:
            shape = shapes[name]
            if name in 'ac':
                scratch += [vm(shape), vm((side, side, 2) + shape)]
            elif name[0] == 'm':
                scratch += [vm((2, n) + shape), vm((2, n) + shape)]
            else:
                scratch += [vm((n,) + shape if name[0] == 'z' else shape), vm((n,) + shape)]
        scratch += [pltpu.SemaphoreType.DMA((len(FLOWS),)), pltpu.SemaphoreType.DMA((len(FLOWS),)), pltpu.SemaphoreType.DMA((len(weights),))]
        scratch += [vm(m.shape), vm(zt.shape), vm(mask.shape, mask.dtype), vm((1, R), rmask.dtype), vm(m.shape), pltpu.SemaphoreType.DMA((4,))]
        cfg = (n, sl, rl, S, R, CM, CZ, H, D, HT, DT, OP, HP)
        vmem = pl.BlockSpec(memory_space=pltpu.VMEM)
        hbm = pl.BlockSpec(memory_space=pl.ANY)
        m_new, z_new = pl.pallas_call(
            functools.partial(step_kernel, cfg),
            out_shape=[jax.ShapeDtypeStruct(m.shape, BF16), jax.ShapeDtypeStruct(zt.shape, BF16)],
            in_specs=[hbm] * (4 + len(weights)),
            out_specs=[hbm, vmem],
            scratch_shapes=scratch,
            compiler_params=pltpu.CompilerParams(collective_id=0, has_side_effects=True, vmem_limit_bytes=60 * 2**20),
            name='evoformer',
        )(m, zt, mask, rmask.reshape(1, R), *weights)
        return m_new, z_new.transpose(0, 2, 1)

    in_specs = (P(('data', 'dap')), P(('data', 'dap')), P('data'), P('data')) + (P(),) * 13
    out_specs = (P(('data', 'dap')), P(('data', 'dap')))
    return jax.shard_map(local_step, mesh=mesh, in_specs=in_specs, out_specs=out_specs, check_vma=False)
```

```python
import functools
import math

import jax
import jax.numpy as jnp
from jax import lax
from jax.experimental import pallas as pl
from jax.experimental.pallas import tpu as pltpu
from jax.sharding import PartitionSpec as P

F32 = jnp.float32
BF16 = jnp.bfloat16
EPS = 1e-5
LOG2E = 1.4426950408889634
NEG = -1e9 * LOG2E
NN = (((1,), (0,)), ((), ()))
NT = (((1,), (1,)), ((), ()))
TN = (((0,), (0,)), ((), ()))
MESH = pl.DeviceIdType.MESH


def mm(a, b, dims=NN):
    return lax.dot_general(a, b, dims, preferred_element_type=F32)


def norm_axis(x, axis):
    mean = jnp.mean(x, axis=axis, keepdims=True)
    centered = x - mean
    var = jnp.mean(centered * centered, axis=axis, keepdims=True)
    return (centered * lax.rsqrt(var + EPS)).astype(BF16)


def one_hot(rows, cols, source):
    r = lax.broadcasted_iota(jnp.int32, (rows, cols), 0)
    c = lax.broadcasted_iota(jnp.int32, (rows, cols), 1)
    return jnp.where(c == source(r), 1.0, 0.0).astype(BF16)


def swap_matrix(a, b):
    return one_hot(a * b, a * b, lambda r: (r % a) * b + r // a)


def softmax_cols(t):
    e = jnp.exp2(t - jnp.max(t, axis=0, keepdims=True))
    return e.astype(BF16), 1.0 / jnp.sum(e, axis=0, keepdims=True)


EXCHANGES = ('b1', 'm1', 'c', 's1', 'z1', 'e1', 'b2', 'a', 'm2', 'e2', 'z2', 's2')
FLOWS = ('b1', 'm1_0', 'm1_1', 's1', 'z1', 'e1', 'b2', 'm2_0', 'm2_1', 'e2', 'z2', 's2',
         'c_a1', 'c_b1', 'c_a2', 'c_b2', 'c_t', 'a_a1', 'a_b1', 'a_a2', 'a_b2', 'a_t')
STRIDE = 13


def step_kernel(cfg, *refs):
    n, sl, rl, S, R, CM, CZ, H, D, HT, DT, OP, HP = cfg
    WM = H * D
    WT = HT * DT
    DP = -(-DT // 16) * 16
    WP = HT * DP
    side = math.isqrt(n // 2)
    chunk = rl * OP // 2
    it = iter(refs)
    (m_hbm, z_hbm, mask_hbm, rmask_hbm, wb_hbm, wr_hbm, wro_hbm, wc_hbm, wco_hbm, wpi_hbm, wpo_hbm,
     wsb_hbm, ws_hbm, wso_hbm, web_hbm, we_hbm, weo_hbm) = [next(it) for _ in range(17)]
    m_out, z_out = next(it), next(it)
    wb, wr, wro, wc, wco, wpi, wpo, wsb, ws, wso, web, we, weo = weights = [next(it) for _ in range(13)]
    wtmp, wpot, wsot, weot = [next(it) for _ in range(4)]
    bias_f, biast_f = next(it), next(it)
    xz, qkvg, gpair, wsp, wep = [next(it) for _ in range(5)]
    qvg, kbuf, gbuf = [next(it) for _ in range(3)]
    mrow, mcol, zb, znb = [next(it) for _ in range(4)]
    abuf, cbuf, abuf2, cbuf2, perm, obuf = [next(it) for _ in range(6)]
    mcolmask, seqmask, rmaskt, colmask, norm_ref = [next(it) for _ in range(5)]
    send = {}
    recv = {}
    for name in EXCHANGES:
        send[name] = next(it)
        recv[name] = next(it)
    send_sem, recv_sem, w_sem = next(it), next(it), next(it)
    m_ref, z_ref, mask_ref, rmask_ref, mfinal, in_sem = [next(it) for _ in range(6)]
    inputs = [pltpu.make_async_copy(src, dst, in_sem.at[i]) for i, (src, dst) in enumerate(
        [(mask_hbm, mask_ref), (rmask_hbm, rmask_ref), (z_hbm, z_ref), (m_hbm, m_ref)])]
    for load in inputs:
        load.start()
    hbm = [wb_hbm, wr_hbm, wro_hbm, wc_hbm, wco_hbm, wpi_hbm, wpo_hbm, wsb_hbm, ws_hbm, wso_hbm, web_hbm, we_hbm, weo_hbm]
    loads = [pltpu.make_async_copy(src, dst, w_sem.at[i]) for i, (src, dst) in enumerate(zip(hbm, weights))]
    for load in loads:
        load.start()
    (ld_wb, ld_wr, ld_wro, ld_wc, ld_wco, ld_wpi, ld_wpo, ld_wsb, ld_ws, ld_wso, ld_web, ld_we, ld_weo) = loads

    me = lax.axis_index('dap')
    barrier = pltpu.get_barrier_semaphore()

    @pl.loop(1, n)
    def _(k):
        pl.semaphore_signal(barrier, inc=1, device_id={'dap': lax.rem(me + k, n)}, device_id_type=MESH)

    core, px, py = me % 2, (me // 2) % side, me // (2 * side)

    def at(y, x, c):
        return {'dap': ((y % side) * side + x % side) * 2 + c % 2}

    def remote(flow, src, dst, device):
        f = FLOWS.index(flow)
        return pltpu.make_async_remote_copy(src_ref=src, dst_ref=dst, send_sem=send_sem.at[f], recv_sem=recv_sem.at[f], device_id=device, device_id_type=MESH)

    def wait_for(flow, sems, like):
        pltpu.make_async_copy(like, like, sems.at[FLOWS.index(flow)]).wait()

    def push(flow, src, dst, scatter):
        @pl.loop(1, n)
        def _(k):
            peer = lax.rem(me + k * STRIDE, n)
            remote(flow, src.at[peer] if scatter else src, dst.at[me], {'dap': peer}).start()
        dst[me] = src[me] if scatter else src[...]

    def target(flow):
        if flow[0] == 'm':
            return recv[flow[:2]].at[int(flow[3])]
        return recv[flow]

    def like(flow):
        if flow[1] != '_':
            return target(flow).at[pl.ds(0, n - 1)]
        dst, part = recv[flow[0]], flow[2:]
        rows = slice(0, chunk)
        if part == 't':
            return dst.at[:, :, 0]
        if part[1] == '1':
            return dst.at[0, pl.ds(0, side - 1), 0, rows]
        return dst.at[pl.ds(0, side - 1), :, 0, rows]

    def arrived(flow):
        wait_for(flow, recv_sem, like(flow))

    def spread(name, half):
        rows = slice(half * chunk, (half + 1) * chunk)
        dst = recv[name]
        dst[py, px, core, rows] = send[name][rows]
        for d in range(1, side):
            device = at(py, px + d, core) if half == 0 else at(py + d, px, core)
            remote(name + '_' + 'ab'[half] + '1', send[name].at[rows], dst.at[py, px, core, rows], device).start()

    def relay(name, half):
        arrived(name + '_' + 'ab'[half] + '1')
        rows = slice(half * chunk, (half + 1) * chunk)
        dst = recv[name]
        for d in range(1, side):
            if half == 0:
                part, device = dst.at[py, :, core, rows], at(py + d, px, core)
            else:
                part, device = dst.at[:, px, core, rows], at(py, px + d, core)
            remote(name + '_' + 'ab'[half] + '2', part, part, device).start()

    def share(name):
        arrived(name + '_a2')
        arrived(name + '_b2')
        part = recv[name].at[:, :, core]
        remote(name + '_t', part, part, at(py, px, core + 1)).start()

    eye = one_hot(R, R, lambda r: r)

    def pair_norm(zref):
        for i in range(rl):
            xz[:, i * R:(i + 1) * R] = norm_axis(zref[i].astype(F32), 0)

    def bias_block(name, w, heads):
        bias_pack(name, w, heads)
        push(name, send[name], recv[name], False)

    def bias_pack(name, w, heads):
        got = mm(w, xz[...]).astype(BF16).astype(F32)
        got = jnp.concatenate([got[:, i * R:(i + 1) * R] for i in range(rl)], axis=0).astype(BF16)
        padded = w.shape[0]
        if padded != heads:
            pack = one_hot(rl * heads, rl * padded, lambda r: (r // heads) * padded + r % heads)
            got = mm(pack, got).astype(BF16)
        send[name][...] = got

    def bias_build(name, heads, group, dst, transpose):
        swap = swap_matrix(group * rl, heads)
        rows = group * rl

        for g in range(n // group):
            got = mm(swap, recv[name][g * group:(g + 1) * group].reshape(rows * heads, R)) * LOG2E
            for h in range(heads):
                dst[h, g * rows:(g + 1) * rows, :] = got[h * rows:(h + 1) * rows]
        if transpose:
            for h in range(heads):
                dst[h] = dst[h].T

    def pair_project(w):
        got = mm(w, xz[...])
        for i in range(rl):
            qkvg[i] = got[:, i * R:(i + 1) * R].astype(BF16)

    def pair_attend(zref, wo, dst):
        scale = DT ** -0.5 * LOG2E

        def row(i, u):
            def part(f, h):
                return qkvg[i, f * WP + h * DP:f * WP + (h + 1) * DP]

            def logits(h):
                return mm(part(1, h).astype(F32).T.astype(BF16), part(0, h))
            ahead = logits(0)
            for h in range(HT):
                t = ahead * scale + biast_f[h]
                if h + 1 < HT:
                    ahead = logits(h + 1)
                t = jnp.where(rmaskt[...] > 0, t, NEG)
                e, inverse = softmax_cols(t)
                o = mm(part(2, h), e) * inverse
                gpair[u, h * DP:(h + 1) * DP, :] = (o * jax.nn.sigmoid(part(3, h).astype(F32))).astype(BF16)
            dst[i] = (zref[i].astype(F32) + mm(wo, gpair[u])).astype(BF16)

        @pl.loop(0, rl // 2)
        def _(t):
            row(2 * t, 0)
            row(2 * t + 1, 1)

    def pair_send(name):
        for i in range(rl):
            znb[i] = zb[i].astype(F32).T.astype(BF16)
        swap = one_hot(4 * rl * rl, 4 * rl * rl, lambda r: (r % rl) * (4 * rl) + r // rl)
        width = 4 * rl

        for g in range(n // 4):
            got = znb[:, g * width:(g + 1) * width, :].reshape(rl * width, CZ)
            send[name][g * 4:(g + 1) * 4] = mm(swap, got).astype(BF16).reshape(4, rl * rl, CZ)
        push(name, send[name], recv[name], True)

    def pair_receive(name):
        rows = 8 * rl
        swap = one_hot(rows * rl, rows * rl, lambda r: ((r % rows) // rl) * (rl * rl) + (r // rows) * rl + r % rl)

        for g in range(n // 8):
            got = mm(swap, recv[name][g * 8:(g + 1) * 8].reshape(rows * rl, CZ)).astype(BF16)
            for i in range(rl):
                znb[i, g * rows:(g + 1) * rows, :] = got[i * rows:(i + 1) * rows]
        for i in range(rl):
            zb[i] = znb[i].astype(F32).T.astype(BF16)

    def outer_update(name, left, wo, zref, dst):
        swap = swap_matrix(4 * rl, 16)
        width = 4 * rl

        per_y = side // 2
        for g in range(n // 4):
            for half in range(OP // 16):
                got = recv[name][g // per_y, (g % per_y) * 2:(g % per_y) * 2 + 2].reshape(width, OP, S)[:, half * 16:(half + 1) * 16].reshape(width * 16, S)
                perm[half * 16:(half + 1) * 16, g * width:(g + 1) * width, :] = mm(swap, got).astype(BF16).reshape(16, width, S)
        for t in range(OP // 2):
            o = mm(left[...], perm[t * 2:t * 2 + 2].reshape(2 * R, S), NT).astype(BF16)
            for u in range(2):
                for i in range(rl):
                    obuf[(t * 2 + u) * OP:(t * 2 + u + 1) * OP, i * R:(i + 1) * R] = o[i * OP:(i + 1) * OP, u * R:(u + 1) * R]
        upd = mm(wo, obuf[...])
        for i in range(rl):
            dst[i] = (zref[i].astype(F32) + upd[:, i * R:(i + 1) * R] * (1.0 / (1e-3 + norm_ref[i:i + 1, :]))).astype(BF16)

    def row_bias_weight(b):
        got = wb[:, b, :].astype(F32)
        return jnp.concatenate([got, jnp.zeros((HP - H, CZ), F32)], axis=0).astype(BF16)

    def project(x, w, p):
        qvg[p, 0:WM] = mm(w[0:WM], x, NT).astype(BF16)
        kbuf[p] = mm(x, w[WM:2 * WM], NT).astype(BF16)
        qvg[p, WM:3 * WM] = mm(w[2 * WM:4 * WM], x, NT).astype(BF16)

    per_tile = 128 // D
    tile_lane = lax.broadcasted_iota(jnp.int32, (16, 128), 1) // D
    head_mask = [jnp.where(tile_lane == j, 1.0, 0.0).astype(BF16) for j in range(per_tile)]

    def attend(p, lo, size, mask, bias):
        scale = D ** -0.5 * LOG2E
        keys = slice(lo, lo + size)

        def query(h, q):
            j = h % per_tile
            parts = [qvg[p, h * D:(h + 1) * D, q:q + 128]]
            if j:
                parts.insert(0, jnp.zeros((j * D, 128), BF16))
            if j + 1 < per_tile:
                parts.append(jnp.zeros(((per_tile - 1 - j) * D, 128), BF16))
            return jnp.concatenate(parts, axis=0)

        def logits(group):
            h, q = group[0]
            tile = (h // per_tile) * 128
            if len(group) == 1:
                kt = kbuf[p, keys, tile:tile + 128].reshape(size // 16, 16, 128)
                kh = (kt * head_mask[h % per_tile][None]).reshape(size, 128)
                return mm(kh, qvg[p, tile:tile + 128, q:q + 128])
            return mm(kbuf[p, keys, tile:tile + 128], jnp.concatenate([query(h, q) for h, q in group], axis=1))
        blocks = [(h, q) for h in range(H) for q in range(lo, lo + size, 128)]
        step = size // 128
        groups = [blocks[b:b + step] for b in range(0, len(blocks), step)]
        ahead = logits(groups[0])
        for b, group in enumerate(groups):
            now = ahead
            if b + 1 < len(groups):
                ahead = logits(groups[b + 1])
            for u, (h, q) in enumerate(group):
                t = now[:, u * 128:(u + 1) * 128] * scale
                if bias is not None:
                    t = t + bias[h]
                t = jnp.where(mask > 0, t, NEG)
                e, inverse = softmax_cols(t)
                o = mm(qvg[p, WM + h * D:WM + (h + 1) * D, keys], e) * inverse
                g = qvg[p, 2 * WM + h * D:2 * WM + (h + 1) * D, q:q + 128].astype(F32)
                gbuf[h * D:(h + 1) * D, q:q + 128] = (o * jax.nn.sigmoid(g)).astype(BF16)

    def row_project(src, w):
        @pl.loop(0, sl // 2)
        def _(t):
            xf = src[pl.ds(2 * t, 2)].astype(F32).reshape(2 * R, CM)
            project(norm_axis(xf, 1), w, t)

    def row_attend(src, wo, bias, dst, lo, hi):
        @pl.loop(lo, hi)
        def _(t):
            for u in range(2):
                row = seqmask[pl.ds(2 * t + u, 1), :]
                mask = mm(eye, jnp.broadcast_to(row, (R, R)).astype(BF16), NT)
                attend(t, u * R, R, mask, bias)
            xf = src[pl.ds(2 * t, 2)].astype(F32).reshape(2 * R, CM)
            upd = mm(gbuf[...], wo[...], TN)
            dst[pl.ds(2 * t, 2)] = (xf + upd).astype(BF16).reshape(2, R, CM)

    def col_attention(load, w, wo, wp, a_dst, c_dst, after):
        @pl.loop(0, rl)
        def _(i):
            xf = load(i)
            project(norm_axis(xf, 1), w, 0)
            pick = jnp.where(lax.broadcasted_iota(jnp.int32, (R, R), 0) == me * rl + i, 1.0, 0.0).astype(BF16)
            attend(0, 0, S, mm(mcolmask[...], pick), None)
            y = (xf + mm(gbuf[...], wo[...], TN)).astype(BF16)
            mcol[i] = y
            x = norm_axis(y.astype(F32), 1)
            half = (mm(wp, x, NT) * colmask[pl.ds(i, 1), :]).astype(BF16)
            at = pl.ds(pl.multiple_of(i * OP, OP), OP)
            a_dst[at, :] = half[0:OP]
            c_dst[at, :] = half[OP:2 * OP]
            after(i)

    for load in inputs:
        load.wait()
    maskf = mask_ref[...].astype(F32).astype(BF16)
    mcolmask[...] = maskf
    seqmask[...] = mask_ref[pl.ds(pl.multiple_of(me * sl, sl), sl), :].astype(F32)
    rmaskt[...] = mm(eye, jnp.broadcast_to(rmask_ref[...].astype(F32), (R, R)).astype(BF16), NT)
    pick = jnp.where(lax.broadcasted_iota(jnp.int32, (8, R), 1) == lax.broadcasted_iota(jnp.int32, (8, R), 0) + me * rl, 1.0, 0.0).astype(BF16)
    colmask[...] = mm(pick, maskf, NT)
    norm_ref[...] = mm(colmask[...].astype(BF16), maskf)

    pair_norm(z_ref)
    ld_wb.wait()
    pl.semaphore_wait(barrier, n - 1)
    bias_block('b1', row_bias_weight(0), H)
    ld_wr.wait()
    row_project(m_ref, wr.at[0])
    ld_wro.wait()
    ld_wpo.wait()
    swap = swap_matrix(16, 16)
    for p in range(OP // 16):
        for q in range(OP // 16):
            got = wpo[0].reshape(OP, OP, CZ)[p * 16:(p + 1) * 16, q * 16:(q + 1) * 16].reshape(256, CZ)
            wtmp[q * 16:(q + 1) * 16, p * 16:(p + 1) * 16, :] = mm(swap, got).astype(BF16).reshape(16, 16, CZ)
    wpot[0] = wtmp[...].reshape(OP * OP, CZ).astype(F32).T.astype(BF16)
    wpot[1] = wpo[1].astype(F32).T.astype(BF16)
    arrived('b1')
    bias_build('b1', H, 8, bias_f, True)

    row_attend(m_ref, wro.at[0], bias_f, mrow, 0, sl // 2)

    per = 16 // rl
    split = one_hot(16 * sl, 16 * sl, lambda r: (r % sl) * 16 + ((r // (2 * sl)) % per) * rl + (r // (2 * sl * per)) * 2 + (r // sl) % 2)

    for g in range(R // 16):
        got = mm(split, mrow[:, g * 16:(g + 1) * 16, :].reshape(sl * 16, CM)).astype(BF16).reshape(2, per, 2 * sl, CM)
        for pair in range(2):
            send['m1'][pair, g * per:(g + 1) * per] = got[pair]
    for pair in range(2):
        push('m1_%d' % pair, send['m1'].at[pair], recv['m1'].at[pair], True)

    for load in (ld_wsb, ld_ws, ld_wso, ld_web, ld_we, ld_weo):
        load.wait()
    heads = one_hot(WP, WT, lambda r: jnp.where(r % DP < DT, (r % DP) * HT + r // DP, -1))
    for raw, out, turned, dst in ((ws, wso, wsp, wsot), (we, weo, wep, weot)):
        for b in range(2):
            for f in range(4):
                turned[b, f * WP:(f + 1) * WP] = mm(heads, raw[b, f * WT:(f + 1) * WT]).astype(BF16)
            dst[b] = mm(heads, out[b]).T.astype(BF16)

    ld_wc.wait()
    ld_wco.wait()
    ld_wpi.wait()
    arrived('m1_0')

    def load_first(i):
        pl.when(i == 2)(lambda: arrived('m1_1'))
        got = recv['m1'][i // 2].astype(F32)
        return jnp.where(i % 2 == 0, got[:, 0:sl], got[:, sl:2 * sl]).reshape(S, CM)

    def after_first(i):
        pl.when(i == rl // 2 - 1)(lambda: spread('c', 0))
    col_attention(load_first, wc.at[0], wco.at[0], wpi[0], abuf, send['c'], after_first)
    spread('c', 1)
    relay('c', 0)

    def send_cols(pair):
        got = [mcol[2 * pair + u].astype(F32).reshape(n, sl, CM) for u in range(2)]
        send['m2'][pair] = jnp.concatenate(got, axis=1).astype(BF16)
        push('m2_%d' % pair, send['m2'].at[pair], recv['m2'].at[pair], True)

    def after_second(i):
        @pl.when(i == 0)
        def _():
            relay('c', 1)

        @pl.when(i == 1)
        def _():
            spread('a', 0)
            send_cols(0)

        @pl.when(i == 2)
        def _():
            share('c')
    col_attention(lambda i: mcol[i].astype(F32), wc.at[1], wco.at[1], wpi[1], send['a'], cbuf2, after_second)
    spread('a', 1)

    arrived('c_t')
    outer_update('c', abuf, wpot[0], z_ref, zb)
    pair_norm(zb)
    bias_block('s1', wsb[0], HT)
    pair_project(wsp[0])
    arrived('s1')
    relay('a', 0)
    relay('a', 1)
    bias_build('s1', HT, 4, biast_f, True)
    pair_attend(zb, wsot[0], zb)
    pair_send('z1')
    pair_norm(zb)
    bias_block('e1', web[0], HT)
    share('a')
    arrived('z1')
    pair_receive('z1')
    pair_norm(zb)
    pair_project(wep[0])
    arrived('e1')
    send_cols(1)
    bias_build('e1', HT, 4, biast_f, False)
    pair_attend(zb, weot[0], zb)

    pair_norm(zb)
    bias_pack('b2', row_bias_weight(1), H)
    arrived('a_t')
    outer_update('a', cbuf2, wpot[1], zb, zb)
    pair_norm(zb)
    bias_block('e2', web[1], HT)
    push('b2', send['b2'], recv['b2'], False)
    pair_project(wep[1])
    arrived('m2_0')
    arrived('m2_1')
    unsplit = one_hot(16 * sl, 16 * sl, lambda r: ((r % 4) // 2) * (8 * sl) + ((r % 16) // 4) * (2 * sl) + (r % 2) * sl + r // 16)

    for g in range(R // 16):
        got = jnp.concatenate([recv['m2'][pair, g * per:(g + 1) * per].reshape(8 * sl, CM) for pair in range(2)], axis=0)
        mrow[:, g * 16:(g + 1) * 16, :] = mm(unsplit, got).astype(BF16).reshape(sl, 16, CM)
    row_project(mrow, wr.at[1])
    arrived('e2')
    bias_build('e2', HT, 4, biast_f, True)
    pair_attend(zb, weot[1], zb)
    pair_send('z2')
    pair_norm(zb)
    bias_block('s2', wsb[1], HT)
    arrived('b2')
    bias_build('b2', H, 8, bias_f, False)
    row_attend(mrow, wro.at[1], bias_f, mfinal, 0, sl // 2)
    store = pltpu.make_async_copy(mfinal, m_out, in_sem.at[0])
    store.start()
    arrived('z2')
    pair_receive('z2')
    pair_norm(zb)
    pair_project(wsp[1])
    arrived('s2')
    bias_build('s2', HT, 4, biast_f, False)
    pair_attend(zb, wsot[1], z_out)
    store.wait()
    for flow in FLOWS:
        wait_for(flow, send_sem, like(flow))


def solution(mesh):
    n = mesh.shape['dap']

    def local_step(m, z, mask, rmask, w_row_bias, w_row_in, w_row_out, w_col_in, w_col_out, w_opm_in, w_opm_out, w_ts_bias, w_ts_in, w_ts_out, w_te_bias, w_te_in, w_te_out):
        sl, R, CM = m.shape
        rl, _, CZ = z.shape
        S = mask.shape[0]
        H, D = w_row_in.shape[3:]
        HT, DT = w_ts_in.shape[3:]
        OP = w_opm_in.shape[3]
        HP = -(-H // 8) * 8
        WM, WT = H * D, HT * DT
        WP = HT * -(-DT // 16) * 16
        zt = z.transpose(0, 2, 1)
        wb = w_row_bias.transpose(2, 0, 1)
        wr = w_row_in.transpose(0, 2, 3, 4, 1).reshape(2, 4 * WM, CM)
        wc = w_col_in.transpose(0, 2, 3, 4, 1).reshape(2, 4 * WM, CM)
        wro = w_row_out.reshape(2, WM, CM)
        wco = w_col_out.reshape(2, WM, CM)
        wpi = w_opm_in.transpose(0, 2, 3, 1).reshape(2, 2 * OP, CM)
        wpo = w_opm_out.reshape(2, OP * OP, CZ)
        wsb = w_ts_bias.transpose(0, 2, 1)
        web = w_te_bias.transpose(0, 2, 1)
        ws = w_ts_in.transpose(0, 2, 4, 3, 1).reshape(2, 4 * WT, CZ)
        we = w_te_in.transpose(0, 2, 4, 3, 1).reshape(2, 4 * WT, CZ)
        wso = w_ts_out.transpose(0, 2, 1, 3).reshape(2, WT, CZ)
        weo = w_te_out.transpose(0, 2, 1, 3).reshape(2, WT, CZ)
        weights = [wb, wr, wro, wc, wco, wpi, wpo, wsb, ws, wso, web, we, weo]

        def vm(shape, dtype=BF16):
            return pltpu.VMEM(shape, dtype)
        scratch = [vm(w.shape) for w in weights]
        scratch += [vm((OP, OP, CZ)), vm((2, CZ, OP * OP)), vm((2, CZ, WP)), vm((2, CZ, WP))]
        scratch += [vm((H, R, R), F32), vm((HT, R, R), F32)]
        scratch += [vm((CZ, rl * R)), vm((rl, 4 * WP, R)), vm((2, WP, R)), vm((2, 4 * WP, CZ)), vm((2, 4 * WP, CZ))]
        scratch += [vm((sl // 2, 3 * WM, S)), vm((sl // 2, S, WM)), vm((WM, S))]
        scratch += [vm((sl, R, CM)), vm((rl, S, CM)), vm((rl, CZ, R)), vm((rl, R, CZ))]
        scratch += [vm((rl * OP, S))] * 4 + [vm((OP, R, S)), vm((OP * OP, rl * R))]
        scratch += [vm((S, R)), vm((sl, R), F32), vm((R, R), F32), vm((8, S), F32), vm((8, R), F32)]
        side = math.isqrt(n // 2)
        bias_row, bias_tri = (rl * H, R), (rl * HT, R)
        shapes = {'b1': bias_row, 'b2': bias_row, 's1': bias_tri, 'e1': bias_tri, 'e2': bias_tri, 's2': bias_tri,
                  'c': (rl * OP, S), 'a': (rl * OP, S), 'm1': (rl * sl // 2, CM), 'm2': (rl * sl // 2, CM), 'z1': (rl * rl, CZ), 'z2': (rl * rl, CZ)}
        for name in EXCHANGES:
            shape = shapes[name]
            if name in 'ac':
                scratch += [vm(shape), vm((side, side, 2) + shape)]
            elif name[0] == 'm':
                scratch += [vm((2, n) + shape), vm((2, n) + shape)]
            else:
                scratch += [vm((n,) + shape if name[0] == 'z' else shape), vm((n,) + shape)]
        scratch += [pltpu.SemaphoreType.DMA((len(FLOWS),)), pltpu.SemaphoreType.DMA((len(FLOWS),)), pltpu.SemaphoreType.DMA((len(weights),))]
        scratch += [vm(m.shape), vm(zt.shape), vm(mask.shape, mask.dtype), vm((1, R), rmask.dtype), vm(m.shape), pltpu.SemaphoreType.DMA((4,))]
        cfg = (n, sl, rl, S, R, CM, CZ, H, D, HT, DT, OP, HP)
        vmem = pl.BlockSpec(memory_space=pltpu.VMEM)
        hbm = pl.BlockSpec(memory_space=pl.ANY)
        m_new, z_new = pl.pallas_call(
            functools.partial(step_kernel, cfg),
            out_shape=[jax.ShapeDtypeStruct(m.shape, BF16), jax.ShapeDtypeStruct(zt.shape, BF16)],
            in_specs=[hbm] * (4 + len(weights)),
            out_specs=[hbm, vmem],
            scratch_shapes=scratch,
            compiler_params=pltpu.CompilerParams(collective_id=0, has_side_effects=True, vmem_limit_bytes=60 * 2**20),
            name='evoformer',
        )(m, zt, mask, rmask.reshape(1, R), *weights)
        return m_new, z_new.transpose(0, 2, 1)

    in_specs = (P(('data', 'dap')), P(('data', 'dap')), P('data'), P('data')) + (P(),) * 13
    out_specs = (P(('data', 'dap')), P(('data', 'dap')))
    return jax.shard_map(local_step, mesh=mesh, in_specs=in_specs, out_specs=out_specs, check_vma=False)
```

```python
import functools
import math

import jax
import jax.numpy as jnp
from jax import lax
from jax.experimental import pallas as pl
from jax.experimental.pallas import tpu as pltpu
from jax.sharding import PartitionSpec as P

F32 = jnp.float32
BF16 = jnp.bfloat16
EPS = 1e-5
LOG2E = 1.4426950408889634
NEG = -1e9 * LOG2E
NN = (((1,), (0,)), ((), ()))
NT = (((1,), (1,)), ((), ()))
TN = (((0,), (0,)), ((), ()))
MESH = pl.DeviceIdType.MESH


def mm(a, b, dims=NN):
    return lax.dot_general(a, b, dims, preferred_element_type=F32)


def norm_axis(x, axis):
    mean = jnp.mean(x, axis=axis, keepdims=True)
    centered = x - mean
    var = jnp.mean(centered * centered, axis=axis, keepdims=True)
    return (centered * lax.rsqrt(var + EPS)).astype(BF16)


def one_hot(rows, cols, source):
    r = lax.broadcasted_iota(jnp.int32, (rows, cols), 0)
    c = lax.broadcasted_iota(jnp.int32, (rows, cols), 1)
    return jnp.where(c == source(r), 1.0, 0.0).astype(BF16)


def swap_matrix(a, b):
    return one_hot(a * b, a * b, lambda r: (r % a) * b + r // a)


def softmax_cols(t):
    e = jnp.exp2(t - jnp.max(t, axis=0, keepdims=True))
    return e.astype(BF16), 1.0 / jnp.sum(e, axis=0, keepdims=True)


EXCHANGES = ('b1', 'm1', 'c', 's1', 'z1', 'e1', 'b2', 'a', 'm2', 'e2', 'z2', 's2')
FLOWS = ('b1', 'm1_0', 'm1_1', 's1', 'z1', 'e1', 'b2', 'm2_0', 'm2_1', 'e2', 'z2', 's2',
         'c_a1', 'c_b1', 'c_a2', 'c_b2', 'c_t', 'a_a1', 'a_b1', 'a_a2', 'a_b2', 'a_t')
STRIDE = 13


def step_kernel(cfg, *refs):
    n, sl, rl, S, R, CM, CZ, H, D, HT, DT, OP, HP = cfg
    WM = H * D
    WT = HT * DT
    DP = -(-DT // 16) * 16
    WP = HT * DP
    side = math.isqrt(n // 2)
    chunk = rl * OP // 2
    it = iter(refs)
    (m_hbm, z_hbm, mask_hbm, rmask_hbm, wb_hbm, wr_hbm, wro_hbm, wc_hbm, wco_hbm, wpi_hbm, wpo_hbm,
     wsb_hbm, ws_hbm, wso_hbm, web_hbm, we_hbm, weo_hbm) = [next(it) for _ in range(17)]
    m_out, z_out = next(it), next(it)
    wb, wr, wro, wc, wco, wpi, wpo, wsb, ws, wso, web, we, weo = weights = [next(it) for _ in range(13)]
    wtmp, wpot, wsot, weot = [next(it) for _ in range(4)]
    bias_f, biast_f = next(it), next(it)
    xz, qkvg, gpair, wsp, wep = [next(it) for _ in range(5)]
    qvg, kbuf, gbuf = [next(it) for _ in range(3)]
    mrow, mcol, zb, znb = [next(it) for _ in range(4)]
    abuf, cbuf, abuf2, cbuf2, perm, obuf = [next(it) for _ in range(6)]
    mcolmask, seqmask, rmaskt, colmask, norm_ref = [next(it) for _ in range(5)]
    send = {}
    recv = {}
    for name in EXCHANGES:
        send[name] = next(it)
        recv[name] = next(it)
    send_sem, recv_sem, w_sem = next(it), next(it), next(it)
    m_ref, z_ref, mask_ref, rmask_ref, mfinal, in_sem = [next(it) for _ in range(6)]
    inputs = [pltpu.make_async_copy(src, dst, in_sem.at[i]) for i, (src, dst) in enumerate(
        [(mask_hbm, mask_ref), (rmask_hbm, rmask_ref), (z_hbm, z_ref), (m_hbm, m_ref)])]
    for load in inputs:
        load.start()
    hbm = [wb_hbm, wr_hbm, wro_hbm, wc_hbm, wco_hbm, wpi_hbm, wpo_hbm, wsb_hbm, ws_hbm, wso_hbm, web_hbm, we_hbm, weo_hbm]
    loads = [pltpu.make_async_copy(src, dst, w_sem.at[i]) for i, (src, dst) in enumerate(zip(hbm, weights))]
    for load in loads:
        load.start()
    (ld_wb, ld_wr, ld_wro, ld_wc, ld_wco, ld_wpi, ld_wpo, ld_wsb, ld_ws, ld_wso, ld_web, ld_we, ld_weo) = loads

    me = lax.axis_index('dap')
    barrier = pltpu.get_barrier_semaphore()

    @pl.loop(1, n)
    def _(k):
        pl.semaphore_signal(barrier, inc=1, device_id={'dap': lax.rem(me + k, n)}, device_id_type=MESH)

    core, px, py = me % 2, (me // 2) % side, me // (2 * side)

    def at(y, x, c):
        return {'dap': ((y % side) * side + x % side) * 2 + c % 2}

    def remote(flow, src, dst, device):
        f = FLOWS.index(flow)
        return pltpu.make_async_remote_copy(src_ref=src, dst_ref=dst, send_sem=send_sem.at[f], recv_sem=recv_sem.at[f], device_id=device, device_id_type=MESH)

    def wait_for(flow, sems, like):
        pltpu.make_async_copy(like, like, sems.at[FLOWS.index(flow)]).wait()

    def push(flow, src, dst, scatter):
        @pl.loop(1, n)
        def _(k):
            peer = lax.rem(me + k * STRIDE, n)
            remote(flow, src.at[peer] if scatter else src, dst.at[me], {'dap': peer}).start()
        dst[me] = src[me] if scatter else src[...]

    def target(flow):
        if flow[0] == 'm':
            return recv[flow[:2]].at[int(flow[3])]
        return recv[flow]

    def like(flow):
        if flow[1] != '_':
            return target(flow).at[pl.ds(0, n - 1)]
        dst, part = recv[flow[0]], flow[2:]
        rows = slice(0, chunk)
        if part == 't':
            return dst.at[:, :, 0]
        if part[1] == '1':
            return dst.at[0, pl.ds(0, side - 1), 0, rows]
        return dst.at[pl.ds(0, side - 1), :, 0, rows]

    def arrived(flow):
        wait_for(flow, recv_sem, like(flow))

    def spread(name, half):
        rows = slice(half * chunk, (half + 1) * chunk)
        dst = recv[name]
        dst[py, px, core, rows] = send[name][rows]
        for d in range(1, side):
            device = at(py, px + d, core) if half == 0 else at(py + d, px, core)
            remote(name + '_' + 'ab'[half] + '1', send[name].at[rows], dst.at[py, px, core, rows], device).start()

    def relay(name, half):
        arrived(name + '_' + 'ab'[half] + '1')
        rows = slice(half * chunk, (half + 1) * chunk)
        dst = recv[name]
        for d in range(1, side):
            if half == 0:
                part, device = dst.at[py, :, core, rows], at(py + d, px, core)
            else:
                part, device = dst.at[:, px, core, rows], at(py, px + d, core)
            remote(name + '_' + 'ab'[half] + '2', part, part, device).start()

    def share(name):
        arrived(name + '_a2')
        arrived(name + '_b2')
        part = recv[name].at[:, :, core]
        remote(name + '_t', part, part, at(py, px, core + 1)).start()

    eye = one_hot(R, R, lambda r: r)

    def pair_norm(zref):
        for i in range(rl):
            xz[:, i * R:(i + 1) * R] = norm_axis(zref[i].astype(F32), 0)

    def bias_block(name, w, heads):
        bias_pack(name, w, heads)
        push(name, send[name], recv[name], False)

    def bias_pack(name, w, heads):
        got = mm(w, xz[...]).astype(BF16).astype(F32)
        got = jnp.concatenate([got[:, i * R:(i + 1) * R] for i in range(rl)], axis=0).astype(BF16)
        padded = w.shape[0]
        if padded != heads:
            pack = one_hot(rl * heads, rl * padded, lambda r: (r // heads) * padded + r % heads)
            got = mm(pack, got).astype(BF16)
        send[name][...] = got

    def bias_build(name, heads, group, dst, transpose):
        swap = swap_matrix(group * rl, heads)
        rows = group * rl

        for g in range(n // group):
            got = mm(swap, recv[name][g * group:(g + 1) * group].reshape(rows * heads, R)) * LOG2E
            for h in range(heads):
                dst[h, g * rows:(g + 1) * rows, :] = got[h * rows:(h + 1) * rows]
        if transpose:
            for h in range(heads):
                dst[h] = dst[h].T

    def pair_project(w):
        got = mm(w, xz[...])
        for i in range(rl):
            qkvg[i] = got[:, i * R:(i + 1) * R].astype(BF16)

    def pair_attend(zref, wo, dst):
        scale = DT ** -0.5 * LOG2E

        def row(i, u):
            def part(f, h):
                return qkvg[i, f * WP + h * DP:f * WP + (h + 1) * DP]

            def logits(h):
                return mm(part(1, h).astype(F32).T.astype(BF16), part(0, h))
            ahead = logits(0)
            for h in range(HT):
                t = ahead * scale + biast_f[h]
                if h + 1 < HT:
                    ahead = logits(h + 1)
                t = jnp.where(rmaskt[...] > 0, t, NEG)
                e, inverse = softmax_cols(t)
                o = mm(part(2, h), e) * inverse
                gpair[u, h * DP:(h + 1) * DP, :] = (o * jax.nn.sigmoid(part(3, h).astype(F32))).astype(BF16)
            dst[i] = (zref[i].astype(F32) + mm(wo, gpair[u])).astype(BF16)

        @pl.loop(0, rl // 2)
        def _(t):
            row(2 * t, 0)
            row(2 * t + 1, 1)

    def pair_send(name):
        for i in range(rl):
            znb[i] = zb[i].astype(F32).T.astype(BF16)
        swap = one_hot(4 * rl * rl, 4 * rl * rl, lambda r: (r % rl) * (4 * rl) + r // rl)
        width = 4 * rl

        for g in range(n // 4):
            got = znb[:, g * width:(g + 1) * width, :].reshape(rl * width, CZ)
            send[name][g * 4:(g + 1) * 4] = mm(swap, got).astype(BF16).reshape(4, rl * rl, CZ)
        push(name, send[name], recv[name], True)

    def pair_receive(name):
        rows = 8 * rl
        swap = one_hot(rows * rl, rows * rl, lambda r: ((r % rows) // rl) * (rl * rl) + (r // rows) * rl + r % rl)

        for g in range(n // 8):
            got = mm(swap, recv[name][g * 8:(g + 1) * 8].reshape(rows * rl, CZ)).astype(BF16)
            for i in range(rl):
                znb[i, g * rows:(g + 1) * rows, :] = got[i * rows:(i + 1) * rows]
        for i in range(rl):
            zb[i] = znb[i].astype(F32).T.astype(BF16)

    def outer_update(name, left, wo, zref, dst):
        swap = swap_matrix(4 * rl, 16)
        width = 4 * rl

        per_y = side // 2
        for g in range(n // 4):
            for half in range(OP // 16):
                got = recv[name][g // per_y, (g % per_y) * 2:(g % per_y) * 2 + 2].reshape(width, OP, S)[:, half * 16:(half + 1) * 16].reshape(width * 16, S)
                perm[half * 16:(half + 1) * 16, g * width:(g + 1) * width, :] = mm(swap, got).astype(BF16).reshape(16, width, S)
        for t in range(OP // 2):
            o = mm(left[...], perm[t * 2:t * 2 + 2].reshape(2 * R, S), NT).astype(BF16)
            for u in range(2):
                for i in range(rl):
                    obuf[(t * 2 + u) * OP:(t * 2 + u + 1) * OP, i * R:(i + 1) * R] = o[i * OP:(i + 1) * OP, u * R:(u + 1) * R]
        upd = mm(wo, obuf[...])
        for i in range(rl):
            dst[i] = (zref[i].astype(F32) + upd[:, i * R:(i + 1) * R] * (1.0 / (1e-3 + norm_ref[i:i + 1, :]))).astype(BF16)

    def row_bias_weight(b):
        got = wb[:, b, :].astype(F32)
        return jnp.concatenate([got, jnp.zeros((HP - H, CZ), F32)], axis=0).astype(BF16)

    def project(x, w, p):
        qvg[p, 0:WM] = mm(w[0:WM], x, NT).astype(BF16)
        kbuf[p] = mm(x, w[WM:2 * WM], NT).astype(BF16)
        qvg[p, WM:3 * WM] = mm(w[2 * WM:4 * WM], x, NT).astype(BF16)

    per_tile = 128 // D
    tile_lane = lax.broadcasted_iota(jnp.int32, (16, 128), 1) // D
    head_mask = [jnp.where(tile_lane == j, 1.0, 0.0).astype(BF16) for j in range(per_tile)]

    def attend(p, lo, size, mask, bias):
        scale = D ** -0.5 * LOG2E
        keys = slice(lo, lo + size)

        def query(h, q):
            j = h % per_tile
            parts = [qvg[p, h * D:(h + 1) * D, q:q + 128]]
            if j:
                parts.insert(0, jnp.zeros((j * D, 128), BF16))
            if j + 1 < per_tile:
                parts.append(jnp.zeros(((per_tile - 1 - j) * D, 128), BF16))
            return jnp.concatenate(parts, axis=0)

        def logits(group):
            h, q = group[0]
            tile = (h // per_tile) * 128
            if len(group) == 1:
                kt = kbuf[p, keys, tile:tile + 128].reshape(size // 16, 16, 128)
                kh = (kt * head_mask[h % per_tile][None]).reshape(size, 128)
                return mm(kh, qvg[p, tile:tile + 128, q:q + 128])
            return mm(kbuf[p, keys, tile:tile + 128], jnp.concatenate([query(h, q) for h, q in group], axis=1))
        blocks = [(h, q) for h in range(H) for q in range(lo, lo + size, 128)]
        step = size // 128
        groups = [blocks[b:b + step] for b in range(0, len(blocks), step)]
        ahead = logits(groups[0])
        for b, group in enumerate(groups):
            now = ahead
            if b + 1 < len(groups):
                ahead = logits(groups[b + 1])
            for u, (h, q) in enumerate(group):
                t = now[:, u * 128:(u + 1) * 128] * scale
                if bias is not None:
                    t = t + bias[h]
                t = jnp.where(mask > 0, t, NEG)
                e, inverse = softmax_cols(t)
                o = mm(qvg[p, WM + h * D:WM + (h + 1) * D, keys], e) * inverse
                g = qvg[p, 2 * WM + h * D:2 * WM + (h + 1) * D, q:q + 128].astype(F32)
                gbuf[h * D:(h + 1) * D, q:q + 128] = (o * jax.nn.sigmoid(g)).astype(BF16)

    def row_project(src, w):
        @pl.loop(0, sl // 2)
        def _(t):
            xf = src[pl.ds(2 * t, 2)].astype(F32).reshape(2 * R, CM)
            project(norm_axis(xf, 1), w, t)

    def row_attend(src, wo, bias, dst, lo, hi):
        @pl.loop(lo, hi)
        def _(t):
            for u in range(2):
                row = seqmask[pl.ds(2 * t + u, 1), :]
                mask = mm(eye, jnp.broadcast_to(row, (R, R)).astype(BF16), NT)
                attend(t, u * R, R, mask, bias)
            xf = src[pl.ds(2 * t, 2)].astype(F32).reshape(2 * R, CM)
            upd = mm(gbuf[...], wo[...], TN)
            dst[pl.ds(2 * t, 2)] = (xf + upd).astype(BF16).reshape(2, R, CM)

    def col_attention(load, w, wo, wp, a_dst, c_dst, after):
        @pl.loop(0, rl)
        def _(i):
            xf = load(i)
            project(norm_axis(xf, 1), w, 0)
            pick = jnp.where(lax.broadcasted_iota(jnp.int32, (R, R), 0) == me * rl + i, 1.0, 0.0).astype(BF16)
            attend(0, 0, S, mm(mcolmask[...], pick), None)
            y = (xf + mm(gbuf[...], wo[...], TN)).astype(BF16)
            mcol[i] = y
            x = norm_axis(y.astype(F32), 1)
            half = (mm(wp, x, NT) * colmask[pl.ds(i, 1), :]).astype(BF16)
            at = pl.ds(pl.multiple_of(i * OP, OP), OP)
            a_dst[at, :] = half[0:OP]
            c_dst[at, :] = half[OP:2 * OP]
            after(i)

    for load in inputs:
        load.wait()
    maskf = mask_ref[...].astype(F32).astype(BF16)
    mcolmask[...] = maskf
    seqmask[...] = mask_ref[pl.ds(pl.multiple_of(me * sl, sl), sl), :].astype(F32)
    rmaskt[...] = mm(eye, jnp.broadcast_to(rmask_ref[...].astype(F32), (R, R)).astype(BF16), NT)
    pick = jnp.where(lax.broadcasted_iota(jnp.int32, (8, R), 1) == lax.broadcasted_iota(jnp.int32, (8, R), 0) + me * rl, 1.0, 0.0).astype(BF16)
    colmask[...] = mm(pick, maskf, NT)
    norm_ref[...] = mm(colmask[...].astype(BF16), maskf)

    pair_norm(z_ref)
    ld_wb.wait()
    pl.semaphore_wait(barrier, n - 1)
    bias_block('b1', row_bias_weight(0), H)
    ld_wr.wait()
    row_project(m_ref, wr.at[0])
    ld_wro.wait()
    ld_wpo.wait()
    swap = swap_matrix(16, 16)
    for p in range(OP // 16):
        for q in range(OP // 16):
            got = wpo[0].reshape(OP, OP, CZ)[p * 16:(p + 1) * 16, q * 16:(q + 1) * 16].reshape(256, CZ)
            wtmp[q * 16:(q + 1) * 16, p * 16:(p + 1) * 16, :] = mm(swap, got).astype(BF16).reshape(16, 16, CZ)
    wpot[0] = wtmp[...].reshape(OP * OP, CZ).astype(F32).T.astype(BF16)
    wpot[1] = wpo[1].astype(F32).T.astype(BF16)
    arrived('b1')
    bias_build('b1', H, 8, bias_f, True)

    row_attend(m_ref, wro.at[0], bias_f, mrow, 0, sl // 2)

    per = 16 // rl
    split = one_hot(16 * sl, 16 * sl, lambda r: (r % sl) * 16 + ((r // (2 * sl)) % per) * rl + (r // (2 * sl * per)) * 2 + (r // sl) % 2)

    for g in range(R // 16):
        got = mm(split, mrow[:, g * 16:(g + 1) * 16, :].reshape(sl * 16, CM)).astype(BF16).reshape(2, per, 2 * sl, CM)
        for pair in range(2):
            send['m1'][pair, g * per:(g + 1) * per] = got[pair]
    for pair in range(2):
        push('m1_%d' % pair, send['m1'].at[pair], recv['m1'].at[pair], True)

    for load in (ld_wsb, ld_ws, ld_wso, ld_web, ld_we, ld_weo):
        load.wait()
    heads = one_hot(WP, WT, lambda r: jnp.where(r % DP < DT, (r % DP) * HT + r // DP, -1))
    for raw, out, turned, dst in ((ws, wso, wsp, wsot), (we, weo, wep, weot)):
        for b in range(2):
            for f in range(4):
                turned[b, f * WP:(f + 1) * WP] = mm(heads, raw[b, f * WT:(f + 1) * WT]).astype(BF16)
            dst[b] = mm(heads, out[b]).T.astype(BF16)

    ld_wc.wait()
    ld_wco.wait()
    ld_wpi.wait()
    arrived('m1_0')

    def load_first(i):
        pl.when(i == 2)(lambda: arrived('m1_1'))
        got = recv['m1'][i // 2].astype(F32)
        return jnp.where(i % 2 == 0, got[:, 0:sl], got[:, sl:2 * sl]).reshape(S, CM)

    def after_first(i):
        pl.when(i == rl // 2 - 1)(lambda: spread('c', 0))
    col_attention(load_first, wc.at[0], wco.at[0], wpi[0], abuf, send['c'], after_first)
    spread('c', 1)
    relay('c', 0)

    def send_cols(pair):
        got = [mcol[2 * pair + u].astype(F32).reshape(n, sl, CM) for u in range(2)]
        send['m2'][pair] = jnp.concatenate(got, axis=1).astype(BF16)
        push('m2_%d' % pair, send['m2'].at[pair], recv['m2'].at[pair], True)

    def after_second(i):
        @pl.when(i == 0)
        def _():
            relay('c', 1)

        @pl.when(i == 1)
        def _():
            spread('a', 0)
            send_cols(0)

        @pl.when(i == 2)
        def _():
            share('c')
    col_attention(lambda i: mcol[i].astype(F32), wc.at[1], wco.at[1], wpi[1], send['a'], cbuf2, after_second)
    spread('a', 1)

    arrived('c_t')
    outer_update('c', abuf, wpot[0], z_ref, zb)
    pair_norm(zb)
    bias_block('s1', wsb[0], HT)
    pair_project(wsp[0])
    arrived('s1')
    relay('a', 0)
    relay('a', 1)
    bias_build('s1', HT, 4, biast_f, True)
    pair_attend(zb, wsot[0], zb)
    pair_send('z1')
    pair_norm(zb)
    bias_block('e1', web[0], HT)
    share('a')
    send_cols(1)
    arrived('z1')
    pair_receive('z1')
    pair_norm(zb)
    pair_project(wep[0])
    arrived('e1')
    bias_build('e1', HT, 4, biast_f, False)
    pair_attend(zb, weot[0], zb)

    pair_norm(zb)
    bias_pack('b2', row_bias_weight(1), H)
    arrived('a_t')
    outer_update('a', cbuf2, wpot[1], zb, zb)
    pair_norm(zb)
    bias_block('e2', web[1], HT)
    push('b2', send['b2'], recv['b2'], False)
    pair_project(wep[1])
    arrived('m2_0')
    arrived('m2_1')
    unsplit = one_hot(16 * sl, 16 * sl, lambda r: ((r % 4) // 2) * (8 * sl) + ((r % 16) // 4) * (2 * sl) + (r % 2) * sl + r // 16)

    for g in range(R // 16):
        got = jnp.concatenate([recv['m2'][pair, g * per:(g + 1) * per].reshape(8 * sl, CM) for pair in range(2)], axis=0)
        mrow[:, g * 16:(g + 1) * 16, :] = mm(unsplit, got).astype(BF16).reshape(sl, 16, CM)
    row_project(mrow, wr.at[1])
    arrived('e2')
    bias_build('e2', HT, 4, biast_f, True)
    pair_attend(zb, weot[1], zb)
    pair_send('z2')
    pair_norm(zb)
    bias_block('s2', wsb[1], HT)
    arrived('b2')
    bias_build('b2', H, 8, bias_f, False)
    row_attend(mrow, wro.at[1], bias_f, mfinal, 0, sl // 2)
    store = pltpu.make_async_copy(mfinal, m_out, in_sem.at[0])
    store.start()
    arrived('z2')
    pair_receive('z2')
    pair_norm(zb)
    pair_project(wsp[1])
    arrived('s2')
    bias_build('s2', HT, 4, biast_f, False)
    pair_attend(zb, wsot[1], z_out)
    store.wait()
    for flow in FLOWS:
        wait_for(flow, send_sem, like(flow))


def solution(mesh):
    n = mesh.shape['dap']

    def local_step(m, z, mask, rmask, w_row_bias, w_row_in, w_row_out, w_col_in, w_col_out, w_opm_in, w_opm_out, w_ts_bias, w_ts_in, w_ts_out, w_te_bias, w_te_in, w_te_out):
        sl, R, CM = m.shape
        rl, _, CZ = z.shape
        S = mask.shape[0]
        H, D = w_row_in.shape[3:]
        HT, DT = w_ts_in.shape[3:]
        OP = w_opm_in.shape[3]
        HP = -(-H // 8) * 8
        WM, WT = H * D, HT * DT
        WP = HT * -(-DT // 16) * 16
        zt = z.transpose(0, 2, 1)
        wb = w_row_bias.transpose(2, 0, 1)
        wr = w_row_in.transpose(0, 2, 3, 4, 1).reshape(2, 4 * WM, CM)
        wc = w_col_in.transpose(0, 2, 3, 4, 1).reshape(2, 4 * WM, CM)
        wro = w_row_out.reshape(2, WM, CM)
        wco = w_col_out.reshape(2, WM, CM)
        wpi = w_opm_in.transpose(0, 2, 3, 1).reshape(2, 2 * OP, CM)
        wpo = w_opm_out.reshape(2, OP * OP, CZ)
        wsb = w_ts_bias.transpose(0, 2, 1)
        web = w_te_bias.transpose(0, 2, 1)
        ws = w_ts_in.transpose(0, 2, 4, 3, 1).reshape(2, 4 * WT, CZ)
        we = w_te_in.transpose(0, 2, 4, 3, 1).reshape(2, 4 * WT, CZ)
        wso = w_ts_out.transpose(0, 2, 1, 3).reshape(2, WT, CZ)
        weo = w_te_out.transpose(0, 2, 1, 3).reshape(2, WT, CZ)
        weights = [wb, wr, wro, wc, wco, wpi, wpo, wsb, ws, wso, web, we, weo]

        def vm(shape, dtype=BF16):
            return pltpu.VMEM(shape, dtype)
        scratch = [vm(w.shape) for w in weights]
        scratch += [vm((OP, OP, CZ)), vm((2, CZ, OP * OP)), vm((2, CZ, WP)), vm((2, CZ, WP))]
        scratch += [vm((H, R, R), F32), vm((HT, R, R), F32)]
        scratch += [vm((CZ, rl * R)), vm((rl, 4 * WP, R)), vm((2, WP, R)), vm((2, 4 * WP, CZ)), vm((2, 4 * WP, CZ))]
        scratch += [vm((sl // 2, 3 * WM, S)), vm((sl // 2, S, WM)), vm((WM, S))]
        scratch += [vm((sl, R, CM)), vm((rl, S, CM)), vm((rl, CZ, R)), vm((rl, R, CZ))]
        scratch += [vm((rl * OP, S))] * 4 + [vm((OP, R, S)), vm((OP * OP, rl * R))]
        scratch += [vm((S, R)), vm((sl, R), F32), vm((R, R), F32), vm((8, S), F32), vm((8, R), F32)]
        side = math.isqrt(n // 2)
        bias_row, bias_tri = (rl * H, R), (rl * HT, R)
        shapes = {'b1': bias_row, 'b2': bias_row, 's1': bias_tri, 'e1': bias_tri, 'e2': bias_tri, 's2': bias_tri,
                  'c': (rl * OP, S), 'a': (rl * OP, S), 'm1': (rl * sl // 2, CM), 'm2': (rl * sl // 2, CM), 'z1': (rl * rl, CZ), 'z2': (rl * rl, CZ)}
        for name in EXCHANGES:
            shape = shapes[name]
            if name in 'ac':
                scratch += [vm(shape), vm((side, side, 2) + shape)]
            elif name[0] == 'm':
                scratch += [vm((2, n) + shape), vm((2, n) + shape)]
            else:
                scratch += [vm((n,) + shape if name[0] == 'z' else shape), vm((n,) + shape)]
        scratch += [pltpu.SemaphoreType.DMA((len(FLOWS),)), pltpu.SemaphoreType.DMA((len(FLOWS),)), pltpu.SemaphoreType.DMA((len(weights),))]
        scratch += [vm(m.shape), vm(zt.shape), vm(mask.shape, mask.dtype), vm((1, R), rmask.dtype), vm(m.shape), pltpu.SemaphoreType.DMA((4,))]
        cfg = (n, sl, rl, S, R, CM, CZ, H, D, HT, DT, OP, HP)
        vmem = pl.BlockSpec(memory_space=pltpu.VMEM)
        hbm = pl.BlockSpec(memory_space=pl.ANY)
        m_new, z_new = pl.pallas_call(
            functools.partial(step_kernel, cfg),
            out_shape=[jax.ShapeDtypeStruct(m.shape, BF16), jax.ShapeDtypeStruct(zt.shape, BF16)],
            in_specs=[hbm] * (4 + len(weights)),
            out_specs=[hbm, vmem],
            scratch_shapes=scratch,
            compiler_params=pltpu.CompilerParams(collective_id=0, has_side_effects=True, vmem_limit_bytes=60 * 2**20),
            name='evoformer',
        )(m, zt, mask, rmask.reshape(1, R), *weights)
        return m_new, z_new.transpose(0, 2, 1)

    in_specs = (P(('data', 'dap')), P(('data', 'dap')), P('data'), P('data')) + (P(),) * 13
    out_specs = (P(('data', 'dap')), P(('data', 'dap')))
    return jax.shard_map(local_step, mesh=mesh, in_specs=in_specs, out_specs=out_specs, check_vma=False)
```
